32 devices in a mesh: dp: 2 (over core), ctx: 4 (over z), tensor: 4 (over y, x).
Axes of the slice: x: 2, y: 2, z: 4, core: 2. Of those that a mesh axis runs over, the one named last changes fastest.
Arguments:
- tokens: bfloat16 [2, 1024, 2048], P('dp', 'ctx'), may hold values from -30 to 30
- segments: int32 [2, 1024], P('dp'), may hold values from 0 to 3, never falling along the last dimension, each value on 1 to 512 neighbouring positions
- first_gain: bfloat16 [2048], replicated, may hold values from 0.5 to 1.5
- query_weight: bfloat16 [2048, 2048], P(None, 'tensor'), may hold values from -0.125 to 0.125
- key_matrix: bfloat16 [2048, 1024], P(None, 'tensor'), may hold values from -0.125 to 0.125
- value_matrix: bfloat16 [2048, 1024], P(None, 'tensor'), may hold values from -0.125 to 0.125
- query_norm_gain: bfloat16 [128], replicated, may hold values from 0.5 to 1.5
- key_gain: bfloat16 [128], replicated, may hold values from 0.5 to 1.5
- output_weight: bfloat16 [2048, 2048], P('tensor'), may hold values from -1.5 to 1.5
- second_gain: bfloat16 [2048], replicated, may hold values from 0.5 to 1.5
- gate_weight: bfloat16 [2048, 6144], P(None, 'tensor'), may hold values from -0.125 to 0.125
- up_weight: bfloat16 [2048, 6144], P(None, 'tensor'), may hold values from -0.125 to 0.125
- down_weight: bfloat16 [6144, 2048], P('tensor'), may hold values from -0.078125 to 0.078125
- cotangent: bfloat16 [2, 1024, 2048], P('dp', 'ctx'), may hold values from -6 to 6
Outputs:
- outputs: bfloat16 [2, 1024, 2048], P('dp', 'ctx')
- token_grad: bfloat16 [2, 1024, 2048], P('dp', 'ctx')
- first_gain_grad: float32 [2048], replicated
- query_weight_grad: float32 [2048, 2048], P(('dp', 'ctx'), 'tensor')
- key_weight_grad: float32 [2048, 1024], P(('dp', 'ctx'), 'tensor')
- value_weight_grad: float32 [2048, 1024], P(('dp', 'ctx'), 'tensor')
- query_gain_grad: float32 [128], replicated
- key_gain_grad: float32 [128], replicated
- output_weight_grad: float32 [2048, 2048], P('tensor', ('dp', 'ctx'))
- second_gain_grad: float32 [2048], replicated
- gate_weight_grad: float32 [2048, 6144], P(('dp', 'ctx'), 'tensor')
- up_weight_grad: float32 [2048, 6144], P(('dp', 'ctx'), 'tensor')
- down_weight_grad: float32 [6144, 2048], P('tensor', ('dp', 'ctx'))
The draws below stay inside these ranges and needn't reach their ends.
Inputs may be any that keep to these rules, and one draw needn't show every extreme that they name: `segments`: in each sequence the segment numbers never fall and every number of 0 to 3 appears; every document has 1 to 512 tokens and one has exactly 512.
All inputs are finite; a program needn't handle non-finite values.
Results may differ from the reference program's by a relative error of at most 0.03.
Values may be sent and summed in bfloat16 or wider, within the bound.
A program may use at most 192 MiB of HBM per device.

```python
import math
import jax
import jax.numpy as jnp
import numpy as np
from jax import lax

MODEL_DIM = 2048
QUERY_HEADS = 16
KEY_VALUE_HEADS = 8
HEAD_DIM = 128
FF = 6144
DOCS = 4
SEQUENCE_LENGTH = 1024
SEQS = 2
DOC_MOST = 512


def draw_tokens(key, part):
    noise_key, row_key, column_key = jax.random.split(key, 3)
    row_scale = jnp.exp(jax.random.uniform(row_key, (SEQS, SEQUENCE_LENGTH, 1), jnp.float32, math.log(0.5), math.log(2.0)))
    column_scale = jnp.exp(jax.random.uniform(column_key, (1, 1, MODEL_DIM), jnp.float32, math.log(0.3), math.log(3.0)))
    base = jnp.clip(jax.random.normal(noise_key, (SEQS, SEQUENCE_LENGTH, MODEL_DIM), jnp.float32), -5.0, 5.0)
    return (base * row_scale * column_scale).astype(jnp.bfloat16)


def strengthened(array, stream_key, source, target, parts, factor):
    owner, partner = [(jnp.arange(array.shape[dim]) // (array.shape[dim] // parts)).reshape([-1 if axis == dim else 1 for axis in range(array.ndim)]) for dim in (source, target)]
    chosen = jax.random.permutation(stream_key, parts)[partner]
    strong = (owner == chosen) | (owner == (partner + parts // 2) % parts)
    return jnp.where(strong, factor * array, array)


def levels(own_key, shape, pieces, least, high):
    def one(dim, shards_of):
        draws = jax.random.uniform(jax.random.fold_in(jax.random.fold_in(own_key, 6), dim), (shards_of,), jnp.float32, least / len(pieces), high / len(pieces))
        return jnp.repeat(jnp.exp(draws), shape[dim] // shards_of).reshape((-1,) + (1,) * (len(shape) - dim - 1))

    level = one(*pieces[0])
    for cut in pieces[1:]:
        level = level * one(*cut)
    return level


def length_profile(count, total, bound, lean):
    loads = [(1 << 20) // math.isqrt(standing ** lean) + 1 for standing in range(2, count + 1)]
    surplus, counts = total - bound - (count - 1), [1] * (count - 1)
    while surplus > 0:
        candidates = [i for i in range(count - 1) if counts[i] < bound]
        pool, left = sum([loads[i] for i in candidates]), surplus
        for i in candidates:
            extra = min(bound - counts[i], max(1, left * loads[i] // pool), surplus)
            counts[i] = counts[i] + extra
            surplus = surplus - extra
    return np.array([bound] + counts)


def ragged_sizes(rng, count, total, most, lean):
    if count == 2:
        one = jax.random.randint(rng, (), max(1, total - most), min(most, total - 1) + 1)
        return jnp.stack([one, total - one])
    tallies = jnp.asarray(length_profile(count, total, most, lean), jnp.int32)
    couples = (count - 1) // 2
    donor, taker = tallies[1:1 + 2 * couples:2], tallies[2:2 + 2 * couples:2]
    room = jnp.minimum(donor - 1, most - taker)
    shifted = jax.random.randint(jax.random.fold_in(rng, 1), (couples,), 0, 1 << 20) % (room + 1)
    tallies = tallies.at[1:1 + 2 * couples:2].set(donor - shifted).at[2:2 + 2 * couples:2].set(taker + shifted)
    return tallies[jax.random.permutation(jax.random.fold_in(rng, 2), count)]


def bell_draw(rng, dims, width, most, cuts=(), kind=jnp.bfloat16):
    result = width * jax.random.normal(rng, dims, jnp.float32)
    if cuts:
        result = result * levels(rng, dims, cuts, -0.22, 0.18)
    return jnp.clip(result, -most, most).astype(kind)


def heavy_noise(rng, shape, deviation, bound, shards, heavy, kind=jnp.bfloat16):
    array = deviation * jax.random.normal(rng, shape, jnp.float32)
    if shards:
        array = array * levels(rng, shape, shards, -0.22, 0.18)
    return jnp.clip(strengthened(array, jax.random.fold_in(rng, 3), *heavy), -bound, bound).astype(kind)


def setup_inputs(seed: int = 0) -> dict:
    key_of = jax.random.split(jax.random.key(seed), 15)
    return {
        "tokens": draw_tokens(jax.random.fold_in(key_of[14], 71), 0),
        "segments": jax.vmap(lambda own: jnp.searchsorted(jnp.cumsum(ragged_sizes(own, DOCS, SEQUENCE_LENGTH, DOC_MOST, 0)), jnp.arange(SEQUENCE_LENGTH), side="right"))(jax.random.split(key_of[1], SEQS)).reshape((SEQS, SEQUENCE_LENGTH)).astype(jnp.int32),
        "first_gain": jnp.clip(1.0 + 0.1 * jax.random.normal(key_of[2], (MODEL_DIM,), jnp.float32), 0.5, 1.5).astype(jnp.bfloat16),
        "query_weight": bell_draw(key_of[3], (MODEL_DIM, QUERY_HEADS * HEAD_DIM), MODEL_DIM ** -0.5, 0.125, ((1, 4),)),
        "key_matrix": bell_draw(key_of[4], (MODEL_DIM, KEY_VALUE_HEADS * HEAD_DIM), MODEL_DIM ** -0.5, 0.125, ((1, 4),)),
        "value_matrix": bell_draw(key_of[5], (MODEL_DIM, KEY_VALUE_HEADS * HEAD_DIM), MODEL_DIM ** -0.5, 0.125, ((1, 4),)),
        "query_norm_gain": jnp.clip(1.0 + 0.1 * jax.random.normal(key_of[6], (HEAD_DIM,), jnp.float32), 0.5, 1.5).astype(jnp.bfloat16),
        "key_gain": jnp.clip(1.0 + 0.1 * jax.random.normal(key_of[7], (HEAD_DIM,), jnp.float32), 0.5, 1.5).astype(jnp.bfloat16),
        "output_weight": bell_draw(key_of[8], (QUERY_HEADS * HEAD_DIM, MODEL_DIM), (QUERY_HEADS * HEAD_DIM // 128) ** -0.5, 1.5, ((0, 4),)),
        "second_gain": jnp.clip(1.0 + 0.1 * jax.random.normal(key_of[9], (MODEL_DIM,), jnp.float32), 0.5, 1.5).astype(jnp.bfloat16),
        "gate_weight": bell_draw(key_of[10], (MODEL_DIM, FF), MODEL_DIM ** -0.5, 0.125, ((1, 4),)),
        "up_weight": bell_draw(key_of[11], (MODEL_DIM, FF), MODEL_DIM ** -0.5, 0.125, ((1, 4),)),
        "down_weight": bell_draw(key_of[12], (FF, MODEL_DIM), FF ** -0.5, 0.078125, ((0, 4),)),
        "cotangent": heavy_noise(key_of[13], (SEQS, SEQUENCE_LENGTH, MODEL_DIM), 1.0, 6.0, ((0, 2), (1, 4)), (1, 2, 4, 2.0)),
    }


epsilon = 1e-06
rope_base = 1000000.0
block_rows = 512
highest_precision = lax.Precision.HIGHEST

@jax.custom_vjp
def lower_precision(v):
    return lax.optimization_barrier(v.astype(jnp.bfloat16)).astype(jnp.float32)

@jax.custom_vjp
def lower_backward(v):
    return v

def low_keep(v):
    return (lower_precision(v), None)

def low_pass(kept, grad):
    return (grad,)

def back_keep(v):
    return (v, None)

def back_low(kept, grad):
    return (lower_precision(grad),)
lower_precision.defvjp(low_keep, low_pass)
lower_backward.defvjp(back_keep, back_low)

def root_mean_norm(values, gain_vector):
    return values * lax.rsqrt(lax.optimization_barrier(jnp.mean(values * values, axis=-1, keepdims=True)) + epsilon) * gain_vector

def rotary_apply(values, cosine_table, sine_table):
    middle = values.shape[-1] // 2
    turned = jnp.concatenate([-values[..., middle:], values[..., :middle]], axis=-1)
    return values * cosine_table + turned * sine_table

def rope_tables(segment_row):
    length_total = segment_row.shape[0]
    places = jnp.arange(length_total, dtype=jnp.int32)
    starts = jnp.concatenate([jnp.ones((1,), dtype=jnp.bool_), segment_row[1:] != segment_row[:-1]])
    begins = lax.cummax(jnp.where(starts, places, 0).astype(jnp.int32), axis=0)
    position = (places - begins).astype(jnp.float32)
    inverse = 1.0 / rope_base ** (jnp.arange(0, HEAD_DIM, 2, dtype=jnp.float32) / HEAD_DIM)
    angles = position[:, None] * inverse[None, :]
    angles = jnp.concatenate([angles, angles], axis=-1)
    return (jnp.cos(angles)[:, None, :], jnp.sin(angles)[:, None, :])

def block_layer(token_rows, params, cosine_table, sine_table, segment_row):
    first_gain, query_weight, key_matrix, value_matrix, query_norm_gain, key_gain, output_weight, second_gain, gate_weight, up_weight, down_weight = params
    first_input_rows = lower_precision(root_mean_norm(token_rows, first_gain))
    query_unnormed = lower_backward(jnp.dot(first_input_rows, query_weight, precision=highest_precision)).reshape(SEQUENCE_LENGTH, QUERY_HEADS, HEAD_DIM)
    key_unnormed = lower_backward(jnp.dot(first_input_rows, key_matrix, precision=highest_precision)).reshape(SEQUENCE_LENGTH, KEY_VALUE_HEADS, HEAD_DIM)
    value_matrix_rows = lower_precision(lower_backward(jnp.dot(first_input_rows, value_matrix, precision=highest_precision))).reshape(SEQUENCE_LENGTH, KEY_VALUE_HEADS, HEAD_DIM)
    query_matrix_rows = lower_precision(rotary_apply(root_mean_norm(query_unnormed, query_norm_gain), cosine_table, sine_table)).reshape(SEQUENCE_LENGTH, KEY_VALUE_HEADS, QUERY_HEADS // KEY_VALUE_HEADS, HEAD_DIM)
    key_rows = lower_precision(rotary_apply(root_mean_norm(key_unnormed, key_gain), cosine_table, sine_table))
    query_block_rows = min(block_rows, SEQUENCE_LENGTH)
    block_count = SEQUENCE_LENGTH // query_block_rows
    key_places = jnp.arange(SEQUENCE_LENGTH, dtype=jnp.int32)

    def attend(block_start):
        query_block = lax.dynamic_slice_in_dim(query_matrix_rows, block_start, query_block_rows, 0)
        query_places = block_start + jnp.arange(query_block_rows, dtype=jnp.int32)
        query_segments = lax.dynamic_slice_in_dim(segment_row, block_start, query_block_rows, 0)
        scores = jnp.einsum('chgd,khd->hgck', query_block, key_rows, precision=highest_precision) * (1.0 / math.sqrt(HEAD_DIM))
        scores = lower_backward(scores)
        allowed = (key_places[None, :] <= query_places[:, None]) & (segment_row[None, :] == query_segments[:, None])
        weights = jnp.where(allowed, jnp.exp(scores), 0.0)
        totals = lax.optimization_barrier(jnp.sum(weights, axis=-1))
        summed = lower_backward(jnp.einsum('hgck,khd->chgd', lower_precision(weights), value_matrix_rows, precision=highest_precision))
        return summed / jnp.moveaxis(totals, 2, 0)[..., None]
    block_starts = (jnp.arange(block_count, dtype=jnp.int32) * query_block_rows).astype(jnp.int32)
    attended = lax.map(jax.checkpoint(attend), block_starts).reshape(SEQUENCE_LENGTH, QUERY_HEADS * HEAD_DIM)
    mixed_sum = lower_backward(jnp.dot(lower_precision(attended), output_weight, precision=highest_precision))
    resid_rows = token_rows + mixed_sum
    second_input = lower_precision(root_mean_norm(resid_rows, second_gain))
    gate_value = lower_backward(jnp.dot(second_input, gate_weight, precision=highest_precision))
    up_value = lower_backward(jnp.dot(second_input, up_weight, precision=highest_precision))
    hidden = lower_precision(jax.nn.silu(gate_value) * up_value)
    return resid_rows + lower_backward(jnp.dot(hidden, down_weight, precision=highest_precision))

def reference(tokens, segments, first_gain, query_weight, key_matrix, value_matrix, query_norm_gain, key_gain, output_weight, second_gain, gate_weight, up_weight, down_weight, cotangent):
    params = tuple((weight_item.astype(jnp.float32) for weight_item in (first_gain, query_weight, key_matrix, value_matrix, query_norm_gain, key_gain, output_weight, second_gain, gate_weight, up_weight, down_weight)))

    def per_sequence(grad_carry, seq_item):
        token_seq, segment_row, grad_seq = seq_item
        cosine_table, sine_table = rope_tables(segment_row)

        def forward(token_rows, param_tuple):
            return block_layer(token_rows, param_tuple, cosine_table, sine_table, segment_row)
        result_rows, pull_back = jax.vjp(forward, token_seq.astype(jnp.float32), params)
        grad_tokens, grad_params = pull_back(grad_seq.astype(jnp.float32))
        grad_carry = tuple((carried + added for carried, added in zip(grad_carry, grad_params)))
        return (grad_carry, (result_rows.astype(jnp.bfloat16), grad_tokens.astype(jnp.bfloat16)))
    zero_grads = tuple((jnp.zeros(weight_item.shape, jnp.float32) for weight_item in params))
    grad_totals, (out_rows, grad_rows) = lax.scan(per_sequence, zero_grads, (tokens, segments, cotangent))
    return (out_rows, grad_rows, grad_totals[0], grad_totals[1], grad_totals[2], grad_totals[3], grad_totals[4], grad_totals[5], grad_totals[6], grad_totals[7], grad_totals[8], grad_totals[9], grad_totals[10])
```

```python
import math

import jax
import jax.numpy as jnp
from jax import lax
from jax.sharding import PartitionSpec as P


epsilon = 1e-06
rope_base = 1000000.0
F32 = jnp.float32
BF16 = jnp.bfloat16


def dot(a, b):
    return jnp.dot(a, b, preferred_element_type=F32)


def dot_nt(a, b):
    return lax.dot_general(a, b, (((1,), (1,)), ((), ())), preferred_element_type=F32)


def dot_tn(a, b):
    return lax.dot_general(a, b, (((0,), (0,)), ((), ())), preferred_element_type=F32)


def norm_forward(values, gain_vector):
    scale_factor = lax.rsqrt(jnp.mean(values * values, axis=-1, keepdims=True) + epsilon)
    normalized = values * scale_factor
    return (normalized * gain_vector, normalized, scale_factor)


def norm_backward(grad_out, gain_vector, normalized, scale_factor):
    scaled = grad_out * gain_vector
    inner_mean = jnp.mean(scaled * normalized, axis=-1, keepdims=True)
    return scale_factor * (scaled - normalized * inner_mean)


def gain_sum(grad_out, normalized):
    return jnp.sum((grad_out * normalized).reshape(-1, normalized.shape[-1]), axis=0)


def rotary_apply(values, cosine_table, sine_table):
    middle = values.shape[-1] // 2
    turned = jnp.concatenate([-values[..., middle:], values[..., :middle]], axis=-1)
    return values * cosine_table + turned * sine_table


def rotate_back(grad_values, cosine_table, sine_table):
    middle = grad_values.shape[-1] // 2
    moved_grads = grad_values * sine_table
    turned = jnp.concatenate([moved_grads[..., middle:], -moved_grads[..., :middle]], axis=-1)
    return grad_values * cosine_table + turned


def shift_line(array, axis, by):
    n = lax.axis_size(axis)
    return lax.ppermute(array, axis, [(i, i + by) for i in range(n) if 0 <= i + by < n])


def swap(array, axis, bit):
    n = lax.axis_size(axis)
    return lax.ppermute(array, axis, [(i, i ^ bit) for i in range(n)])


def tensor_scatter(partial):
    n = lax.axis_size("tensor")
    me = lax.axis_index("tensor")
    rows = partial.shape[0] // n
    total = lax.dynamic_slice_in_dim(partial, me * rows, rows, 0)
    low = partial.astype(BF16)
    for j in range(1, n):
        block = lax.dynamic_slice_in_dim(low, (me ^ j) * rows, rows, 0)
        total = total + swap(block, "tensor", j).astype(F32)
    return total


def tensor_gather(shard):
    n = lax.axis_size("tensor")
    me = lax.axis_index("tensor")
    rows = shard.shape[0]
    out = jnp.zeros((n * rows, shard.shape[1]), shard.dtype)
    out = lax.dynamic_update_slice_in_dim(out, shard, me * rows, 0)
    for j in range(1, n):
        out = lax.dynamic_update_slice_in_dim(out, swap(shard, "tensor", j), (me ^ j) * rows, 0)
    return out


def line_gather(block):
    n = lax.axis_size("ctx")
    ups, downs = [], []
    up = down = block
    for _ in range(n - 1):
        up = shift_line(up, "ctx", 1)
        down = shift_line(down, "ctx", -1)
        ups.append(up)
        downs.append(down)
    z = lax.axis_index("ctx")
    own = [block]
    for d in range(1, n):
        own.append(jnp.where(z + d < n, downs[d - 1], ups[n - d - 1]))
    other = [swap(b, "dp", 1) for b in own]
    return own + other


def column_exchange(array):
    n = lax.axis_size("ctx")
    width = array.shape[1] // (2 * n)
    dp, z = lax.axis_index("dp"), lax.axis_index("ctx")
    slots = []
    for e in range(2):
        for d in range(n):
            target_dp, target_z = dp ^ e, (z - d) % n
            block = lax.dynamic_slice_in_dim(array, (target_dp * n + target_z) * width, width, 1)
            pairs = [
                (a * n + b, (a ^ e) * n + (b - d) % n) for a in range(2) for b in range(n)
            ]
            if e or d:
                block = lax.ppermute(block, ("dp", "ctx"), pairs)
            slots.append(block)
    return slots


def line_scatter(halves_fn, blocks_axis_rows):
    raise NotImplementedError


def block_scatter(partial):
    n = lax.axis_size("ctx")
    dp, z = lax.axis_index("dp"), lax.axis_index("ctx")
    mine = lax.dynamic_slice_in_dim(partial, dp * n, n, 0)
    theirs = lax.dynamic_slice_in_dim(partial, (1 - dp) * n, n, 0)
    summed = (mine.astype(F32) + swap(theirs, "dp", 1).astype(F32)).astype(BF16)

    def at(index):
        return lax.dynamic_index_in_dim(summed, jnp.clip(index, 0, n - 1), 0, keepdims=False)

    up = down = None
    for s in range(n - 1):
        send_up, send_down = at(z + n - 1 - s), at(z - (n - 1 - s))
        if s:
            send_up = (send_up.astype(F32) + up.astype(F32)).astype(BF16)
            send_down = (send_down.astype(F32) + down.astype(F32)).astype(BF16)
        up = lax.ppermute(send_up, "ctx", [(i, i + 1) for i in range(n - 1) if i <= s])
        down = lax.ppermute(send_down, "ctx", [(n - 1 - i, n - 2 - i) for i in range(n - 1) if i <= s])
    return at(z).astype(F32) + up.astype(F32) + down.astype(F32)


def slots_dot(left, right):
    return dot_tn(jnp.concatenate(left, 0), jnp.concatenate(right, 0))


def small_sum(vector):
    n_t, n_c = lax.axis_size("tensor"), lax.axis_size("ctx")
    total = vector
    for j in range(1, n_t):
        total = total + swap(vector, "tensor", j)
    first = total
    for e in range(2):
        for d in range(n_c):
            if e or d:
                pairs = [(a * n_c + b, (a ^ e) * n_c + (b ^ d)) for a in range(2) for b in range(n_c)]
                total = total + lax.ppermute(first, ("dp", "ctx"), pairs)
    return total


def per_device(
    tokens,
    segments,
    first_gain,
    query_weight,
    key_matrix,
    value_matrix,
    query_norm_gain,
    key_gain,
    output_weight,
    second_gain,
    gate_weight,
    up_weight,
    down_weight,
    cotangent,
):
    _, part_len, width = tokens.shape
    head = query_norm_gain.shape[0]
    query_heads = query_weight.shape[1] // head
    key_heads = key_matrix.shape[1] // head
    group = query_heads // key_heads
    n_ctx = lax.axis_size("ctx")
    n_tensor = lax.axis_size("tensor")
    z, t = lax.axis_index("ctx"), lax.axis_index("tensor")
    length = segments.shape[1]
    reach = -(-(length // 2 - 1) // part_len)
    share = part_len // n_tensor
    part_start = z * part_len
    first_gain_f = first_gain.astype(F32)
    second_gain_f = second_gain.astype(F32)
    query_gain_f = query_norm_gain.astype(F32)
    key_gain_f = key_gain.astype(F32)

    def share_of(rows):
        return lax.dynamic_slice_in_dim(rows, t * share, share, 0)

    token_low = tokens.reshape(part_len, width)
    cot = cotangent.reshape(part_len, width)
    x1 = norm_forward(token_low.astype(F32), first_gain_f)[0].astype(BF16)
    row = segments[0]
    places = jnp.arange(length, dtype=jnp.int32)
    my_segments = lax.dynamic_slice_in_dim(row, part_start, part_len, 0)
    my_places = part_start + jnp.arange(part_len, dtype=jnp.int32)
    earlier = (row[None, :] < my_segments[:, None]).astype(jnp.int32)
    begins = jnp.sum(earlier, axis=1)
    position = (my_places - begins).astype(F32)
    inverse = 1.0 / rope_base ** (jnp.arange(0, head, 2, dtype=F32) / head)
    angles = position[:, None] * inverse[None, :]
    angles = jnp.concatenate([angles, angles], axis=-1)
    cosine, sine = jnp.cos(angles)[:, None, :], jnp.sin(angles)[:, None, :]

    key_raw = dot(x1, key_matrix).reshape(part_len, key_heads, head)
    value = dot(x1, value_matrix).astype(BF16)
    key_scaled, key_normed, key_scale = norm_forward(key_raw, key_gain_f)
    key_rot = rotary_apply(key_scaled, cosine, sine).astype(BF16).reshape(part_len, -1)
    kv = jnp.concatenate([key_rot, value], axis=1)
    kv_list = [kv]
    for _ in range(reach):
        kv_list.append(shift_line(kv_list[-1], "ctx", 1))
    query_raw = dot(x1, query_weight).reshape(part_len, query_heads, head)
    query_scaled, query_normed, query_scale = norm_forward(query_raw, query_gain_f)
    query_rot = (
        rotary_apply(query_scaled, cosine, sine).astype(BF16).reshape(part_len, key_heads, group, head)
    )
    keys_all = jnp.concatenate(kv_list[::-1], axis=0)
    span = keys_all.shape[0]
    keys = keys_all[:, : key_heads * head].reshape(span, key_heads, head)
    values = keys_all[:, key_heads * head :].reshape(span, key_heads, head)
    padded_row = jnp.concatenate([jnp.full((reach * part_len,), -1, jnp.int32), row])
    key_segments = lax.dynamic_slice_in_dim(padded_row, part_start, span, 0)
    causal = jnp.arange(span)[None, :] <= (jnp.arange(part_len) + reach * part_len)[:, None]
    allowed = causal & (key_segments[None, :] == my_segments[:, None])
    inv_root = 1.0 / math.sqrt(head)

    scores = jnp.einsum("chgd,khd->hgck", query_rot, keys, preferred_element_type=F32) * inv_root
    weights = jnp.where(allowed, jnp.exp(scores), 0.0)
    totals = jnp.sum(weights, axis=-1)
    weights_low = weights.astype(BF16)
    summed = jnp.einsum("hgck,khd->chgd", weights_low, values, preferred_element_type=F32)
    totals_c = jnp.moveaxis(totals, 2, 0)[..., None]
    attended = summed / totals_c
    attended_low = attended.reshape(part_len, -1).astype(BF16)

    resid = share_of(token_low).astype(F32) + tensor_scatter(dot(attended_low, output_weight))
    second_scaled, second_normed, second_scale = norm_forward(resid, second_gain_f)
    x2 = tensor_gather(second_scaled.astype(BF16))

    cot_slots = column_exchange(cot)
    x1_slots = column_exchange(x1)
    grad_hidden = dot_nt(cot, down_weight)
    gate = dot(x2, gate_weight)
    up = dot(x2, up_weight)
    sig = jax.nn.sigmoid(gate)
    act = gate * sig
    hidden = (act * up).astype(BF16)
    hidden_slots = line_gather(hidden)
    grad_gate = (grad_hidden * up * (sig * (1.0 + gate * (1.0 - sig)))).astype(BF16)
    grad_up = (grad_hidden * act).astype(BF16)
    grad_second = tensor_scatter(dot_nt(grad_gate, gate_weight) + dot_nt(grad_up, up_weight))

    gate_partial = dot_tn(x2, grad_gate).astype(BF16).reshape(2 * n_ctx, -1, grad_gate.shape[1])
    up_partial = dot_tn(x2, grad_up).astype(BF16).reshape(2 * n_ctx, -1, grad_up.shape[1])
    gate_grad = block_scatter(gate_partial)
    up_grad = block_scatter(up_partial)
    outputs_share = (resid + tensor_scatter(dot(hidden, down_weight))).astype(BF16)
    outputs = tensor_gather(outputs_share)

    grad_resid = share_of(cot).astype(F32) + norm_backward(
        grad_second, second_gain_f, second_normed, second_scale
    )
    second_gain_part = gain_sum(grad_second, second_normed)
    grad_mixed = tensor_gather(grad_resid.astype(BF16))
    grad_attended = dot_nt(grad_mixed, output_weight).reshape(part_len, key_heads, group, head)
    output_partial = dot_tn(grad_mixed, attended_low).astype(BF16).reshape(2 * n_ctx, -1, attended_low.shape[1])
    output_grad = block_scatter(output_partial).T

    grad_scaled = (grad_attended / totals_c).astype(BF16)
    delta = jnp.moveaxis(jnp.sum(grad_attended * attended, axis=-1), 0, 2) / totals
    grad_weights = jnp.einsum("chgd,khd->hgck", grad_scaled, values, preferred_element_type=F32)
    grad_scores = (weights * (grad_weights - delta[..., None])).astype(BF16)
    grad_query = jnp.einsum("hgck,khd->chgd", grad_scores, keys, preferred_element_type=F32) * inv_root
    grad_keys = jnp.einsum("hgck,chgd->khd", grad_scores, query_rot, preferred_element_type=F32) * inv_root
    grad_values = jnp.einsum("hgck,chgd->khd", weights_low, grad_scaled, preferred_element_type=F32)
    grad_kv = jnp.concatenate([grad_keys.reshape(span, -1), grad_values.reshape(span, -1)], axis=1)
    grad_kv = grad_kv.reshape(reach + 1, part_len, -1)
    carry = None
    for r in range(reach):
        send = grad_kv[r] if carry is None else grad_kv[r] + carry.astype(F32)
        carry = shift_line(send.astype(BF16), "ctx", -1)
    grad_kv_own = grad_kv[reach] + carry.astype(F32)
    grad_key_own = grad_kv_own[:, : key_heads * head].reshape(part_len, key_heads, head)
    grad_value_low = grad_kv_own[:, key_heads * head :].astype(BF16)

    grad_query_scaled = rotate_back(grad_query.reshape(part_len, query_heads, head), cosine, sine)
    query_gain_part = gain_sum(grad_query_scaled, query_normed)
    grad_query_low = (
        norm_backward(grad_query_scaled, query_gain_f, query_normed, query_scale)
        .reshape(part_len, -1)
        .astype(BF16)
    )
    grad_key_scaled = rotate_back(grad_key_own, cosine, sine)
    key_gain_part = gain_sum(grad_key_scaled, key_normed)
    grad_key_low = (
        norm_backward(grad_key_scaled, key_gain_f, key_normed, key_scale)
        .reshape(part_len, -1)
        .astype(BF16)
    )
    grad_first = tensor_scatter(
        dot_nt(grad_query_low, query_weight)
        + dot_nt(grad_key_low, key_matrix)
        + dot_nt(grad_value_low, value_matrix)
    )
    qkv_slots = line_gather(jnp.concatenate([grad_query_low, grad_key_low, grad_value_low], axis=1))
    tokens_share = share_of(token_low).astype(F32)
    _, first_normed, first_scale = norm_forward(tokens_share, first_gain_f)
    token_grad = tensor_gather(
        (grad_resid + norm_backward(grad_first, first_gain_f, first_normed, first_scale)).astype(BF16)
    )
    first_gain_part = gain_sum(grad_first, first_normed)

    down_grad = slots_dot(hidden_slots, cot_slots)
    qkv_grad = slots_dot(x1_slots, qkv_slots)
    q_width, k_width = query_weight.shape[1], key_matrix.shape[1]
    gains = small_sum(jnp.concatenate([first_gain_part, second_gain_part, query_gain_part, key_gain_part]))
    return (
        outputs.reshape(tokens.shape),
        token_grad.reshape(tokens.shape),
        gains[:width],
        qkv_grad[:, :q_width],
        qkv_grad[:, q_width : q_width + k_width],
        qkv_grad[:, q_width + k_width :],
        gains[2 * width : 2 * width + head],
        gains[2 * width + head :],
        output_grad,
        gains[width : 2 * width],
        gate_grad,
        up_grad,
        down_grad,
    )


def solution(mesh):
    return jax.shard_map(
        per_device,
        mesh=mesh,
        in_specs=(
            P("dp", "ctx", None),
            P("dp", None),
            P(),
            P(None, "tensor"),
            P(None, "tensor"),
            P(None, "tensor"),
            P(),
            P(),
            P("tensor", None),
            P(),
            P(None, "tensor"),
            P(None, "tensor"),
            P("tensor", None),
            P("dp", "ctx", None),
        ),
        out_specs=(
            P("dp", "ctx", None),
            P("dp", "ctx", None),
            P(),
            P(("dp", "ctx"), "tensor"),
            P(("dp", "ctx"), "tensor"),
            P(("dp", "ctx"), "tensor"),
            P(),
            P(),
            P("tensor", ("dp", "ctx")),
            P(),
            P(("dp", "ctx"), "tensor"),
            P(("dp", "ctx"), "tensor"),
            P("tensor", ("dp", "ctx")),
        ),
        check_vma=False,
    )
```

```python
import functools
import math

import jax
import jax.numpy as jnp
from jax import lax
from jax.experimental import pallas as pl
from jax.experimental.pallas import tpu as pltpu
from jax.sharding import PartitionSpec as P

epsilon = 1e-06
rope_base = 1000000.0
F32 = jnp.float32
BF16 = jnp.bfloat16
MESH = pl.DeviceIdType.MESH
TILE = 256


def dot(a, b):
    return jnp.dot(a, b, preferred_element_type=F32)


def dot_nt(a, b):
    return lax.dot_general(a, b, (((1,), (1,)), ((), ())), preferred_element_type=F32)


def dot_tn(a, b):
    return lax.dot_general(a, b, (((0,), (0,)), ((), ())), preferred_element_type=F32)


def remote(src, dst, send_sem, recv_sem, **device):
    return pltpu.make_async_remote_copy(
        src_ref=src,
        dst_ref=dst,
        send_sem=send_sem,
        recv_sem=recv_sem,
        device_id=device,
        device_id_type=MESH,
    )


def tiles(total, size, body):
    size = min(size, total)

    def step(i, _):
        body(pl.multiple_of(i * size, size), size)
        return 0

    lax.fori_loop(0, total // size, step, 0)


class Dims:
    pass


def layer_kernel(
    dm,
    tok_hbm,
    cot_hbm,
    g1,
    g2,
    gq,
    gk,
    cos,
    sin,
    qseg,
    kseg,
    qw_hbm,
    kw_hbm,
    vw_hbm,
    ow_hbm,
    gw_hbm,
    uw_hbm,
    dw_hbm,
    out_hbm,
    tgrad_hbm,
    gate_out,
    up_out,
    outw_out,
    hid_all,
    qkv_all,
    x1t_all,
    cott_all,
    gains_out,
    s,
):
    T, D, H, QH, KH, F, n, nt, reach, S, R = (
        dm.T, dm.D, dm.H, dm.QH, dm.KH, dm.F, dm.n, dm.nt, dm.reach, dm.S, dm.R,
    )
    group = QH // KH
    span = (reach + 1) * T
    KV = KH * H
    inv_root = 1.0 / math.sqrt(H)
    dp, z, t = lax.axis_index("dp"), lax.axis_index("ctx"), lax.axis_index("tensor")
    zz = n - 1 - z

    barrier = pltpu.get_barrier_semaphore()
    for j in range(1, nt):
        pl.semaphore_signal(barrier, inc=1, device_id={"tensor": t ^ j}, device_id_type=MESH)
    for e in range(2):
        for d in range(n):
            if e or d:
                pl.semaphore_signal(
                    barrier,
                    inc=1,
                    device_id={"dp": dp ^ e, "ctx": lax.rem(z + d, n)},
                    device_id_type=MESH,
                )

    loads = [
        (tok_hbm, s.tok), (kw_hbm, s.kw), (vw_hbm, s.vw), (qw_hbm, s.qw), (cot_hbm, s.cot),
        (ow_hbm, s.ow), (dw_hbm, s.dw), (gw_hbm, s.gw), (uw_hbm, s.uw),
    ]
    loads = [pltpu.make_async_copy(a, b, s.load_sem.at[i]) for i, (a, b) in enumerate(loads)]
    for load in loads:
        load.start()
    (l_tok, l_kw, l_vw, l_qw, l_cot, l_ow, l_dw, l_gw, l_uw) = loads

    def scatter_start(k, buf, recv):
        for j in range(1, nt):
            peer = t ^ j
            remote(
                buf.at[pl.ds(pl.multiple_of(peer * S, S), S)], recv.at[j - 1],
                s.pl_s.at[k, j - 1], s.pl_r.at[k, j - 1], tensor=peer,
            ).start()

    def scatter_sum(k, buf, recv, base):
        mine = pl.ds(pl.multiple_of(t * S, S), S)
        for j in range(1, nt):
            remote(
                buf.at[mine], recv.at[j - 1], s.pl_s.at[k, j - 1], s.pl_r.at[k, j - 1], tensor=t ^ j
            ).wait()
        total = base + buf[mine, :].astype(F32)
        for j in range(1, nt):
            total = total + recv[j - 1].astype(F32)
        return total

    def gather_start(k, full):
        mine = pl.ds(pl.multiple_of(t * S, S), S)
        for j in range(1, nt):
            remote(
                full.at[mine], full.at[mine], s.pl_s.at[k, j - 1], s.pl_r.at[k, j - 1], tensor=t ^ j
            ).start()

    def gather_wait(k, full):
        mine = pl.ds(pl.multiple_of(t * S, S), S)
        for j in range(1, nt):
            peer = t ^ j
            theirs = pl.ds(pl.multiple_of(peer * S, S), S)
            copy = remote(
                full.at[mine], full.at[theirs], s.pl_s.at[k, j - 1], s.pl_r.at[k, j - 1], tensor=peer
            )
            copy.wait_send()
            copy.wait_recv()

    mine = pl.ds(pl.multiple_of(t * S, S), S)

    def spread_start(k, share, full, own):
        own_copy(share, full, own).start()
        for j in range(1, nt):
            remote(
                share, full.at[mine], s.pl_s.at[k, j - 1], s.pl_r.at[k, j - 1], tensor=t ^ j
            ).start()

    def own_copy(share, full, own):
        return pltpu.make_async_copy(share, full.at[mine], s.load_sem.at[own])

    def spread_wait(k, share, full, own):
        own_copy(share, full, own).wait()
        for j in range(1, nt):
            peer = t ^ j
            theirs = pl.ds(pl.multiple_of(peer * S, S), S)
            copy = remote(share, full.at[theirs], s.pl_s.at[k, j - 1], s.pl_r.at[k, j - 1], tensor=peer)
            copy.wait_send()
            copy.wait_recv()

    def line_copy(k, all_ref, up, step, src=None):
        idx = (z - step) if up else (z + step)
        ref = all_ref.at[dp, idx]
        return remote(
            ref if src is None else src, ref,
            s.ag_s.at[k, 0 if up else 1, step], s.ag_r.at[k, 0 if up else 1, step],
            ctx=(z + 1) if up else (z - 1),
        )

    def core_copy(k, all_ref, slot, idx, src=None):
        ref = all_ref.at[dp, idx]
        return remote(
            ref if src is None else src, ref, s.agx_s.at[k, slot], s.agx_r.at[k, slot], dp=1 - dp
        )

    def gather_line_start(k, src, all_ref):
        pltpu.make_async_copy(src, all_ref.at[dp, z], s.own_sem.at[k]).start()

        @pl.when(z < n - 1)
        def _():
            line_copy(k, all_ref, True, 0, src).start()

        @pl.when(z > 0)
        def _():
            line_copy(k, all_ref, False, 0, src).start()

        core_copy(k, all_ref, 0, z, src).start()

    def gather_line_step(k, all_ref, step):
        @pl.when(z >= step)
        def _():
            ref = all_ref.at[dp, z - step]
            remote(ref, ref, s.ag_s.at[k, 0, step - 1], s.ag_r.at[k, 0, step - 1], ctx=z - 1).wait_recv()
            if step < n - 1:

                @pl.when(z < n - 1)
                def _():
                    line_copy(k, all_ref, True, step).start()

            core_copy(k, all_ref, step, z - step).start()

        @pl.when(zz >= step)
        def _():
            ref = all_ref.at[dp, z + step]
            remote(ref, ref, s.ag_s.at[k, 1, step - 1], s.ag_r.at[k, 1, step - 1], ctx=z + 1).wait_recv()
            if step < n - 1:

                @pl.when(z > 0)
                def _():
                    line_copy(k, all_ref, False, step).start()

            core_copy(k, all_ref, n - 1 + step, z + step).start()

    def gather_line_finish(k, src, all_ref):
        pltpu.make_async_copy(src, all_ref.at[dp, z], s.own_sem.at[k]).wait()
        for step in range(n - 1):

            @pl.when((z >= step) & (z < n - 1))
            def _():
                line_copy(k, all_ref, True, step, src).wait_send()

            @pl.when((zz >= step) & (z > 0))
            def _():
                line_copy(k, all_ref, False, step, src).wait_send()

        def both(slot, idx):
            ref = all_ref.at[1 - dp, idx]
            copy = remote(src, ref, s.agx_s.at[k, slot], s.agx_r.at[k, slot], dp=1 - dp)
            copy.wait_send()
            copy.wait_recv()

        both(0, z)
        for step in range(1, n):

            @pl.when(z >= step)
            def _():
                both(step, z - step)

            @pl.when(zz >= step)
            def _():
                both(n - 1 + step, z + step)

    def columns_copy(k, src, all_ref, e, d):
        to_dp, to_z = dp ^ e, lax.rem(z + d, n)
        rows = pl.ds(pl.multiple_of((to_dp * n + to_z) * R, R), R)
        return remote(
            src.at[rows], all_ref.at[dp, z], s.aa_s.at[k, e * n + d], s.aa_r.at[k, e * n + d],
            dp=to_dp, ctx=to_z,
        )

    def columns_own(k, src, all_ref):
        rows = pl.ds(pl.multiple_of((dp * n + z) * R, R), R)
        return pltpu.make_async_copy(src.at[rows], all_ref.at[dp, z], s.aa_s.at[k, 0])

    def columns_start(k, src, all_ref):
        columns_own(k, src, all_ref).start()
        for d in range(n):
            for e in range(2):
                if e or d:
                    columns_copy(k, src, all_ref, e, d).start()

    def columns_wait_send(k, src, all_ref):
        columns_own(k, src, all_ref).wait()
        for e in range(2):
            for d in range(n):
                if e or d:
                    columns_copy(k, src, all_ref, e, d).wait_send()

    def columns_wait_recv(k, src, all_ref):
        for e in range(2):
            for d in range(n):
                if e or d:
                    ref = all_ref.at[dp ^ e, lax.rem(z - d + n, n)]
                    remote(
                        src.at[pl.ds(0, R)], ref, s.aa_s.at[k, e * n + d], s.aa_r.at[k, e * n + d], dp=dp ^ e
                    ).wait_recv()

    def job_dp_start(job, k, b):
        slot = job.dp_slot(b)

        def body(c, w):
            slot[:, pl.ds(c, w)] = job.part((1 - dp) * n + b, c, w).astype(BF16)

        tiles(job.cols, 512, body)
        remote(slot, job.dp_recv(b), s.dp_s.at[k, b], s.dp_r.at[k, b], dp=1 - dp).start()

    def job_dp_wait_send(job, k, b):
        remote(job.dp_slot(b), job.dp_recv(b), s.dp_s.at[k, b], s.dp_r.at[k, b], dp=1 - dp).wait_send()

    def job_dp_wait_all(job, k):
        for b in range(n):
            remote(job.dp_slot(b), job.dp_recv(b), s.dp_s.at[k, b], s.dp_r.at[k, b], dp=1 - dp).wait_recv()

    def chain_copy(job, k, up, step):
        i = 0 if up else 1
        return remote(
            job.chain_slot(up, step), job.chain(up, step), s.ch_s.at[k, i, step], s.ch_r.at[k, i, step],
            ctx=(z + 1) if up else (z - 1),
        )

    def chain_step(job, k, step):
        for up in (True, False):
            pos = z if up else zz

            @pl.when((pos <= step) & (pos < n - 1))
            def _(up=up, pos=pos):
                target = (z + n - 1 - step) if up else (z - (n - 1 - step))
                slot = job.chain_slot(up, step)
                if step:

                    @pl.when(pos >= 1)
                    def _():
                        chain_copy(job, k, up, step - 1).wait_recv()

                def body(c, w):
                    cs = pl.ds(c, w)
                    total = job.part(dp * n + target, c, w) + job.dp_recv(target)[:, cs].astype(F32)
                    if step:
                        prev = job.chain(up, step - 1)[:, cs].astype(F32)
                        total = total + jnp.where(pos >= 1, prev, 0.0)
                    slot[:, cs] = total.astype(BF16)

                tiles(job.cols, 512, body)
                chain_copy(job, k, up, step).start()

    def chain_wait_send(job, k, step):
        for up in (True, False):
            pos = z if up else zz

            @pl.when((pos <= step) & (pos < n - 1))
            def _(up=up):
                chain_copy(job, k, up, step).wait_send()

    def chain_final(job, k, out_ref):
        for up in (True, False):
            pos = z if up else zz

            @pl.when(pos >= 1)
            def _(up=up):
                chain_copy(job, k, up, n - 2).wait_recv()

        def body(c, w):
            cs = pl.ds(c, w)
            total = job.part(dp * n + z, c, w) + job.dp_recv(z)[:, cs].astype(F32)
            a = job.chain(True, n - 2)[:, cs].astype(F32)
            b = job.chain(False, n - 2)[:, cs].astype(F32)
            out_ref[:, cs] = total + jnp.where(z >= 1, a, 0.0) + jnp.where(zz >= 1, b, 0.0)

        tiles(job.cols, 512, body)

    l_tok.wait()
    x = s.tok[...].astype(F32)
    scale = lax.rsqrt(jnp.mean(x * x, axis=-1, keepdims=True) + epsilon)
    s.x1[...] = (x * scale * g1[...]).astype(BF16)
    s.tokshare[...] = s.tok[mine, :].astype(F32)

    def rms(v):
        return lax.rsqrt(jnp.mean(v * v, axis=-1, keepdims=True) + epsilon)

    def rope(v):
        return v * cos[...] + pltpu.roll(v, H // 2, 1) * sin[...]

    def rope_back(g):
        return g * cos[...] + pltpu.roll(g * sin[...], H // 2, 1)

    own_rows = pl.ds(reach * T, T)
    l_kw.wait()
    l_vw.wait()
    s.k_raw[...] = dot(s.x1[...], s.kw[...])
    s.kv[own_rows, KV : 2 * KV] = dot(s.x1[...], s.vw[...]).astype(BF16)
    for h in range(KH):
        raw = s.k_raw[:, h * H : (h + 1) * H]
        s.kv[own_rows, h * H : (h + 1) * H] = rope(raw * rms(raw) * gk[...]).astype(BF16)
    pl.semaphore_wait(barrier, (nt - 1) + (2 * n - 1))

    def kv_copy(r):
        return remote(
            s.kv.at[pl.ds((reach - r + 1) * T, T)], s.kv.at[pl.ds((reach - r) * T, T)],
            s.kv_s.at[r - 1], s.kv_r.at[r - 1], ctx=z + 1,
        )

    def kv_send(r):
        @pl.when((z < n - 1) & (z >= r - 1))
        def _():
            kv_copy(r).start()

    kv_send(1)
    for r in range(1, reach + 1):

        @pl.when(z < r)
        def _():
            s.kv[pl.ds((reach - r) * T, T), :] = jnp.zeros((T, 2 * KV), BF16)

    l_qw.wait()
    s.q_raw[...] = dot(s.x1[...], s.qw[...])
    for h in range(QH):
        raw = s.q_raw[:, h * H : (h + 1) * H]
        s.q_rot[:, h * H : (h + 1) * H] = rope(raw * rms(raw) * gq[...]).astype(BF16)
    for r in range(1, reach + 1):

        @pl.when(z >= r)
        def _():
            kv_copy(r).wait_recv()

        if r < reach:
            kv_send(r + 1)
    rows_i = lax.broadcasted_iota(jnp.int32, (T, span), 0) + reach * T
    cols_i = lax.broadcasted_iota(jnp.int32, (T, span), 1)
    allowed = (cols_i <= rows_i) & (qseg[...] == kseg[...])
    s.mask[...] = jnp.where(allowed, 1.0, 0.0).astype(F32)

    def weights_of(h, g):
        hs = pl.ds(pl.multiple_of(h * H, H), H)
        q = s.q_rot[:, hs]
        k = s.kv[:, pl.ds(pl.multiple_of(g * H, H), H)]
        return q, k, jnp.where(s.mask[...] > 0.0, jnp.exp(dot_nt(q, k) * inv_root), 0.0)

    def attend(h, _):
        g = h // group
        hs = pl.ds(pl.multiple_of(h * H, H), H)
        _q, _k, w = weights_of(h, g)
        v = s.kv[:, pl.ds(pl.multiple_of(KV + g * H, H), H)]
        total = jnp.sum(w, axis=-1, keepdims=True)
        att = dot(w.astype(BF16), v) / total
        s.tot[:, hs] = jnp.broadcast_to(total, (T, H))
        s.att[:, hs] = att
        s.att_low[:, hs] = att.astype(BF16)
        return 0

    lax.fori_loop(0, QH, attend, 0)

    l_ow.wait()

    def body(c, w):
        s.send_a[:, pl.ds(c, w)] = dot(s.att_low[...], s.ow[:, pl.ds(c, w)]).astype(BF16)

    tiles(D, TILE, body)
    scatter_start(0, s.send_a, s.recv0)

    l_cot.wait()
    s.cotshare[...] = s.cot[mine, :].astype(F32)

    def body(c, w):
        s.xt[pl.ds(c, w), :] = s.x1[:, pl.ds(c, w)].astype(F32).T.astype(BF16)
        s.cott[pl.ds(c, w), :] = s.cot[:, pl.ds(c, w)].astype(F32).T.astype(BF16)

    tiles(D, TILE, body)
    columns_start(0, s.cott, cott_all)
    columns_start(1, s.xt, x1t_all)
    l_dw.wait()

    def body(c, w):
        s.gh[:, pl.ds(c, w)] = dot_nt(s.cot[...], s.dw[pl.ds(c, w), :])

    tiles(F, TILE, body)
    for h in range(QH):
        s.attt[h * H : (h + 1) * H, :] = s.att[:, h * H : (h + 1) * H].T.astype(BF16)

    s.resid[...] = scatter_sum(0, s.send_a, s.recv0, s.tokshare[...])
    resid = s.resid[...]
    s.x2[mine, :] = (resid * rms(resid) * g2[...]).astype(BF16)
    gather_start(1, s.x2)
    l_gw.wait()
    l_uw.wait()
    gather_wait(1, s.x2)

    def body(c, w):
        cs = pl.ds(c, w)
        gate = dot(s.x2[...], s.gw[:, cs])
        up = dot(s.x2[...], s.uw[:, cs])
        gh = s.gh[:, cs]
        sig = jax.nn.sigmoid(gate)
        act = gate * sig
        s.hid[:, cs] = (act * up).astype(BF16)
        s.gg[:, cs] = (gh * up * (sig * (1.0 + gate * (1.0 - sig)))).astype(BF16)
        s.gu[:, cs] = (gh * act).astype(BF16)

    tiles(F, TILE, body)
    gather_line_start(0, s.hid, hid_all)

    def body(c, w):
        rs = pl.ds(c, w)
        s.send_a[:, rs] = (
            dot_nt(s.gg[...], s.gw[rs, :]) + dot_nt(s.gu[...], s.uw[rs, :])
        ).astype(BF16)

    tiles(D, TILE, body)
    scatter_start(2, s.send_a, s.recv1)
    pl.semaphore_signal(s.credit, inc=1, device_id={"dp": 1 - dp}, device_id_type=MESH)

    columns_wait_send(1, s.xt, x1t_all)

    def body(c, w):
        s.xt[pl.ds(c, w), :] = s.x2[:, pl.ds(c, w)].astype(F32).T.astype(BF16)

    tiles(D, TILE, body)

    class WeightJob:
        def __init__(self, k, grad):
            self.k, self.grad, self.cols = k, grad, F

        def part(self, block, c, w):
            rows = pl.ds(pl.multiple_of(block * R, R), R)
            return dot(s.xt[rows, :], self.grad[:, pl.ds(c, w)])

        def dp_slot(self, b):
            return s.gw.at[pl.ds(b * R, R)]

        def dp_recv(self, b):
            return s.uw.at[pl.ds(pl.multiple_of((self.k * n + b) * R, R), R)]

        def chain_slot(self, up, step):
            i = (0 if self.k else n) + (step if up else n - 2 - step)
            return s.gw.at[pl.ds(i * R, R)]

        def chain(self, up, step):
            return s.chain.at[self.k, 0 if up else 1, step]

    class OutJob:
        cols = R

        def part(self, block, c, w):
            cs = pl.ds(pl.multiple_of(block * R + c, 128), w)
            return dot(s.attt[...], s.gm[:, cs])

        def dp_slot(self, b):
            return s.cott.at[pl.ds(b * QH * H, QH * H), pl.ds(0, R)]

        def dp_recv(self, b):
            return s.o_recv.at[b]

        def chain_slot(self, up, step):
            return s.o_csend.at[step if up else n - 2 - step]

        def chain(self, up, step):
            return s.o_chain.at[0 if up else 1, step]

    gate_job, up_job, out_job = WeightJob(0, s.gg), WeightJob(1, s.gu), OutJob()
    order = [b for i in range((n + 1) // 2) for b in dict.fromkeys((n - 1 - i, i))]

    pl.semaphore_wait(s.credit, 1)
    for b in order:
        job_dp_start(gate_job, 0, b)

    def body(c, w):
        s.send_b[:, pl.ds(c, w)] = dot(s.hid[...], s.dw[:, pl.ds(c, w)]).astype(BF16)

    tiles(D, TILE, body)
    scatter_start(3, s.send_b, s.recv2)
    for b in order:
        job_dp_wait_send(gate_job, 0, b)
        job_dp_start(up_job, 1, b)
    gather_line_step(0, hid_all, 1)

    grad_second = scatter_sum(2, s.send_a, s.recv1, jnp.zeros((S, D), F32))
    resid = s.resid[...]
    scale = rms(resid)
    normed = resid * scale
    s.gains[:, D : 2 * D] = jnp.sum(grad_second * normed, axis=0, keepdims=True)
    scaled = grad_second * g2[...]
    inner = jnp.mean(scaled * normed, axis=-1, keepdims=True)
    s.gresid[...] = s.cotshare[...] + scale * (scaled - normed * inner)
    s.gm[mine, :] = s.gresid[...].astype(BF16)
    gather_start(4, s.gm)
    job_dp_wait_all(gate_job, 0)
    chain_step(gate_job, 0, 0)
    s.outsh[...] = scatter_sum(3, s.send_b, s.recv2, s.resid[...]).astype(BF16)
    gather_wait(4, s.gm)
    spread_start(5, s.outsh, out_hbm, 0)

    def body(c, w):
        s.gatt[:, pl.ds(c, w)] = dot_nt(s.gm[...], s.ow[pl.ds(c, w), :])

    tiles(QH * H, TILE, body)
    s.gq_acc[...] = jnp.zeros((1, H), F32)

    def back(g, _):
        ks = pl.ds(pl.multiple_of(g * H, H), H)
        vs = pl.ds(pl.multiple_of(KV + g * H, H), H)
        v = s.kv[:, vs]
        grad_k = jnp.zeros((span, H), F32)
        grad_v = jnp.zeros((span, H), F32)
        for i in range(group):
            h = g * group + i
            hs = pl.ds(pl.multiple_of(h * H, H), H)
            q, k, w = weights_of(h, g)
            ga, total = s.gatt[:, hs], s.tot[:, hs]
            gs = (ga / total).astype(BF16)
            delta = jnp.sum(ga * s.att[:, hs], axis=-1, keepdims=True) / total[:, :1]
            ds = (w * (dot_nt(gs, v) - delta)).astype(BF16)
            grad_k = grad_k + dot_tn(ds, q) * inv_root
            grad_v = grad_v + dot_tn(w.astype(BF16), gs)
            gr = rope_back(dot(ds, k) * inv_root)
            raw = s.q_raw[:, hs]
            r = rms(raw)
            nq = raw * r
            s.gq_acc[...] += jnp.sum(gr * nq, axis=0, keepdims=True)
            sc = gr * gq[...]
            s.dqkv[:, hs] = (r * (sc - nq * jnp.mean(sc * nq, axis=-1, keepdims=True))).astype(BF16)
        s.dkv[:, ks] = grad_k.astype(BF16)
        s.dkv[:, vs] = grad_v.astype(BF16)
        return 0

    lax.fori_loop(0, KH, back, 0)
    s.gains[:, 2 * D : 2 * D + H] = s.gq_acc[...]

    def dkv_copy(i):
        return remote(
            s.dkv.at[pl.ds(i * T, T)], s.dkv_in.at[i], s.dkv_s.at[i], s.dkv_r.at[i], ctx=z - 1
        )

    for i in range(reach):
        if i:

            @pl.when((z < n - 1) & (z + 1 >= reach - i + 1))
            def _():
                dkv_copy(i - 1).wait_recv()
                rows = pl.ds(i * T, T)
                s.dkv[rows, :] = (s.dkv[rows, :].astype(F32) + s.dkv_in[i - 1].astype(F32)).astype(BF16)

        @pl.when(z >= reach - i)
        def _():
            dkv_copy(i).start()

        if i == 0:
            job_dp_wait_all(up_job, 1)
            gather_line_step(0, hid_all, 2)
            columns_wait_send(0, s.cott, cott_all)
            for b in order:
                job_dp_start(out_job, 2, b)
            for b in order:
                job_dp_wait_send(up_job, 1, b)
            chain_step(gate_job, 0, 1)

    def last_block():
        rows = pl.ds(reach * T, T)
        own = s.dkv[rows, :].astype(F32)
        extra = s.dkv_in[reach - 1].astype(F32)
        return own + jnp.where(z < n - 1, extra, 0.0)

    @pl.when(z < n - 1)
    def _():
        dkv_copy(reach - 1).wait_recv()

    own = last_block()
    s.dqkv[:, QH * H + KV :] = own[:, KV:].astype(BF16)
    gk_sum = jnp.zeros((1, H), F32)
    for h in range(KH):
        gr = rope_back(own[:, h * H : (h + 1) * H])
        raw = s.k_raw[:, h * H : (h + 1) * H]
        r = rms(raw)
        nk = raw * r
        gk_sum = gk_sum + jnp.sum(gr * nk, axis=0, keepdims=True)
        sc = gr * gk[...]
        s.dqkv[:, QH * H + h * H : QH * H + (h + 1) * H] = (
            r * (sc - nk * jnp.mean(sc * nk, axis=-1, keepdims=True))
        ).astype(BF16)
    s.gains[:, 2 * D + H :] = gk_sum
    gather_line_start(1, s.dqkv, qkv_all)

    q_c, k_c, v_c = pl.ds(0, QH * H), pl.ds(QH * H, KV), pl.ds(QH * H + KV, KV)

    def body(c, w):
        rs = pl.ds(c, w)
        s.send_a[:, rs] = (
            dot_nt(s.dqkv[:, q_c], s.qw[rs, :])
            + dot_nt(s.dqkv[:, k_c], s.kw[rs, :])
            + dot_nt(s.dqkv[:, v_c], s.vw[rs, :])
        ).astype(BF16)

    tiles(D, TILE, body)
    scatter_start(6, s.send_a, s.recv3)
    job_dp_wait_all(out_job, 2)
    chain_step(out_job, 2, 0)
    chain_step(gate_job, 0, 2)
    grad_first = scatter_sum(6, s.send_a, s.recv3, jnp.zeros((S, D), F32))
    tokshare = s.tokshare[...]
    scale = rms(tokshare)
    normed = tokshare * scale
    s.gains[:, :D] = jnp.sum(grad_first * normed, axis=0, keepdims=True)
    scaled = grad_first * g1[...]
    inner = jnp.mean(scaled * normed, axis=-1, keepdims=True)
    s.tgsh[...] = (s.gresid[...] + scale * (scaled - normed * inner)).astype(BF16)
    spread_start(7, s.tgsh, tgrad_hbm, 1)
    for j in range(1, nt):
        remote(s.gains, s.gains_p.at[j - 1], s.pl_s.at[8, j - 1], s.pl_r.at[8, j - 1], tensor=t ^ j).start()
    for step in range(3, n):
        gather_line_step(0, hid_all, step)
    for step in range(3, n - 1):
        chain_step(gate_job, 0, step)
    chain_step(up_job, 1, 0)
    for j in range(1, nt):
        remote(s.gains, s.gains_p.at[j - 1], s.pl_s.at[8, j - 1], s.pl_r.at[8, j - 1], tensor=t ^ j).wait()
    total = s.gains[...]
    for j in range(1, nt):
        total = total + s.gains_p[j - 1]
    s.gains2[...] = total

    def gain_copy(e, d):
        i = e * n + d
        return remote(
            s.gains2, s.gains_x.at[i - 1], s.ga_s.at[i], s.ga_r.at[i], dp=dp ^ e, ctx=lax.rem(z + d, n)
        )

    for e in range(2):
        for d in range(n):
            if e or d:
                gain_copy(e, d).start()
    for step in range(1, n - 1):
        gather_line_step(1, qkv_all, step)
        chain_step(out_job, 2, step)
        chain_step(up_job, 1, step)
    def gate_copy():
        return pltpu.make_async_copy(s.gh.at[pl.ds(0, R)], gate_out, s.load_sem.at[2])

    def up_copy():
        return pltpu.make_async_copy(s.gh.at[pl.ds(0, R)], up_out, s.load_sem.at[3])

    chain_final(gate_job, 0, s.gh.at[pl.ds(0, R)])
    gate_copy().start()
    chain_final(out_job, 2, outw_out)
    gather_line_step(1, qkv_all, n - 1)
    gate_copy().wait()
    chain_final(up_job, 1, s.gh.at[pl.ds(0, R)])
    up_copy().start()
    for e in range(2):
        for d in range(n):
            if e or d:
                gain_copy(e, d).wait()
    total = s.gains2[...]
    for i in range(2 * n - 1):
        total = total + s.gains_x[i]
    gains_out[...] = total

    gather_line_finish(0, s.hid, hid_all)
    gather_line_finish(1, s.dqkv, qkv_all)
    columns_wait_recv(0, s.cott, cott_all)
    columns_wait_recv(1, s.xt, x1t_all)
    for b in range(n):
        job_dp_wait_send(out_job, 2, b)
    for st in range(n - 1):
        chain_wait_send(gate_job, 0, st)
        chain_wait_send(up_job, 1, st)
        chain_wait_send(out_job, 2, st)
    for r in range(1, reach + 1):

        @pl.when((z < n - 1) & (z >= r - 1))
        def _():
            kv_copy(r).wait_send()

    for i in range(reach):

        @pl.when(z >= reach - i)
        def _():
            dkv_copy(i).wait_send()

    spread_wait(5, s.outsh, out_hbm, 0)
    spread_wait(7, s.tgsh, tgrad_hbm, 1)
    up_copy().wait()


def run_layer(dm, *operands):
    T, D, H, F, n, nt, reach, S, R = dm.T, dm.D, dm.H, dm.F, dm.n, dm.nt, dm.reach, dm.S, dm.R
    QC, KV = dm.QH * H, dm.KH * H
    span = (reach + 1) * T
    G = 2 * D + 2 * H
    dma = pltpu.SemaphoreType.DMA
    scratch = dict(
        tok=((T, D), BF16), x1=((T, D), BF16), cot=((T, D), BF16), x2=((T, D), BF16), gm=((T, D), BF16),
        outsh=((S, D), BF16), tgsh=((S, D), BF16), xt=((D, T), BF16), cott=((D, T), BF16),
        qw=((D, QC), BF16), kw=((D, KV), BF16), vw=((D, KV), BF16), ow=((QC, D), BF16),
        gw=((D, F), BF16), uw=((D, F), BF16), dw=((F, D), BF16),
        tokshare=((S, D), F32), cotshare=((S, D), F32), resid=((S, D), F32), gresid=((S, D), F32),
        k_raw=((T, KV), F32), q_raw=((T, QC), F32), q_rot=((T, QC), BF16), kv=((span, 2 * KV), BF16),
        mask=((T, span), F32), tot=((T, QC), F32), att=((T, QC), F32), att_low=((T, QC), BF16),
        attt=((QC, T), BF16), gatt=((T, QC), F32), gq_acc=((1, H), F32),
        recv0=((nt - 1, S, D), BF16), recv1=((nt - 1, S, D), BF16),
        gh=((T, F), F32), hid=((T, F), BF16), gg=((T, F), BF16), gu=((T, F), BF16),
        dkv=((span, 2 * KV), BF16), dkv_in=((reach, T, 2 * KV), BF16), dqkv=((T, QC + 2 * KV), BF16),
        chain=((2, 2, n - 1, R, F), BF16),
        o_recv=((n, QC, R), BF16), o_csend=((n - 1, QC, R), BF16),
        o_chain=((2, n - 1, QC, R), BF16),
        gains=((1, G), F32), gains2=((1, G), F32), gains_p=((nt - 1, 1, G), F32),
        gains_x=((2 * n - 1, 1, G), F32),
    )
    sems = dict(
        load_sem=(9,), own_sem=(2,), pl_s=(9, nt - 1), pl_r=(9, nt - 1), ag_s=(2, 2, n - 1), ag_r=(2, 2, n - 1),
        agx_s=(2, 2 * n - 1), agx_r=(2, 2 * n - 1), aa_s=(2, 2 * n), aa_r=(2, 2 * n),
        dp_s=(3, n), dp_r=(3, n), ch_s=(3, 2, n - 1), ch_r=(3, 2, n - 1), kv_s=(reach,), kv_r=(reach,),
        dkv_s=(reach,), dkv_r=(reach,), ga_s=(2 * n,), ga_r=(2 * n,),
    )
    names = list(scratch) + list(sems) + ["credit"]
    shapes = [pltpu.VMEM(*v) for v in scratch.values()] + [dma(v) for v in sems.values()]
    shapes.append(pltpu.SemaphoreType.REGULAR)

    def body(*refs):
        fixed = len(refs) - len(names)
        s = Dims()
        for name, ref in zip(names, refs[fixed:]):
            setattr(s, name, ref)
        for alias, of in dm.alias.items():
            setattr(s, alias, getattr(s, of))
        layer_kernel(dm, *refs[:fixed], s)

    hbm = pl.BlockSpec(memory_space=pl.ANY)
    vmem = pl.BlockSpec(memory_space=pltpu.VMEM)
    return pl.pallas_call(
        body,
        out_shape=(
            jax.ShapeDtypeStruct((T, D), BF16),
            jax.ShapeDtypeStruct((T, D), BF16),
            jax.ShapeDtypeStruct((R, F), F32),
            jax.ShapeDtypeStruct((R, F), F32),
            jax.ShapeDtypeStruct((QC, R), F32),
            jax.ShapeDtypeStruct((2, n, T, F), BF16),
            jax.ShapeDtypeStruct((2, n, T, QC + 2 * KV), BF16),
            jax.ShapeDtypeStruct((2, n, R, T), BF16),
            jax.ShapeDtypeStruct((2, n, R, T), BF16),
            jax.ShapeDtypeStruct((1, G), F32),
        ),
        in_specs=[hbm] * 2 + [vmem] * 8 + [hbm] * 7,
        out_specs=[hbm] * 4 + [vmem] + [hbm] * 4 + [vmem],
        scratch_shapes=shapes,
        compiler_params=pltpu.CompilerParams(
            collective_id=0, has_side_effects=True, vmem_limit_bytes=67043328
        ),
        name="layer",
    )(*operands)


def per_device(
    tokens,
    segments,
    first_gain,
    query_weight,
    key_matrix,
    value_matrix,
    query_norm_gain,
    key_gain,
    output_weight,
    second_gain,
    gate_weight,
    up_weight,
    down_weight,
    cotangent,
):
    _, T, D = tokens.shape
    dm = Dims()
    dm.T, dm.D, dm.H, dm.F = T, D, query_norm_gain.shape[0], gate_weight.shape[1]
    dm.QH, dm.KH = query_weight.shape[1] // dm.H, key_matrix.shape[1] // dm.H
    dm.n, dm.nt = lax.axis_size("ctx"), lax.axis_size("tensor")
    length = segments.shape[1]
    dm.reach = -(-(length // 2 - 1) // T)
    dm.S, dm.R = T // dm.nt, D // (2 * dm.n)
    dm.alias = {"send_b": "x1", "send_a": "tok", "recv2": "recv0", "recv3": "recv1"}
    H = dm.H
    start = lax.axis_index("ctx") * T
    row = segments[0]
    mine = lax.dynamic_slice_in_dim(row, start, T, 0)
    begins = jnp.sum((row[None, :] < mine[:, None]).astype(jnp.int32), axis=1)
    position = (start + jnp.arange(T, dtype=jnp.int32) - begins).astype(F32)
    inverse = 1.0 / rope_base ** (jnp.arange(0, H, 2, dtype=F32) / H)
    angles = position[:, None] * inverse[None, :]
    cosine, sine = jnp.cos(angles), jnp.sin(angles)
    cosine = jnp.concatenate([cosine, cosine], axis=-1)
    sine = jnp.concatenate([-sine, sine], axis=-1)
    padded = jnp.concatenate([jnp.full((dm.reach * T,), -1, jnp.int32), row])
    keys = lax.dynamic_slice_in_dim(padded, start, (dm.reach + 1) * T, 0)

    out, tgrad, gate_g, up_g, out_g, hid, qkv, x1t, cott, gains = run_layer(
        dm,
        tokens.reshape(T, D),
        cotangent.reshape(T, D),
        first_gain.astype(F32)[None],
        second_gain.astype(F32)[None],
        query_norm_gain.astype(F32)[None],
        key_gain.astype(F32)[None],
        cosine,
        sine,
        mine[:, None],
        keys[None],
        query_weight,
        key_matrix,
        value_matrix,
        output_weight,
        gate_weight,
        up_weight,
        down_weight,
    )

    down_g = jnp.einsum("abtf,abct->fc", hid, cott, preferred_element_type=F32)
    qkv_g = jnp.einsum("abct,abtm->cm", x1t, qkv, preferred_element_type=F32)
    QC, KV = dm.QH * H, dm.KH * H
    gains = gains[0]
    return (
        out.reshape(tokens.shape),
        tgrad.reshape(tokens.shape),
        gains[:D],
        qkv_g[:, :QC],
        qkv_g[:, QC : QC + KV],
        qkv_g[:, QC + KV :],
        gains[2 * D : 2 * D + H],
        gains[2 * D + H :],
        out_g,
        gains[D : 2 * D],
        gate_g,
        up_g,
        down_g,
    )


def solution(mesh):
    return jax.shard_map(
        per_device,
        mesh=mesh,
        in_specs=(
            P("dp", "ctx", None),
            P("dp", None),
            P(),
            P(None, "tensor"),
            P(None, "tensor"),
            P(None, "tensor"),
            P(),
            P(),
            P("tensor", None),
            P(),
            P(None, "tensor"),
            P(None, "tensor"),
            P("tensor", None),
            P("dp", "ctx", None),
        ),
        out_specs=(
            P("dp", "ctx", None),
            P("dp", "ctx", None),
            P(),
            P(("dp", "ctx"), "tensor"),
            P(("dp", "ctx"), "tensor"),
            P(("dp", "ctx"), "tensor"),
            P(),
            P(),
            P("tensor", ("dp", "ctx")),
            P(),
            P(("dp", "ctx"), "tensor"),
            P(("dp", "ctx"), "tensor"),
            P("tensor", ("dp", "ctx")),
        ),
        check_vma=False,
    )
```

```python
import functools
import math

import jax
import jax.numpy as jnp
import numpy as np
from jax import lax
from jax.experimental import pallas as pl
from jax.experimental.pallas import tpu as pltpu
from jax.sharding import PartitionSpec as P

epsilon = 1e-06
rope_base = 1000000.0
F32 = jnp.float32
BF16 = jnp.bfloat16
MESH = pl.DeviceIdType.MESH
TILE = 256


def dot(a, b):
    return jnp.dot(a, b, preferred_element_type=F32)


def dot_nt(a, b):
    return lax.dot_general(a, b, (((1,), (1,)), ((), ())), preferred_element_type=F32)


def dot_tn(a, b):
    return lax.dot_general(a, b, (((0,), (0,)), ((), ())), preferred_element_type=F32)


def remote(src, dst, send_sem, recv_sem, **device):
    return pltpu.make_async_remote_copy(
        src_ref=src,
        dst_ref=dst,
        send_sem=send_sem,
        recv_sem=recv_sem,
        device_id=device,
        device_id_type=MESH,
    )


def tiles(total, size, body):
    size = min(size, total)

    def step(i, _):
        body(pl.multiple_of(i * size, size), size)
        return 0

    lax.fori_loop(0, total // size, step, 0)


class Dims:
    pass


def layer_kernel(
    dm,
    tok_hbm,
    cot_hbm,
    gain_in,
    inverse,
    seg_row,
    qw_hbm,
    kw_hbm,
    vw_hbm,
    ow_hbm,
    gw_hbm,
    uw_hbm,
    dw_hbm,
    out_hbm,
    tgrad_hbm,
    gate_out,
    up_out,
    down_out,
    q_out,
    k_out,
    v_out,
    outw_out,
    gains_out,
    att_all,
    s,
):
    T, D, H, QH, KH, F, n, nt, reach, S, R = (
        dm.T, dm.D, dm.H, dm.QH, dm.KH, dm.F, dm.n, dm.nt, dm.reach, dm.S, dm.R,
    )
    group = QH // KH
    span = (reach + 1) * T
    KV = KH * H
    inv_root = 1.0 / math.sqrt(H)
    C = R // nt
    g1 = gain_in.at[:, pl.ds(0, D)]
    g2 = gain_in.at[:, pl.ds(D, D)]
    gq = gain_in.at[:, pl.ds(2 * D, H)]
    gk = gain_in.at[:, pl.ds(2 * D + H, H)]
    cos, sin = s.cos, s.sin
    dp, z, t = lax.axis_index("dp"), lax.axis_index("ctx"), lax.axis_index("tensor")
    zz = n - 1 - z
    nl = n // 2
    zh, zl = z // nl, lax.rem(z, nl)
    zzl = nl - 1 - zl

    barrier = pltpu.get_barrier_semaphore()
    for j in range(1, nt):
        pl.semaphore_signal(barrier, inc=1, device_id={"tensor": t ^ j}, device_id_type=MESH)
    for e in range(2):
        for d in range(n):
            if e or d:
                pl.semaphore_signal(
                    barrier,
                    inc=1,
                    device_id={"dp": dp ^ e, "ctx": lax.rem(z + d, n)},
                    device_id_type=MESH,
                )

    loads = [
        (tok_hbm, s.tok), (cot_hbm, s.cot), (kw_hbm, s.kw), (vw_hbm, s.vw), (qw_hbm, s.qw),
        (ow_hbm, s.ow), (dw_hbm, s.dw), (gw_hbm, s.gw), (uw_hbm, s.uw),
    ]
    loads = [pltpu.make_async_copy(a, b, s.load_sem.at[i]) for i, (a, b) in enumerate(loads)]
    for load in loads:
        load.start()
    (l_tok, l_cot, l_kw, l_vw, l_qw, l_ow, l_dw, l_gw, l_uw) = loads

    def scatter_start(k, buf, recv):
        for j in range(1, nt):
            peer = t ^ j
            remote(
                buf.at[pl.ds(pl.multiple_of(peer * S, S), S)], recv.at[j - 1],
                s.pl_s.at[k, j - 1], s.pl_r.at[k, j - 1], tensor=peer,
            ).start()

    def scatter_sum(k, buf, recv, base):
        mine = pl.ds(pl.multiple_of(t * S, S), S)
        for j in range(1, nt):
            remote(
                buf.at[mine], recv.at[j - 1], s.pl_s.at[k, j - 1], s.pl_r.at[k, j - 1], tensor=t ^ j
            ).wait()
        total = base + buf[mine, :].astype(F32)
        for j in range(1, nt):
            total = total + recv[j - 1].astype(F32)
        return total

    def gather_start(k, full):
        mine = pl.ds(pl.multiple_of(t * S, S), S)
        for j in range(1, nt):
            remote(
                full.at[mine], full.at[mine], s.pl_s.at[k, j - 1], s.pl_r.at[k, j - 1], tensor=t ^ j
            ).start()

    def gather_wait(k, full):
        mine = pl.ds(pl.multiple_of(t * S, S), S)
        for j in range(1, nt):
            peer = t ^ j
            theirs = pl.ds(pl.multiple_of(peer * S, S), S)
            copy = remote(
                full.at[mine], full.at[theirs], s.pl_s.at[k, j - 1], s.pl_r.at[k, j - 1], tensor=peer
            )
            copy.wait_send()
            copy.wait_recv()

    mine = pl.ds(pl.multiple_of(t * S, S), S)

    def spread_start(k, share, full, own):
        own_copy(share, full, own).start()
        for j in range(1, nt):
            remote(
                share, full.at[mine], s.pl_s.at[k, j - 1], s.pl_r.at[k, j - 1], tensor=t ^ j
            ).start()

    def own_copy(share, full, own):
        return pltpu.make_async_copy(share, full.at[mine], s.load_sem.at[own])

    def spread_wait(k, share, full, own):
        own_copy(share, full, own).wait()
        for j in range(1, nt):
            peer = t ^ j
            theirs = pl.ds(pl.multiple_of(peer * S, S), S)
            copy = remote(share, full.at[theirs], s.pl_s.at[k, j - 1], s.pl_r.at[k, j - 1], tensor=peer)
            copy.wait_send()
            copy.wait_recv()

    def mirror(i, src, dst):
        return remote(src.at[mine], dst.at[mine], s.mi_s.at[i], s.mi_r.at[i], ctx=zz)

    def mirror_x1(d):
        cols = pl.ds(pl.multiple_of((d * n + (1 - zh) * nl) * R, 128), nl * R)
        return remote(
            s.x1.at[:, cols], s.x1b.at[:, pl.ds(d * nl * R, nl * R)], s.mi_s.at[2 + d], s.mi_r.at[2 + d], ctx=zz
        )

    def mirror_qkv():
        return remote(
            s.dqkv.at[pl.ds(0, T)], s.dqkv.at[pl.ds(T, T)], s.mi_s.at[4], s.mi_r.at[4], ctx=zz
        )

    def line_copy(k, all_ref, up, step, src=None):
        idx = (z - step) if up else (z + step)
        ref = all_ref.at[dp, idx]
        return remote(
            ref if src is None else src, ref,
            s.ag_s.at[k, 0 if up else 1, step], s.ag_r.at[k, 0 if up else 1, step],
            ctx=(z + 1) if up else (z - 1),
        )

    def core_copy(k, all_ref, slot, idx, src=None):
        ref = all_ref.at[dp, idx]
        return remote(
            ref if src is None else src, ref, s.agx_s.at[k, slot], s.agx_r.at[k, slot], dp=1 - dp
        )

    def gather_line_start(k, src, all_ref):
        pltpu.make_async_copy(src, all_ref.at[dp, z], s.own_sem.at[k]).start()

        @pl.when(z < n - 1)
        def _():
            line_copy(k, all_ref, True, 0, src).start()

        @pl.when(z > 0)
        def _():
            line_copy(k, all_ref, False, 0, src).start()

        core_copy(k, all_ref, 0, z, src).start()

    def gather_line_step(k, all_ref, step):
        @pl.when(z >= step)
        def _():
            ref = all_ref.at[dp, z - step]
            remote(ref, ref, s.ag_s.at[k, 0, step - 1], s.ag_r.at[k, 0, step - 1], ctx=z - 1).wait_recv()
            if step < n - 1:

                @pl.when(z < n - 1)
                def _():
                    line_copy(k, all_ref, True, step).start()

            core_copy(k, all_ref, step, z - step).start()

        @pl.when(zz >= step)
        def _():
            ref = all_ref.at[dp, z + step]
            remote(ref, ref, s.ag_s.at[k, 1, step - 1], s.ag_r.at[k, 1, step - 1], ctx=z + 1).wait_recv()
            if step < n - 1:

                @pl.when(z > 0)
                def _():
                    line_copy(k, all_ref, False, step).start()

            core_copy(k, all_ref, n - 1 + step, z + step).start()

    def gather_line_finish(k, src, all_ref):
        pltpu.make_async_copy(src, all_ref.at[dp, z], s.own_sem.at[k]).wait()
        for step in range(n - 1):

            @pl.when((z >= step) & (z < n - 1))
            def _():
                line_copy(k, all_ref, True, step, src).wait_send()

            @pl.when((zz >= step) & (z > 0))
            def _():
                line_copy(k, all_ref, False, step, src).wait_send()

        def both(slot, idx):
            ref = all_ref.at[1 - dp, idx]
            copy = remote(src, ref, s.agx_s.at[k, slot], s.agx_r.at[k, slot], dp=1 - dp)
            copy.wait_send()
            copy.wait_recv()

        both(0, z)
        for step in range(1, n):

            @pl.when(z >= step)
            def _():
                both(step, z - step)

            @pl.when(zz >= step)
            def _():
                both(n - 1 + step, z + step)

    me = dp * n + z

    def columns_src(k, src, block):
        if k < 2:
            rows = pl.ds(pl.multiple_of(lax.rem(block, n) * R + t * C, C), C)
            return src.at[rows, pl.ds(pl.multiple_of(block // n * T, T), T)]
        return src.at[mine, pl.ds(pl.multiple_of(block * R, R), R)]

    def columns_copy(k, src, all_ref, e, d):
        to_dp, to_z = dp ^ e, lax.rem(z + d, n)
        return remote(
            columns_src(k, src, to_dp * n + to_z), all_ref.at[t, me],
            s.aa_s.at[k, e * n + d], s.aa_r.at[k, e * n + d], dp=to_dp, ctx=to_z,
        )

    def columns_own(k, src, all_ref):
        return pltpu.make_async_copy(columns_src(k, src, me), all_ref.at[t, me], s.aa_s.at[k, 0])

    def columns_start(k, src, all_ref):
        columns_own(k, src, all_ref).start()
        for d in range(n):
            for e in range(2):
                if e or d:
                    columns_copy(k, src, all_ref, e, d).start()

    def columns_wait_send(k, src, all_ref):
        for e in range(2):
            for d in range(n):
                if e or d:
                    columns_copy(k, src, all_ref, e, d).wait_send()

    def columns_wait_recv(k, src, all_ref):
        columns_own(k, src, all_ref).wait()
        for e in range(2):
            for d in range(n):
                if e or d:
                    ref = all_ref.at[t, (dp ^ e) * n + lax.rem(z - d + n, n)]
                    remote(
                        columns_src(k, src, me), ref, s.aa_s.at[k, e * n + d], s.aa_r.at[k, e * n + d],
                        dp=dp ^ e, ctx=lax.rem(z - d + n, n),
                    ).wait_recv()

    def share_start(k, all_ref):
        for j in range(1, nt):
            remote(
                all_ref.at[t], all_ref.at[t], s.pl_s.at[10 + k, j - 1], s.pl_r.at[10 + k, j - 1], tensor=t ^ j
            ).start()

    def share_wait(k, all_ref):
        for j in range(1, nt):
            copy = remote(
                all_ref.at[t], all_ref.at[t ^ j], s.pl_s.at[10 + k, j - 1], s.pl_r.at[10 + k, j - 1], tensor=t ^ j
            )
            copy.wait_send()
            copy.wait_recv()

    def job_dp_start(job, k, b):
        slot = job.dp_slot(b)

        def body(c, w):
            slot[:, pl.ds(c, w)] = job.part((1 - dp) * nl + b, c, w).astype(BF16)

        tiles(job.cols, 512, body)
        remote(slot, job.dp_recv(b), s.dp_s.at[k, b], s.dp_r.at[k, b], dp=1 - dp).start()

    def job_dp_wait_send(job, k, b):
        remote(job.dp_slot(b), job.dp_recv(b), s.dp_s.at[k, b], s.dp_r.at[k, b], dp=1 - dp).wait_send()

    def job_dp_wait_all(job, k):
        for b in range(nl):
            remote(job.dp_slot(b), job.dp_recv(b), s.dp_s.at[k, b], s.dp_r.at[k, b], dp=1 - dp).wait_recv()

    def chain_copy(job, k, up, step, part):
        i = 0 if up else 1
        width = job.cols // 2
        cols = pl.ds(part * width, width)
        return remote(
            job.chain_slot(up, step).at[:, cols], job.chain(up, step).at[:, cols],
            s.ch_s.at[k, i, step, part], s.ch_r.at[k, i, step, part],
            ctx=(z + 1) if up else (z - 1),
        )

    def chain_step(job, k, step, ways=(True, False), parts=(0, 1)):
        width = job.cols // 2
        for part in parts:
            for up in ways:
                pos = zl if up else zzl

                @pl.when((pos <= step) & (pos < nl - 1))
                def _(up=up, pos=pos, part=part):
                    target = (zl + nl - 1 - step) if up else (zl - (nl - 1 - step))
                    slot = job.chain_slot(up, step)
                    if step:

                        @pl.when(pos >= 1)
                        def _():
                            chain_copy(job, k, up, step - 1, part).wait_recv()

                    def body(c, w):
                        cs = pl.ds(pl.multiple_of(part * width + c, 128), w)
                        total = job.part(dp * nl + target, cs.start, w)
                        total = total + job.dp_recv(target)[:, cs].astype(F32)
                        if step:
                            prev = job.chain(up, step - 1)[:, cs].astype(F32)
                            total = total + jnp.where(pos >= 1, prev, 0.0)
                        slot[:, cs] = total.astype(BF16)

                    tiles(width, 256 if width % 256 == 0 else 128, body)
                    chain_copy(job, k, up, step, part).start()

    def chain_wait_send(job, k, step):
        for up in (True, False):
            pos = zl if up else zzl

            @pl.when((pos <= step) & (pos < nl - 1))
            def _(up=up):
                for part in range(2):
                    chain_copy(job, k, up, step, part).wait_send()

    def chain_final(job, k, out_ref):
        for up in (True, False):
            pos = zl if up else zzl

            @pl.when(pos >= 1)
            def _(up=up):
                for part in range(2):
                    chain_copy(job, k, up, nl - 2, part).wait_recv()

        def body(c, w):
            cs = pl.ds(c, w)
            total = job.part(dp * nl + zl, c, w) + job.dp_recv(zl)[:, cs].astype(F32)
            a = job.chain(True, nl - 2)[:, cs].astype(F32)
            b = job.chain(False, nl - 2)[:, cs].astype(F32)
            out_ref[:, cs] = total + jnp.where(zl >= 1, a, 0.0) + jnp.where(zzl >= 1, b, 0.0)

        tiles(job.cols, 512, body)

    l_tok.wait()
    x = s.tok[...].astype(F32)
    scale = lax.rsqrt(jnp.mean(x * x, axis=-1, keepdims=True) + epsilon)
    s.x1[...] = (x * scale * g1[...]).astype(BF16)
    s.tokshare[...] = s.tok[mine, :].astype(F32)
    l_cot.wait()
    pl.semaphore_wait(barrier, (nt - 1) + (2 * n - 1))
    pl.when(zh == 1)(lambda: mirror(0, s.cot, s.cot2).start())

    def rms(v):
        return lax.rsqrt(jnp.mean(v * v, axis=-1, keepdims=True) + epsilon)

    def rope(v):
        return v * cos[...] + pltpu.roll(v, H // 2, 1) * sin[...]

    def rope_back(g):
        return g * cos[...] + pltpu.roll(g * sin[...], H // 2, 1)

    L = seg_row.shape[1]
    s.segs[:, : reach * T] = jnp.full((1, reach * T), -1, jnp.int32)
    s.segs[:, reach * T :] = seg_row[...]
    row = seg_row[...]
    at_me = lax.broadcasted_iota(jnp.int32, (T, L), 1) == lax.broadcasted_iota(jnp.int32, (T, L), 0) + z * T
    row_f = jnp.broadcast_to(row.astype(F32), (T, L))
    qseg_f = jnp.sum(jnp.where(at_me, row_f, 0.0), axis=1, keepdims=True)
    begins = jnp.sum(jnp.where(row_f < qseg_f, 1.0, 0.0), axis=1, keepdims=True)
    position = (lax.broadcasted_iota(jnp.int32, (T, H), 0) + z * T).astype(F32) - begins
    angles = position * inverse[...]
    cos[...] = jnp.cos(angles)
    lane = lax.broadcasted_iota(jnp.int32, (T, H), 1)
    turned = jnp.sin(angles)
    sin[...] = jnp.where(lane < H // 2, -turned, turned)

    own_rows = pl.ds(reach * T, T)
    l_kw.wait()
    l_vw.wait()
    s.k_raw[...] = dot(s.x1[...], s.kw[...])
    s.kv[own_rows, KV : 2 * KV] = dot(s.x1[...], s.vw[...]).astype(BF16)
    for h in range(KH):
        raw = s.k_raw[:, h * H : (h + 1) * H]
        s.kv[own_rows, h * H : (h + 1) * H] = rope(raw * rms(raw) * gk[...]).astype(BF16)

    def kv_copy(r):
        return remote(
            s.kv.at[pl.ds((reach - r + 1) * T, T)], s.kv.at[pl.ds((reach - r) * T, T)],
            s.kv_s.at[r - 1], s.kv_r.at[r - 1], ctx=z + 1,
        )

    def kv_send(r):
        @pl.when((z < n - 1) & (z >= r - 1))
        def _():
            kv_copy(r).start()

    kv_send(1)
    for r in range(1, reach + 1):

        @pl.when(z < r)
        def _():
            s.kv[pl.ds((reach - r) * T, T), :] = jnp.zeros((T, 2 * KV), BF16)

    l_qw.wait()
    s.q_raw[...] = dot(s.x1[...], s.qw[...])
    for h in range(QH):
        raw = s.q_raw[:, h * H : (h + 1) * H]
        s.q_rot[:, h * H : (h + 1) * H] = rope(raw * rms(raw) * gq[...]).astype(BF16)
    for r in range(1, reach + 1):

        @pl.when(z >= r)
        def _():
            kv_copy(r).wait_recv()

        if r < reach:
            kv_send(r + 1)
    rows_i = lax.broadcasted_iota(jnp.int32, (T, span), 0) + reach * T
    cols_i = lax.broadcasted_iota(jnp.int32, (T, span), 1)
    kseg_f = s.segs[:, pl.ds(pl.multiple_of(z * T, T), span)].astype(F32)
    allowed = (cols_i <= rows_i) & (qseg_f == kseg_f)
    s.mask[...] = jnp.where(allowed, 1.0, 0.0).astype(F32)

    def weights_of(h, g):
        hs = pl.ds(pl.multiple_of(h * H, H), H)
        q = s.q_rot[:, hs]
        k = s.kv[:, pl.ds(pl.multiple_of(g * H, H), H)]
        return q, k, jnp.where(s.mask[...] > 0.0, jnp.exp(dot_nt(q, k) * inv_root), 0.0)

    def attend(h, _):
        g = h // group
        hs = pl.ds(pl.multiple_of(h * H, H), H)
        _q, _k, w = weights_of(h, g)
        v = s.kv[:, pl.ds(pl.multiple_of(KV + g * H, H), H)]
        total = jnp.sum(w, axis=-1, keepdims=True)
        att = dot(w.astype(BF16), v) / total
        s.tot[:, hs] = jnp.broadcast_to(total, (T, H))
        s.att[:, hs] = att
        s.att_low[:, hs] = att.astype(BF16)
        s.attt[hs, :] = att.T.astype(BF16)
        return 0

    lax.fori_loop(0, QH, attend, 0)

    l_ow.wait()

    def body(c, w):
        s.send_a[:, pl.ds(c, w)] = dot(s.att_low[...], s.ow[:, pl.ds(c, w)]).astype(BF16)

    tiles(D, TILE, body)
    scatter_start(0, s.send_a, s.recv0)

    def transpose_half(src, dst, place):
        for d in range(2):

            def body(c, w):
                cs = pl.ds(pl.multiple_of((d * n + zh * nl) * R + c, 128), w)
                rows = pl.ds(pl.multiple_of(d * nl * R + c, 128), w)
                dst[rows, place * T : (place + 1) * T] = src[:, cs].astype(F32).T.astype(BF16)

            tiles(nl * R, TILE, body)

    s.cotshare[...] = s.cot[mine, :].astype(F32)

    transpose_half(s.x1, s.x1t, 0)
    transpose_half(s.cot, s.cott, 0)
    l_dw.wait()

    def hidden_grad(cot, out):
        def body(c, w):
            out[:, pl.ds(c, w)] = dot_nt(cot[...], s.dw[pl.ds(c, w), :])

        tiles(F, TILE, body)

    def cot_share():
        mirror(0, s.cot, s.cot2).wait_recv()
        gather_start(9, s.cot2)

    hidden_grad(s.cot, s.gh)

    s.resid[...] = scatter_sum(0, s.send_a, s.recv0, s.tokshare[...])
    resid = s.resid[...]
    s.x2[mine, :] = (resid * rms(resid) * g2[...]).astype(BF16)
    gather_start(1, s.x2)
    mirror(1, s.x2, s.x2b).start()
    pl.when(zh == 0)(lambda: mirror(0, s.cot, s.cot2).start())
    gather_line_start(2, s.attt, att_all)
    l_gw.wait()
    l_uw.wait()
    gather_wait(1, s.x2)

    def mirrored_share():
        mirror(1, s.x2, s.x2b).wait_recv()
        gather_start(10, s.x2b)

    pl.when(zh == 1)(mirrored_share)
    pl.when(zh == 0)(cot_share)

    def feed(x, grad_hidden, place):
        rows = pl.ds(place * T, T)

        def body(c, w):
            cs = pl.ds(c, w)
            gate = dot(x[...], s.gw[:, cs])
            up = dot(x[...], s.uw[:, cs])
            gh = grad_hidden[:, cs]
            sig = jax.nn.sigmoid(gate)
            act = gate * sig
            s.hid[rows, cs] = (act * up).astype(BF16)
            s.gg[rows, cs] = (gh * up * (sig * (1.0 + gate * (1.0 - sig)))).astype(BF16)
            s.gu[rows, cs] = (gh * act).astype(BF16)

        tiles(F, TILE, body)

    feed(s.x2, s.gh, 0)
    pl.when(zh == 0)(mirrored_share)
    pl.when(zh == 1)(cot_share)
    for d in range(2):
        mirror_x1(d).start()
    own_part = pl.ds(0, T)

    def body(c, w):
        rs = pl.ds(c, w)
        s.send_a[:, rs] = (
            dot_nt(s.gg[own_part, :], s.gw[rs, :]) + dot_nt(s.gu[own_part, :], s.uw[rs, :])
        ).astype(BF16)

    tiles(D, TILE, body)
    transpose_half(s.x2, s.xt, 0)
    mirror(1, s.x2, s.x2b).wait_send()
    scatter_start(2, s.send_a, s.recv1)

    def body(c, w):
        s.send_b[:, pl.ds(c, w)] = dot(s.hid[own_part, :], s.dw[:, pl.ds(c, w)]).astype(BF16)

    tiles(D, TILE, body)
    gather_wait(9, s.cot2)
    hidden_grad(s.cot2, s.gh2)
    transpose_half(s.cot2, s.cott, 1)
    gather_wait(10, s.x2b)
    feed(s.x2b, s.gh2, 1)
    transpose_half(s.x2b, s.xt, 1)
    gather_line_step(2, att_all, 1)
    pl.semaphore_signal(s.credit, inc=1, device_id={"dp": 1 - dp}, device_id_type=MESH)

    grad_second = scatter_sum(2, s.send_a, s.recv1, jnp.zeros((S, D), F32))
    resid = s.resid[...]
    scale = rms(resid)
    normed = resid * scale
    s.gains[:, D : 2 * D] = jnp.sum(grad_second * normed, axis=0, keepdims=True)
    scaled = grad_second * g2[...]
    inner = jnp.mean(scaled * normed, axis=-1, keepdims=True)
    s.gresid[...] = s.cotshare[...] + scale * (scaled - normed * inner)
    s.gm[mine, :] = s.gresid[...].astype(BF16)
    gather_start(4, s.gm)
    columns_start(2, s.gm, s.gmc)

    class WeightJob:
        def __init__(self, k, left, grad):
            self.k, self.left, self.grad, self.cols = k, left, grad, grad.shape[1]

        def part(self, block, c, w):
            rows = pl.ds(pl.multiple_of(block * R, R), R)
            return dot(self.left[rows, :], self.grad[:, pl.ds(c, w)])

        def dp_slot(self, b):
            return s.gw.at[pl.ds(b * R, R), pl.ds(0, self.cols)]

        def dp_recv(self, b):
            return s.uw.at[pl.ds(pl.multiple_of((self.k * nl + b) * R, R), R), pl.ds(0, self.cols)]

        def chain_slot(self, up, step):
            i = nl + self.k * (nl - 1) + (step if up else nl - 2 - step)
            return s.gw.at[pl.ds(i * R, R), pl.ds(0, self.cols)]

        def chain(self, up, step):
            return s.chain.at[self.k, 0 if up or nl == 2 else 1, step, :, pl.ds(0, self.cols)]

    jobs = [
        WeightJob(0, s.cott, s.hid),
        WeightJob(1, s.xt, s.gg),
        WeightJob(2, s.xt, s.gu),
        WeightJob(3, s.x1t, s.dqkv),
    ]
    order = [b for i in range((nl + 1) // 2) for b in dict.fromkeys((nl - 1 - i, i))]

    def job_dp(k):
        for b in order:
            if k:
                job_dp_wait_send(jobs[k - 1], k - 1, b)
            job_dp_start(jobs[k], k, b)

    pl.semaphore_wait(s.credit, 1)
    job_dp(0)
    job_dp_wait_all(jobs[0], 0)
    chain_step(jobs[0], 0, 0, (True, False), (0,))
    chain_step(jobs[0], 0, 0, (True,), (1,))
    job_dp(1)
    gather_line_step(2, att_all, 2)
    gather_wait(4, s.gm)
    scatter_start(3, s.send_b, s.recv2)
    for d in range(2):
        mirror_x1(d).wait_recv()

    def body(c, w):
        s.x1t[pl.ds(c, w), T : 2 * T] = s.x1b[:, pl.ds(c, w)].astype(F32).T.astype(BF16)

    tiles(D // 2, TILE, body)

    gatt = s.gh.at[:, pl.ds(0, QH * H)]

    def body(c, w):
        gatt[:, pl.ds(c, w)] = dot_nt(s.gm[...], s.ow[pl.ds(c, w), :])

    tiles(QH * H, TILE, body)
    s.gq_acc[...] = jnp.zeros((1, H), F32)

    def back(g, _):
        ks = pl.ds(pl.multiple_of(g * H, H), H)
        vs = pl.ds(pl.multiple_of(KV + g * H, H), H)
        v = s.kv[:, vs]
        grad_k = jnp.zeros((span, H), F32)
        grad_v = jnp.zeros((span, H), F32)
        for i in range(group):
            h = g * group + i
            hs = pl.ds(pl.multiple_of(h * H, H), H)
            q, k, w = weights_of(h, g)
            ga, total = gatt[:, hs], s.tot[:, hs]
            gs = (ga / total).astype(BF16)
            delta = jnp.sum(ga * s.att[:, hs], axis=-1, keepdims=True) / total[:, :1]
            ds = (w * (dot_nt(gs, v) - delta)).astype(BF16)
            grad_k = grad_k + dot_tn(ds, q) * inv_root
            grad_v = grad_v + dot_tn(w.astype(BF16), gs)
            gr = rope_back(dot(ds, k) * inv_root)
            raw = s.q_raw[:, hs]
            r = rms(raw)
            nq = raw * r
            s.gq_acc[...] += jnp.sum(gr * nq, axis=0, keepdims=True)
            sc = gr * gq[...]
            s.dqkv[:T, hs] = (r * (sc - nq * jnp.mean(sc * nq, axis=-1, keepdims=True))).astype(BF16)
        s.dkv[:, ks] = grad_k.astype(BF16)
        s.dkv[:, vs] = grad_v.astype(BF16)
        return 0

    lax.fori_loop(0, KH, back, 0)
    s.gains[:, 2 * D : 2 * D + H] = s.gq_acc[...]

    def dkv_copy(i):
        return remote(
            s.dkv.at[pl.ds(i * T, T)], s.dkv_in.at[i], s.dkv_s.at[i], s.dkv_r.at[i], ctx=z - 1
        )

    for i in range(reach):
        if i:

            @pl.when((z < n - 1) & (z + 1 >= reach - i + 1))
            def _():
                dkv_copy(i - 1).wait_recv()
                rows = pl.ds(i * T, T)
                s.dkv[rows, :] = (s.dkv[rows, :].astype(F32) + s.dkv_in[i - 1].astype(F32)).astype(BF16)

        @pl.when(z >= reach - i)
        def _():
            dkv_copy(i).start()

        if i == 0:
            job_dp_wait_all(jobs[1], 1)
            chain_step(jobs[1], 1, 0, (True,))
            job_dp(2)

    chain_step(jobs[0], 0, 0, (False,), (1,))
    chain_step(jobs[1], 1, 0, (False,))

    @pl.when(z < n - 1)
    def _():
        dkv_copy(reach - 1).wait_recv()

    own = s.dkv[pl.ds(reach * T, T), :].astype(F32)
    own = own + jnp.where(z < n - 1, s.dkv_in[reach - 1].astype(F32), 0.0)
    s.dqkv[:T, QH * H + KV :] = own[:, KV:].astype(BF16)
    gk_sum = jnp.zeros((1, H), F32)
    for h in range(KH):
        gr = rope_back(own[:, h * H : (h + 1) * H])
        raw = s.k_raw[:, h * H : (h + 1) * H]
        r = rms(raw)
        nk = raw * r
        gk_sum = gk_sum + jnp.sum(gr * nk, axis=0, keepdims=True)
        sc = gr * gk[...]
        s.dqkv[:T, QH * H + h * H : QH * H + (h + 1) * H] = (
            r * (sc - nk * jnp.mean(sc * nk, axis=-1, keepdims=True))
        ).astype(BF16)
    s.gains[:, 2 * D + H :] = gk_sum
    mirror_qkv().start()
    job_dp_wait_all(jobs[2], 2)
    chain_step(jobs[2], 2, 0)

    q_c, k_c, v_c = pl.ds(0, QH * H), pl.ds(QH * H, KV), pl.ds(QH * H + KV, KV)

    def body(c, w):
        rs = pl.ds(c, w)
        s.send_a[:, rs] = (
            dot_nt(s.dqkv[:T, q_c], s.qw[rs, :])
            + dot_nt(s.dqkv[:T, k_c], s.kw[rs, :])
            + dot_nt(s.dqkv[:T, v_c], s.vw[rs, :])
        ).astype(BF16)

    tiles(D, TILE, body)
    scatter_start(6, s.send_a, s.recv3)
    s.outsh[...] = scatter_sum(3, s.send_b, s.recv2, s.resid[...]).astype(BF16)
    grad_first = scatter_sum(6, s.send_a, s.recv3, jnp.zeros((S, D), F32))
    tokshare = s.tokshare[...]
    scale = rms(tokshare)
    normed = tokshare * scale
    s.gains[:, :D] = jnp.sum(grad_first * normed, axis=0, keepdims=True)
    scaled = grad_first * g1[...]
    inner = jnp.mean(scaled * normed, axis=-1, keepdims=True)
    s.tgsh[...] = (s.gresid[...] + scale * (scaled - normed * inner)).astype(BF16)
    spread_start(7, s.tgsh, tgrad_hbm, 1)
    for j in range(1, nt):
        remote(s.gains, s.gains_p.at[j - 1], s.pl_s.at[8, j - 1], s.pl_r.at[8, j - 1], tensor=t ^ j).start()
    columns_wait_recv(2, s.gm, s.gmc)
    share_start(2, s.gmc)
    spread_start(5, s.outsh, out_hbm, 0)
    for j in range(1, nt):
        remote(s.gains, s.gains_p.at[j - 1], s.pl_s.at[8, j - 1], s.pl_r.at[8, j - 1], tensor=t ^ j).wait()
    total = s.gains[...]
    for j in range(1, nt):
        total = total + s.gains_p[j - 1]
    s.gains2[...] = total

    def gain_copy(e, d):
        i = e * n + d
        return remote(
            s.gains2, s.gains_x.at[i - 1], s.ga_s.at[i], s.ga_r.at[i], dp=dp ^ e, ctx=lax.rem(z + d, n)
        )

    for e in range(2):
        for d in range(n):
            if e or d:
                gain_copy(e, d).start()
    mirror_qkv().wait_recv()
    job_dp(3)
    job_dp_wait_all(jobs[3], 3)
    chain_step(jobs[3], 3, 0)
    for step in range(1, nl - 1):
        for k, job in enumerate(jobs):
            chain_step(job, k, step)

    stage = s.gh2.at[pl.ds(0, R), pl.ds(0, QH * H + 2 * KV)]

    def gate_copy():
        return pltpu.make_async_copy(s.gh.at[pl.ds(0, R)], gate_out, s.load_sem.at[2])

    def up_copy():
        return pltpu.make_async_copy(s.gh.at[pl.ds(0, R)], up_out, s.load_sem.at[3])

    def qkv_copies():
        parts = [(q_out, 0, QH * H), (k_out, QH * H, KV), (v_out, QH * H + KV, KV)]
        return [
            pltpu.make_async_copy(stage.at[:, pl.ds(a, w)], ref, s.load_sem.at[6 + i])
            for i, (ref, a, w) in enumerate(parts)
        ]

    rows = pl.ds(0, R)
    chain_final(jobs[0], 0, s.gh.at[rows])
    width = min(256, F)
    flip = s.gh2.at[:, pl.ds(QH * H + 2 * KV, 2 * R)]

    def down_copy(i):
        return pltpu.make_async_copy(
            flip.at[pl.ds(0, width), pl.ds((i % 2) * R, R)],
            down_out.at[pl.ds(i * width, width)],
            s.load_sem.at[4 + i % 2],
        )

    count = F // width
    for i in range(count):
        if i >= 2:
            down_copy(i - 2).wait()
        flip[:width, (i % 2) * R : (i % 2 + 1) * R] = s.gh[rows, i * width : (i + 1) * width].T
        down_copy(i).start()
    for i in range(max(0, count - 2), count):
        down_copy(i).wait()
    for step in range(3, n):
        gather_line_step(2, att_all, step)
    gather_line_finish(2, s.attt, att_all)
    share_wait(2, s.gmc)

    def load(i):
        slot = lax.rem(i, 2)
        return pltpu.make_async_copy(
            att_all.at[i // n, lax.rem(i, n)],
            s.dw.at[pl.ds(pl.multiple_of(slot * QH * H, QH * H), QH * H), pl.ds(0, T)],
            s.stage_sem.at[slot],
        )

    load(0).start()
    outw_out[...] = jnp.zeros(outw_out.shape, F32)

    def step(i, _):
        @pl.when(i + 1 < 2 * n)
        def _():
            load(i + 1).start()

        load(i).wait()
        slot = lax.rem(i, 2)
        left = s.dw[pl.ds(pl.multiple_of(slot * QH * H, QH * H), QH * H), pl.ds(0, T)]
        outw_out[...] += dot(left, s.gmc[:, i].reshape(T, R))
        return 0

    lax.fori_loop(0, 2 * n, step, 0)
    chain_final(jobs[1], 1, s.gh.at[rows])
    gate_copy().start()
    chain_final(jobs[3], 3, stage)
    for copy in qkv_copies():
        copy.start()
    gate_copy().wait()
    chain_final(jobs[2], 2, s.gh.at[rows])
    up_copy().start()
    for e in range(2):
        for d in range(n):
            if e or d:
                gain_copy(e, d).wait()
    total = s.gains2[...]
    for i in range(2 * n - 1):
        total = total + s.gains_x[i]
    gains_out[...] = total

    columns_wait_send(2, s.gm, s.gmc)
    mirror(0, s.cot, s.cot2).wait_send()
    mirror_qkv().wait_send()
    for d in range(2):
        mirror_x1(d).wait_send()
    for b in order:
        job_dp_wait_send(jobs[-1], len(jobs) - 1, b)
    for st in range(nl - 1):
        for k, job in enumerate(jobs):
            chain_wait_send(job, k, st)
    for r in range(1, reach + 1):

        @pl.when((z < n - 1) & (z >= r - 1))
        def _():
            kv_copy(r).wait_send()

    for i in range(reach):

        @pl.when(z >= reach - i)
        def _():
            dkv_copy(i).wait_send()

    spread_wait(5, s.outsh, out_hbm, 0)
    spread_wait(7, s.tgsh, tgrad_hbm, 1)
    up_copy().wait()
    for copy in qkv_copies():
        copy.wait()


def run_layer(dm, *operands):
    T, D, H, F, n, nt, reach, S, R = dm.T, dm.D, dm.H, dm.F, dm.n, dm.nt, dm.reach, dm.S, dm.R
    QC, KV = dm.QH * H, dm.KH * H
    span = (reach + 1) * T
    G = 2 * D + 2 * H
    dma = pltpu.SemaphoreType.DMA
    scratch = dict(
        tok=((T, D), BF16), x1=((T, D), BF16), send_b=((T, D), BF16), cot=((T, D), BF16), x2=((T, D), BF16),
        outsh=((S, D), BF16), tgsh=((S, D), BF16), xt=((D // 2, 2 * T), BF16), cott=((D // 2, 2 * T), BF16),
        cot2=((T, D), BF16), x2b=((T, D), BF16),
        qw=((D, QC), BF16), kw=((D, KV), BF16), vw=((D, KV), BF16), ow=((QC, D), BF16),
        gw=((D, F), BF16), uw=((D, F), BF16), dw=((F, D), BF16),
        tokshare=((S, D), F32), cotshare=((S, D), F32), resid=((S, D), F32), gresid=((S, D), F32),
        k_raw=((T, KV), F32), q_raw=((T, QC), F32), q_rot=((T, QC), BF16), kv=((span, 2 * KV), BF16),
        mask=((T, span), F32), tot=((T, QC), F32), att=((T, QC), F32), att_low=((T, QC), BF16),
        attt=((QC, T), BF16), gq_acc=((1, H), F32),
        recv0=((nt - 1, S, D), BF16), recv1=((nt - 1, S, D), BF16),
        gh=((T, F), F32), hid=((2 * T, F), BF16), gg=((2 * T, F), BF16), gu=((2 * T, F), BF16),
        dkv=((span, 2 * KV), BF16), dkv_in=((reach, T, 2 * KV), BF16), dqkv=((2 * T, QC + 2 * KV), BF16),
        chain=((4, 1 if n == 4 else 2, n // 2 - 1, R, F), BF16),

        gmc=((nt, 2 * n, S, R), BF16), x1b=((T, D // 2), BF16), x1t=((D // 2, 2 * T), BF16), gh2=((T, F), F32),
        cos=((T, H), F32), sin=((T, H), F32), segs=((1, reach * T + dm.L), jnp.int32),
        gains=((1, G), F32), gains2=((1, G), F32), gains_p=((nt - 1, 1, G), F32),
        gains_x=((2 * n - 1, 1, G), F32),
    )
    sems = dict(
        load_sem=(9,), own_sem=(3,), pl_s=(13, nt - 1), pl_r=(13, nt - 1), ag_s=(3, 2, n - 1), ag_r=(3, 2, n - 1),
        agx_s=(3, 2 * n - 1), agx_r=(3, 2 * n - 1), aa_s=(3, 2 * n), aa_r=(3, 2 * n), stage_sem=(2,),
        dp_s=(4, n // 2), dp_r=(4, n // 2), ch_s=(4, 2, n // 2 - 1, 2), ch_r=(4, 2, n // 2 - 1, 2), mi_s=(5,), mi_r=(5,), kv_s=(reach,), kv_r=(reach,),
        dkv_s=(reach,), dkv_r=(reach,), ga_s=(2 * n,), ga_r=(2 * n,),
    )
    names = list(scratch) + list(sems) + ["credit"]
    shapes = [pltpu.VMEM(*v) for v in scratch.values()] + [dma(v) for v in sems.values()]
    shapes.append(pltpu.SemaphoreType.REGULAR)

    def body(*refs):
        fixed = len(refs) - len(names)
        s = Dims()
        for name, ref in zip(names, refs[fixed:]):
            setattr(s, name, ref)
        for alias, of in dm.alias.items():
            setattr(s, alias, getattr(s, of))
        layer_kernel(dm, *refs[:fixed], s)

    hbm = pl.BlockSpec(memory_space=pl.ANY)
    vmem = pl.BlockSpec(memory_space=pltpu.VMEM)
    return pl.pallas_call(
        body,
        out_shape=(
            jax.ShapeDtypeStruct((T, D), BF16),
            jax.ShapeDtypeStruct((T, D), BF16),
            jax.ShapeDtypeStruct((R, F), F32),
            jax.ShapeDtypeStruct((R, F), F32),
            jax.ShapeDtypeStruct((F, R), F32),
            jax.ShapeDtypeStruct((R, QC), F32),
            jax.ShapeDtypeStruct((R, KV), F32),
            jax.ShapeDtypeStruct((R, KV), F32),
            jax.ShapeDtypeStruct((QC, R), F32),
            jax.ShapeDtypeStruct((1, G), F32),
            jax.ShapeDtypeStruct((2, n, QC, T), BF16),
        ),
        in_specs=[hbm] * 2 + [vmem] * 3 + [hbm] * 7,
        out_specs=[hbm] * 8 + [vmem] * 2 + [hbm],
        scratch_shapes=shapes,
        compiler_params=pltpu.CompilerParams(
            collective_id=0, has_side_effects=True, vmem_limit_bytes=67043328
        ),
        name="layer",
    )(*operands)


def per_device(
    tokens,
    segments,
    first_gain,
    query_weight,
    key_matrix,
    value_matrix,
    query_norm_gain,
    key_gain,
    output_weight,
    second_gain,
    gate_weight,
    up_weight,
    down_weight,
    cotangent,
):
    _, T, D = tokens.shape
    dm = Dims()
    dm.T, dm.D, dm.H, dm.F = T, D, query_norm_gain.shape[0], gate_weight.shape[1]
    dm.QH, dm.KH = query_weight.shape[1] // dm.H, key_matrix.shape[1] // dm.H
    dm.n, dm.nt = lax.axis_size("ctx"), lax.axis_size("tensor")
    length = segments.shape[1]
    dm.reach = -(-(length // 2 - 1) // T)
    dm.S, dm.R = T // dm.nt, D // (2 * dm.n)
    dm.alias = {"send_a": "tok", "gm": "x2", "recv2": "recv0", "recv3": "recv1"}
    H = dm.H
    dm.L = length
    inverse = (1.0 / rope_base ** (np.arange(0, H, 2, dtype=np.float32) / np.float32(H))).astype(np.float32)
    inverse = np.concatenate([inverse, inverse])[None]
    all_gains = jnp.concatenate([first_gain, second_gain, query_norm_gain, key_gain]).astype(F32)[None]
    out, tgrad, gate_g, up_g, down_g, q_g, k_g, v_g, out_g, gains = run_layer(
        dm,
        tokens.reshape(T, D),
        cotangent.reshape(T, D),
        all_gains,
        inverse,
        segments,
        query_weight,
        key_matrix,
        value_matrix,
        output_weight,
        gate_weight,
        up_weight,
        down_weight,
    )[:10]
    gains = gains[0]
    return (
        out.reshape(tokens.shape),
        tgrad.reshape(tokens.shape),
        gains[:D],
        q_g,
        k_g,
        v_g,
        gains[2 * D : 2 * D + H],
        gains[2 * D + H :],
        out_g,
        gains[D : 2 * D],
        gate_g,
        up_g,
        down_g,
    )


def solution(mesh):
    return jax.shard_map(
        per_device,
        mesh=mesh,
        in_specs=(
            P("dp", "ctx", None),
            P("dp", None),
            P(),
            P(None, "tensor"),
            P(None, "tensor"),
            P(None, "tensor"),
            P(),
            P(),
            P("tensor", None),
            P(),
            P(None, "tensor"),
            P(None, "tensor"),
            P("tensor", None),
            P("dp", "ctx", None),
        ),
        out_specs=(
            P("dp", "ctx", None),
            P("dp", "ctx", None),
            P(),
            P(("dp", "ctx"), "tensor"),
            P(("dp", "ctx"), "tensor"),
            P(("dp", "ctx"), "tensor"),
            P(),
            P(),
            P("tensor", ("dp", "ctx")),
            P(),
            P(("dp", "ctx"), "tensor"),
            P(("dp", "ctx"), "tensor"),
            P("tensor", ("dp", "ctx")),
        ),
        check_vma=False,
    )
```

```python
import functools
import math

import jax
import jax.numpy as jnp
import numpy as np
from jax import lax
from jax.experimental import pallas as pl
from jax.experimental.pallas import tpu as pltpu
from jax.sharding import PartitionSpec as P

epsilon = 1e-06
rope_base = 1000000.0
F32 = jnp.float32
BF16 = jnp.bfloat16
MESH = pl.DeviceIdType.MESH
TILE = 256


def dot(a, b):
    return jnp.dot(a, b, preferred_element_type=F32)


def dot_nt(a, b):
    return lax.dot_general(a, b, (((1,), (1,)), ((), ())), preferred_element_type=F32)


def dot_tn(a, b):
    return lax.dot_general(a, b, (((0,), (0,)), ((), ())), preferred_element_type=F32)


def remote(src, dst, send_sem, recv_sem, **device):
    return pltpu.make_async_remote_copy(
        src_ref=src,
        dst_ref=dst,
        send_sem=send_sem,
        recv_sem=recv_sem,
        device_id=device,
        device_id_type=MESH,
    )


def tiles(total, size, body):
    size = min(size, total)

    def step(i, _):
        body(pl.multiple_of(i * size, size), size)
        return 0

    lax.fori_loop(0, total // size, step, 0)


class Dims:
    pass


def layer_kernel(
    dm,
    tok_hbm,
    cot_hbm,
    first_in,
    second_in,
    query_in,
    key_in,
    inverse,
    seg_row,
    qw_hbm,
    kw_hbm,
    vw_hbm,
    ow_hbm,
    gw_hbm,
    uw_hbm,
    dw_hbm,
    out_hbm,
    tgrad_hbm,
    gate_out,
    up_out,
    down_out,
    q_out,
    k_out,
    v_out,
    outw_out,
    gains_out,
    att_all,
    s,
):
    T, D, H, QH, KH, F, n, nt, reach, S, R = (
        dm.T, dm.D, dm.H, dm.QH, dm.KH, dm.F, dm.n, dm.nt, dm.reach, dm.S, dm.R,
    )
    group = QH // KH
    span = (reach + 1) * T
    KV = KH * H
    inv_root = 1.0 / math.sqrt(H)
    C = R // nt
    gain_in = s.gain_in
    for place, ref in ((0, first_in), (D, second_in), (2 * D, query_in), (2 * D + H, key_in)):
        for i in range(ref.shape[0]):
            gain_in[:, place + i * H : place + (i + 1) * H] = ref[i : i + 1, :].astype(F32)
    g1 = gain_in.at[:, pl.ds(0, D)]
    g2 = gain_in.at[:, pl.ds(D, D)]
    gq = gain_in.at[:, pl.ds(2 * D, H)]
    gk = gain_in.at[:, pl.ds(2 * D + H, H)]
    cos, sin = s.cos, s.sin
    dp, z, t = lax.axis_index("dp"), lax.axis_index("ctx"), lax.axis_index("tensor")
    zz = n - 1 - z
    nl = n // 2
    zh, zl = z // nl, lax.rem(z, nl)
    zzl = nl - 1 - zl

    barrier = pltpu.get_barrier_semaphore()
    for j in range(1, nt):
        pl.semaphore_signal(barrier, inc=1, device_id={"tensor": t ^ j}, device_id_type=MESH)
    for e in range(2):
        for d in range(n):
            if e or d:
                pl.semaphore_signal(
                    barrier,
                    inc=1,
                    device_id={"dp": dp ^ e, "ctx": lax.rem(z + d, n)},
                    device_id_type=MESH,
                )

    loads = [
        (tok_hbm, s.tok), (cot_hbm, s.cot), (kw_hbm, s.kw), (vw_hbm, s.vw), (qw_hbm, s.qw),
        (ow_hbm, s.ow), (dw_hbm, s.dw), (gw_hbm, s.gw), (uw_hbm, s.uw),
    ]
    loads = [pltpu.make_async_copy(a, b, s.load_sem.at[i]) for i, (a, b) in enumerate(loads)]
    for load in loads:
        load.start()
    (l_tok, l_cot, l_kw, l_vw, l_qw, l_ow, l_dw, l_gw, l_uw) = loads

    def scatter_start(k, buf, recv):
        for j in range(1, nt):
            peer = t ^ j
            remote(
                buf.at[pl.ds(pl.multiple_of(peer * S, S), S)], recv.at[j - 1],
                s.pl_s.at[k, j - 1], s.pl_r.at[k, j - 1], tensor=peer,
            ).start()

    def scatter_sum(k, buf, recv, base):
        mine = pl.ds(pl.multiple_of(t * S, S), S)
        for j in range(1, nt):
            remote(
                buf.at[mine], recv.at[j - 1], s.pl_s.at[k, j - 1], s.pl_r.at[k, j - 1], tensor=t ^ j
            ).wait()
        total = base + buf[mine, :].astype(F32)
        for j in range(1, nt):
            total = total + recv[j - 1].astype(F32)
        return total

    def rows_of(peer, half=None):
        if half is None:
            return pl.ds(pl.multiple_of(peer * S, S), S)
        return pl.ds(pl.multiple_of(peer * S + half * (S // 2), S // 2), S // 2)

    def gather_copy(k, full, j):
        rows = rows_of(t)
        return remote(full.at[rows], full.at[rows], s.pl_s.at[k, j - 1], s.pl_r.at[k, j - 1], tensor=t ^ j)

    def gather_arrived(k, full, j):
        rows = rows_of(t ^ j)
        return remote(full.at[rows], full.at[rows], s.pl_s.at[k, j - 1], s.pl_r.at[k, j - 1], tensor=t ^ j)

    def relay_copy(k, full, origin, half, to):
        rows = rows_of(origin, half)
        sems = (s.pl2_s.at[k], s.pl2_r.at[k]) if half else (s.pl_s.at[k, 2], s.pl_r.at[k, 2])
        return remote(full.at[rows], full.at[rows], *sems, tensor=to)

    def gather_start(k, full):
        for j in range(1, nt) if nt != 4 else (1, 2):
            gather_copy(k, full, j).start()

    def gather_forward(k, full):
        if nt == 4:
            gather_arrived(k, full, 1).wait_recv()
            relay_copy(k, full, t ^ 1, 0, t ^ 2).start()
            gather_arrived(k, full, 2).wait_recv()
            relay_copy(k, full, t ^ 2, 1, t ^ 1).start()

    def gather_wait(k, full):
        for j in range(1, nt) if nt != 4 else (1, 2):
            gather_copy(k, full, j).wait_send()
            if nt != 4:
                gather_arrived(k, full, j).wait_recv()
        if nt == 4:
            relay_copy(k, full, t ^ 1, 0, t ^ 2).wait_send()
            relay_copy(k, full, t ^ 2, 1, t ^ 1).wait_send()
            relay_copy(k, full, t ^ 3, 0, t ^ 2).wait_recv()
            relay_copy(k, full, t ^ 3, 1, t ^ 1).wait_recv()

    mine = pl.ds(pl.multiple_of(t * S, S), S)

    def spread_start(k, share, full, own):
        own_copy(share, full, own).start()
        for j in range(1, nt):
            remote(
                share, full.at[mine], s.pl_s.at[k, j - 1], s.pl_r.at[k, j - 1], tensor=t ^ j
            ).start()

    def own_copy(share, full, own):
        return pltpu.make_async_copy(share, full.at[mine], s.load_sem.at[own])

    def spread_wait(k, share, full, own):
        own_copy(share, full, own).wait()
        for j in range(1, nt):
            peer = t ^ j
            theirs = pl.ds(pl.multiple_of(peer * S, S), S)
            copy = remote(share, full.at[theirs], s.pl_s.at[k, j - 1], s.pl_r.at[k, j - 1], tensor=peer)
            copy.wait_send()
            copy.wait_recv()

    def mirror(i, src, dst):
        return remote(src.at[mine], dst.at[mine], s.mi_s.at[i], s.mi_r.at[i], ctx=zz)

    def mirror_x1(d):
        cols = pl.ds(pl.multiple_of((d * n + (1 - zh) * nl) * R, 128), nl * R)
        return remote(
            s.x1.at[:, cols], s.x1b.at[:, pl.ds(d * nl * R, nl * R)], s.mi_s.at[2 + d], s.mi_r.at[2 + d], ctx=zz
        )

    def mirror_qkv():
        return remote(
            s.dqkv.at[pl.ds(0, T)], s.dqkv.at[pl.ds(T, T)], s.mi_s.at[4], s.mi_r.at[4], ctx=zz
        )

    def line_copy(k, all_ref, up, step, src=None):
        idx = (z - step) if up else (z + step)
        ref = all_ref.at[dp, idx]
        return remote(
            ref if src is None else src, ref,
            s.ag_s.at[k, 0 if up else 1, step], s.ag_r.at[k, 0 if up else 1, step],
            ctx=(z + 1) if up else (z - 1),
        )

    def core_copy(k, all_ref, slot, idx, src=None):
        ref = all_ref.at[dp, idx]
        return remote(
            ref if src is None else src, ref, s.agx_s.at[k, slot], s.agx_r.at[k, slot], dp=1 - dp
        )

    def gather_line_start(k, src, all_ref):
        pltpu.make_async_copy(src, all_ref.at[dp, z], s.own_sem.at[k]).start()

        @pl.when(z < n - 1)
        def _():
            line_copy(k, all_ref, True, 0, src).start()

        @pl.when(z > 0)
        def _():
            line_copy(k, all_ref, False, 0, src).start()

        core_copy(k, all_ref, 0, z, src).start()

    def gather_line_step(k, all_ref, step):
        @pl.when(z >= step)
        def _():
            ref = all_ref.at[dp, z - step]
            remote(ref, ref, s.ag_s.at[k, 0, step - 1], s.ag_r.at[k, 0, step - 1], ctx=z - 1).wait_recv()
            if step < n - 1:

                @pl.when(z < n - 1)
                def _():
                    line_copy(k, all_ref, True, step).start()

            core_copy(k, all_ref, step, z - step).start()

        @pl.when(zz >= step)
        def _():
            ref = all_ref.at[dp, z + step]
            remote(ref, ref, s.ag_s.at[k, 1, step - 1], s.ag_r.at[k, 1, step - 1], ctx=z + 1).wait_recv()
            if step < n - 1:

                @pl.when(z > 0)
                def _():
                    line_copy(k, all_ref, False, step).start()

            core_copy(k, all_ref, n - 1 + step, z + step).start()

    def gather_line_finish(k, src, all_ref):
        pltpu.make_async_copy(src, all_ref.at[dp, z], s.own_sem.at[k]).wait()
        for step in range(n - 1):

            @pl.when((z >= step) & (z < n - 1))
            def _():
                line_copy(k, all_ref, True, step, src).wait_send()

            @pl.when((zz >= step) & (z > 0))
            def _():
                line_copy(k, all_ref, False, step, src).wait_send()

        def both(slot, idx):
            ref = all_ref.at[1 - dp, idx]
            copy = remote(src, ref, s.agx_s.at[k, slot], s.agx_r.at[k, slot], dp=1 - dp)
            copy.wait_send()
            copy.wait_recv()

        both(0, z)
        for step in range(1, n):

            @pl.when(z >= step)
            def _():
                both(step, z - step)

            @pl.when(zz >= step)
            def _():
                both(n - 1 + step, z + step)

    me = dp * n + z

    def columns_src(k, src, block):
        if k < 2:
            rows = pl.ds(pl.multiple_of(lax.rem(block, n) * R + t * C, C), C)
            return src.at[rows, pl.ds(pl.multiple_of(block // n * T, T), T)]
        return src.at[mine, pl.ds(pl.multiple_of(block * R, R), R)]

    def columns_copy(k, src, all_ref, e, d):
        to_dp, to_z = dp ^ e, lax.rem(z + d, n)
        return remote(
            columns_src(k, src, to_dp * n + to_z), all_ref.at[t, me],
            s.aa_s.at[k, e * n + d], s.aa_r.at[k, e * n + d], dp=to_dp, ctx=to_z,
        )

    def columns_own(k, src, all_ref):
        return pltpu.make_async_copy(columns_src(k, src, me), all_ref.at[t, me], s.aa_s.at[k, 0])

    def columns_start(k, src, all_ref):
        columns_own(k, src, all_ref).start()
        for d in range(n):
            for e in range(2):
                if e or d:
                    columns_copy(k, src, all_ref, e, d).start()

    def columns_wait_send(k, src, all_ref):
        for e in range(2):
            for d in range(n):
                if e or d:
                    columns_copy(k, src, all_ref, e, d).wait_send()

    def columns_wait_recv(k, src, all_ref):
        columns_own(k, src, all_ref).wait()
        for e in range(2):
            for d in range(n):
                if e or d:
                    ref = all_ref.at[t, (dp ^ e) * n + lax.rem(z - d + n, n)]
                    remote(
                        columns_src(k, src, me), ref, s.aa_s.at[k, e * n + d], s.aa_r.at[k, e * n + d],
                        dp=dp ^ e, ctx=lax.rem(z - d + n, n),
                    ).wait_recv()

    def share_start(k, all_ref):
        for j in range(1, nt):
            remote(
                all_ref.at[t], all_ref.at[t], s.pl_s.at[10 + k, j - 1], s.pl_r.at[10 + k, j - 1], tensor=t ^ j
            ).start()

    def share_wait(k, all_ref):
        for j in range(1, nt):
            copy = remote(
                all_ref.at[t], all_ref.at[t ^ j], s.pl_s.at[10 + k, j - 1], s.pl_r.at[10 + k, j - 1], tensor=t ^ j
            )
            copy.wait_send()
            copy.wait_recv()

    def job_dp_start(job, k, b):
        slot = job.dp_slot(b)

        def body(c, w):
            slot[:, pl.ds(c, w)] = job.part((1 - dp) * nl + b, c, w).astype(BF16)

        tiles(job.cols, 512, body)
        remote(slot, job.dp_recv(b), s.dp_s.at[k, b], s.dp_r.at[k, b], dp=1 - dp).start()

    def job_dp_wait_send(job, k, b):
        remote(job.dp_slot(b), job.dp_recv(b), s.dp_s.at[k, b], s.dp_r.at[k, b], dp=1 - dp).wait_send()

    def job_dp_wait_all(job, k):
        for b in range(nl):
            remote(job.dp_slot(b), job.dp_recv(b), s.dp_s.at[k, b], s.dp_r.at[k, b], dp=1 - dp).wait_recv()

    def chain_copy(job, k, up, step, part):
        i = 0 if up else 1
        width = job.cols // 2
        cols = pl.ds(part * width, width)
        return remote(
            job.chain_slot(up, step).at[:, cols], job.chain(up, step).at[:, cols],
            s.ch_s.at[k, i, step, part], s.ch_r.at[k, i, step, part],
            ctx=(z + 1) if up else (z - 1),
        )

    def chain_step(job, k, step, ways=(True, False), parts=(0, 1)):
        width = job.cols // 2
        for part in parts:
            for up in ways:
                pos = zl if up else zzl

                @pl.when((pos <= step) & (pos < nl - 1))
                def _(up=up, pos=pos, part=part):
                    target = (zl + nl - 1 - step) if up else (zl - (nl - 1 - step))
                    slot = job.chain_slot(up, step)
                    if step:

                        @pl.when(pos >= 1)
                        def _():
                            chain_copy(job, k, up, step - 1, part).wait_recv()

                    def body(c, w):
                        cs = pl.ds(pl.multiple_of(part * width + c, 128), w)
                        total = job.part(dp * nl + target, cs.start, w)
                        total = total + job.dp_recv(target)[:, cs].astype(F32)
                        if step:
                            prev = job.chain(up, step - 1)[:, cs].astype(F32)
                            total = total + jnp.where(pos >= 1, prev, 0.0)
                        slot[:, cs] = total.astype(BF16)

                    tiles(width, 256 if width % 256 == 0 else 128, body)
                    chain_copy(job, k, up, step, part).start()

    def chain_wait_send(job, k, step):
        for up in (True, False):
            pos = zl if up else zzl

            @pl.when((pos <= step) & (pos < nl - 1))
            def _(up=up):
                for part in range(2):
                    chain_copy(job, k, up, step, part).wait_send()

    def chain_final(job, k, out_ref):
        for up in (True, False):
            pos = zl if up else zzl

            @pl.when(pos >= 1)
            def _(up=up):
                for part in range(2):
                    chain_copy(job, k, up, nl - 2, part).wait_recv()

        def body(c, w):
            cs = pl.ds(c, w)
            total = job.part(dp * nl + zl, c, w) + job.dp_recv(zl)[:, cs].astype(F32)
            a = job.chain(True, nl - 2)[:, cs].astype(F32)
            b = job.chain(False, nl - 2)[:, cs].astype(F32)
            out_ref[:, cs] = total + jnp.where(zl >= 1, a, 0.0) + jnp.where(zzl >= 1, b, 0.0)

        tiles(job.cols, 512, body)

    l_tok.wait()
    x = s.tok[...].astype(F32)
    scale = lax.rsqrt(jnp.mean(x * x, axis=-1, keepdims=True) + epsilon)
    s.x1[...] = (x * scale * g1[...]).astype(BF16)
    s.tokshare[...] = s.tok[mine, :].astype(F32)
    l_cot.wait()
    pl.semaphore_wait(barrier, (nt - 1) + (2 * n - 1))
    pl.when(zh == 1)(lambda: mirror(0, s.cot, s.cot2).start())

    def rms(v):
        return lax.rsqrt(jnp.mean(v * v, axis=-1, keepdims=True) + epsilon)

    def rope(v):
        return v * cos[...] + pltpu.roll(v, H // 2, 1) * sin[...]

    def rope_back(g):
        return g * cos[...] + pltpu.roll(g * sin[...], H // 2, 1)

    L = seg_row.shape[1]
    s.segs[:, : reach * T] = jnp.full((1, reach * T), -1, jnp.int32)
    s.segs[:, reach * T :] = seg_row[...]
    row = seg_row[...]
    at_me = lax.broadcasted_iota(jnp.int32, (T, L), 1) == lax.broadcasted_iota(jnp.int32, (T, L), 0) + z * T
    row_f = jnp.broadcast_to(row.astype(F32), (T, L))
    qseg_f = jnp.sum(jnp.where(at_me, row_f, 0.0), axis=1, keepdims=True)
    begins = jnp.sum(jnp.where(row_f < qseg_f, 1.0, 0.0), axis=1, keepdims=True)
    position = (lax.broadcasted_iota(jnp.int32, (T, H), 0) + z * T).astype(F32) - begins
    angles = position * inverse[...]
    cos[...] = jnp.cos(angles)
    lane = lax.broadcasted_iota(jnp.int32, (T, H), 1)
    turned = jnp.sin(angles)
    sin[...] = jnp.where(lane < H // 2, -turned, turned)

    own_rows = pl.ds(reach * T, T)
    l_kw.wait()
    l_vw.wait()
    def kv_copy(r, c):
        lanes = pl.ds(c * 2 * H, 2 * H)
        return remote(
            s.kv.at[pl.ds((reach - r + 1) * T, T), lanes], s.kv.at[pl.ds((reach - r) * T, T), lanes],
            s.kv_s.at[r - 1, c], s.kv_r.at[r - 1, c], ctx=z + 1,
        )

    def kv_send(r, c):
        @pl.when((z < n - 1) & (z >= r - 1))
        def _():
            kv_copy(r, c).start()

    for h in range(KH):
        hs = pl.ds(h * H, H)
        raw = dot(s.x1[...], s.kw[:, hs])
        s.k_raw[:, hs] = raw
        s.kv[own_rows, 2 * h * H : (2 * h + 1) * H] = rope(raw * rms(raw) * gk[...]).astype(BF16)
        s.kv[own_rows, (2 * h + 1) * H : (2 * h + 2) * H] = dot(s.x1[...], s.vw[:, hs]).astype(BF16)
        kv_send(1, h)
    for r in range(1, reach + 1):

        @pl.when(z < r)
        def _():
            s.kv[pl.ds((reach - r) * T, T), :] = jnp.zeros((T, 2 * KV), BF16)

    l_qw.wait()
    s.q_raw[...] = dot(s.x1[...], s.qw[...])
    for h in range(QH):
        raw = s.q_raw[:, h * H : (h + 1) * H]
        s.q_rot[:, h * H : (h + 1) * H] = rope(raw * rms(raw) * gq[...]).astype(BF16)
    for r in range(1, reach + 1):
        for c in range(KH):

            @pl.when(z >= r)
            def _(r=r, c=c):
                kv_copy(r, c).wait_recv()

            if r < reach:
                kv_send(r + 1, c)
    rows_i = lax.broadcasted_iota(jnp.int32, (T, span), 0) + reach * T
    cols_i = lax.broadcasted_iota(jnp.int32, (T, span), 1)
    kseg_f = s.segs[:, pl.ds(pl.multiple_of(z * T, T), span)].astype(F32)
    allowed = (cols_i <= rows_i) & (qseg_f == kseg_f)
    s.mask[...] = jnp.where(allowed, 1.0, 0.0).astype(F32)

    def weights_of(h, g):
        hs = pl.ds(pl.multiple_of(h * H, H), H)
        q = s.q_rot[:, hs]
        k = s.kv[:, pl.ds(pl.multiple_of(2 * g * H, H), H)]
        return q, k, jnp.where(s.mask[...] > 0.0, jnp.exp(dot_nt(q, k) * inv_root), 0.0)

    def attend(h, _):
        g = h // group
        hs = pl.ds(pl.multiple_of(h * H, H), H)
        _q, _k, w = weights_of(h, g)
        v = s.kv[:, pl.ds(pl.multiple_of((2 * g + 1) * H, H), H)]
        total = jnp.sum(w, axis=-1, keepdims=True)
        att = dot(w.astype(BF16), v) / total
        s.tot[:, hs] = jnp.broadcast_to(total, (T, H))
        s.att[:, hs] = att
        s.att_low[:, hs] = att.astype(BF16)
        s.attt[hs, :] = att.T.astype(BF16)
        return 0

    lax.fori_loop(0, QH, attend, 0)

    l_ow.wait()

    def body(c, w):
        s.send_a[:, pl.ds(c, w)] = dot(s.att_low[...], s.ow[:, pl.ds(c, w)]).astype(BF16)

    tiles(D, TILE, body)
    scatter_start(0, s.send_a, s.recv0)

    def transpose_half(src, dst, place):
        for d in range(2):

            def body(c, w):
                cs = pl.ds(pl.multiple_of((d * n + zh * nl) * R + c, 128), w)
                rows = pl.ds(pl.multiple_of(d * nl * R + c, 128), w)
                dst[rows, place * T : (place + 1) * T] = src[:, cs].astype(F32).T.astype(BF16)

            tiles(nl * R, TILE, body)

    s.cotshare[...] = s.cot[mine, :].astype(F32)

    transpose_half(s.x1, s.x1t, 0)
    transpose_half(s.cot, s.cott, 0)
    l_dw.wait()

    def hidden_grad(cot, out):
        def body(c, w):
            out[:, pl.ds(c, w)] = dot_nt(cot[...], s.dw[pl.ds(c, w), :])

        tiles(F, TILE, body)

    def cot_share():
        mirror(0, s.cot, s.cot2).wait_recv()
        gather_start(9, s.cot2)

    hidden_grad(s.cot, s.gh)
    pl.when(z == nl - 1)(lambda: mirror(0, s.cot, s.cot2).start())

    s.resid[...] = scatter_sum(0, s.send_a, s.recv0, s.tokshare[...])
    resid = s.resid[...]
    s.x2[mine, :] = (resid * rms(resid) * g2[...]).astype(BF16)
    gather_start(1, s.x2)
    mirror(1, s.x2, s.x2b).start()
    pl.when(z < nl - 1)(lambda: mirror(0, s.cot, s.cot2).start())
    l_gw.wait()
    l_uw.wait()
    gather_forward(1, s.x2)
    gather_wait(1, s.x2)

    def mirrored_share():
        mirror(1, s.x2, s.x2b).wait_recv()
        gather_start(10, s.x2b)

    pl.when(zh == 1)(mirrored_share)
    pl.when(zh == 0)(cot_share)

    def feed(x, grad_hidden, place):
        rows = pl.ds(place * T, T)

        def body(c, w):
            cs = pl.ds(c, w)
            gate = dot(x[...], s.gw[:, cs])
            up = dot(x[...], s.uw[:, cs])
            gh = grad_hidden[:, cs]
            sig = jax.nn.sigmoid(gate)
            act = gate * sig
            s.hid[rows, cs] = (act * up).astype(BF16)
            s.gg[rows, cs] = (gh * up * (sig * (1.0 + gate * (1.0 - sig)))).astype(BF16)
            s.gu[rows, cs] = (gh * act).astype(BF16)

        tiles(F, TILE, body)

    feed(s.x2, s.gh, 0)
    pl.when(zh == 0)(mirrored_share)
    pl.when(zh == 1)(cot_share)
    pl.when(zh == 0)(lambda: gather_forward(9, s.cot2))
    pl.when(zh == 1)(lambda: gather_forward(10, s.x2b))
    gather_line_start(2, s.attt, att_all)
    for d in range(2):
        mirror_x1(d).start()
    own_part = pl.ds(0, T)

    def body(c, w):
        rs = pl.ds(c, w)
        s.send_a[:, rs] = (
            dot_nt(s.gg[own_part, :], s.gw[rs, :]) + dot_nt(s.gu[own_part, :], s.uw[rs, :])
        ).astype(BF16)

    tiles(D, TILE, body)
    transpose_half(s.x2, s.xt, 0)
    pl.when(zh == 0)(lambda: gather_forward(10, s.x2b))
    pl.when(zh == 1)(lambda: gather_forward(9, s.cot2))
    mirror(1, s.x2, s.x2b).wait_send()
    scatter_start(2, s.send_a, s.recv1)

    def body(c, w):
        s.send_b[:, pl.ds(c, w)] = dot(s.hid[own_part, :], s.dw[:, pl.ds(c, w)]).astype(BF16)

    tiles(D, TILE, body)
    gather_wait(9, s.cot2)
    hidden_grad(s.cot2, s.gh2)
    transpose_half(s.cot2, s.cott, 1)
    gather_wait(10, s.x2b)
    feed(s.x2b, s.gh2, 1)
    transpose_half(s.x2b, s.xt, 1)
    gather_line_step(2, att_all, 1)
    pl.semaphore_signal(s.credit, inc=1, device_id={"dp": 1 - dp}, device_id_type=MESH)

    grad_second = scatter_sum(2, s.send_a, s.recv1, jnp.zeros((S, D), F32))
    resid = s.resid[...]
    scale = rms(resid)
    normed = resid * scale
    s.gains[:, D : 2 * D] = jnp.sum(grad_second * normed, axis=0, keepdims=True)
    scaled = grad_second * g2[...]
    inner = jnp.mean(scaled * normed, axis=-1, keepdims=True)
    s.gresid[...] = s.cotshare[...] + scale * (scaled - normed * inner)
    s.gm[mine, :] = s.gresid[...].astype(BF16)
    gather_start(4, s.gm)
    columns_start(2, s.gm, s.gmc)

    class WeightJob:
        def __init__(self, k, left, grad):
            self.k, self.left, self.grad, self.cols = k, left, grad, grad.shape[1]

        def part(self, block, c, w):
            rows = pl.ds(pl.multiple_of(block * R, R), R)
            return dot(self.left[rows, :], self.grad[:, pl.ds(c, w)])

        def dp_slot(self, b):
            return s.gw.at[pl.ds(b * R, R), pl.ds(0, self.cols)]

        def dp_recv(self, b):
            return s.uw.at[pl.ds(pl.multiple_of((self.k * nl + b) * R, R), R), pl.ds(0, self.cols)]

        def chain_slot(self, up, step):
            i = nl + self.k * (nl - 1) + (step if up else nl - 2 - step)
            return s.gw.at[pl.ds(i * R, R), pl.ds(0, self.cols)]

        def chain(self, up, step):
            return s.chain.at[self.k, 0 if up or nl == 2 else 1, step, :, pl.ds(0, self.cols)]

    jobs = [
        WeightJob(0, s.cott, s.hid),
        WeightJob(1, s.xt, s.gg),
        WeightJob(2, s.xt, s.gu),
        WeightJob(3, s.x1t, s.dqkv),
    ]
    order = [b for i in range((nl + 1) // 2) for b in dict.fromkeys((nl - 1 - i, i))]

    def job_dp(k):
        for b in order:
            if k:
                job_dp_wait_send(jobs[k - 1], k - 1, b)
            job_dp_start(jobs[k], k, b)

    pl.semaphore_wait(s.credit, 1)
    job_dp(0)
    job_dp_wait_all(jobs[0], 0)
    chain_step(jobs[0], 0, 0, (True, False), (0,))
    chain_step(jobs[0], 0, 0, (True,), (1,))
    pl.when(zh == 0)(lambda: chain_step(jobs[0], 0, 0, (False,), (1,)))
    gather_forward(4, s.gm)
    job_dp(1)
    gather_wait(4, s.gm)
    scatter_start(3, s.send_b, s.recv2)
    for d in range(2):
        mirror_x1(d).wait_recv()

    def body(c, w):
        s.x1t[pl.ds(c, w), T : 2 * T] = s.x1b[:, pl.ds(c, w)].astype(F32).T.astype(BF16)

    tiles(D // 2, TILE, body)

    gatt = s.gh.at[:, pl.ds(0, QH * H)]

    def body(c, w):
        gatt[:, pl.ds(c, w)] = dot_nt(s.gm[...], s.ow[pl.ds(c, w), :])

    tiles(QH * H, TILE, body)
    s.gq_acc[...] = jnp.zeros((1, H), F32)

    def back(g, _):
        ks = pl.ds(pl.multiple_of(g * H, H), H)
        vs = pl.ds(pl.multiple_of(KV + g * H, H), H)
        v = s.kv[:, pl.ds(pl.multiple_of((2 * g + 1) * H, H), H)]
        grad_k = jnp.zeros((span, H), F32)
        grad_v = jnp.zeros((span, H), F32)
        for i in range(group):
            h = g * group + i
            hs = pl.ds(pl.multiple_of(h * H, H), H)
            q, k, w = weights_of(h, g)
            ga, total = gatt[:, hs], s.tot[:, hs]
            gs = (ga / total).astype(BF16)
            delta = jnp.sum(ga * s.att[:, hs], axis=-1, keepdims=True) / total[:, :1]
            ds = (w * (dot_nt(gs, v) - delta)).astype(BF16)
            grad_k = grad_k + dot_tn(ds, q) * inv_root
            grad_v = grad_v + dot_tn(w.astype(BF16), gs)
            gr = rope_back(dot(ds, k) * inv_root)
            raw = s.q_raw[:, hs]
            r = rms(raw)
            nq = raw * r
            s.gq_acc[...] += jnp.sum(gr * nq, axis=0, keepdims=True)
            sc = gr * gq[...]
            s.dqkv[:T, hs] = (r * (sc - nq * jnp.mean(sc * nq, axis=-1, keepdims=True))).astype(BF16)
        s.dkv[:, ks] = grad_k.astype(BF16)
        s.dkv[:, vs] = grad_v.astype(BF16)
        return 0

    lax.fori_loop(0, KH, back, 0)
    s.gains[:, 2 * D : 2 * D + H] = s.gq_acc[...]

    def dkv_copy(i):
        return remote(
            s.dkv.at[pl.ds(i * T, T)], s.dkv_in.at[i], s.dkv_s.at[i], s.dkv_r.at[i], ctx=z - 1
        )

    for i in range(reach):
        if i:

            @pl.when((z < n - 1) & (z + 1 >= reach - i + 1))
            def _():
                dkv_copy(i - 1).wait_recv()
                rows = pl.ds(i * T, T)
                s.dkv[rows, :] = (s.dkv[rows, :].astype(F32) + s.dkv_in[i - 1].astype(F32)).astype(BF16)

        @pl.when(z >= reach - i)
        def _():
            dkv_copy(i).start()

        if i == 0:
            job_dp_wait_all(jobs[1], 1)
            chain_step(jobs[1], 1, 0, (True,))
            job_dp(2)

    pl.when(zh == 1)(lambda: chain_step(jobs[0], 0, 0, (False,), (1,)))

    @pl.when(z < n - 1)
    def _():
        dkv_copy(reach - 1).wait_recv()

    own = s.dkv[pl.ds(reach * T, T), :].astype(F32)
    own = own + jnp.where(z < n - 1, s.dkv_in[reach - 1].astype(F32), 0.0)
    s.dqkv[:T, QH * H + KV :] = own[:, KV:].astype(BF16)
    gk_sum = jnp.zeros((1, H), F32)
    for h in range(KH):
        gr = rope_back(own[:, h * H : (h + 1) * H])
        raw = s.k_raw[:, h * H : (h + 1) * H]
        r = rms(raw)
        nk = raw * r
        gk_sum = gk_sum + jnp.sum(gr * nk, axis=0, keepdims=True)
        sc = gr * gk[...]
        s.dqkv[:T, QH * H + h * H : QH * H + (h + 1) * H] = (
            r * (sc - nk * jnp.mean(sc * nk, axis=-1, keepdims=True))
        ).astype(BF16)
    s.gains[:, 2 * D + H :] = gk_sum
    mirror_qkv().start()
    chain_step(jobs[1], 1, 0, (False,))
    gather_line_step(2, att_all, 2)
    job_dp_wait_all(jobs[2], 2)
    chain_step(jobs[2], 2, 0)

    q_c, k_c, v_c = pl.ds(0, QH * H), pl.ds(QH * H, KV), pl.ds(QH * H + KV, KV)

    def body(c, w):
        rs = pl.ds(c, w)
        s.send_a[:, rs] = (
            dot_nt(s.dqkv[:T, q_c], s.qw[rs, :])
            + dot_nt(s.dqkv[:T, k_c], s.kw[rs, :])
            + dot_nt(s.dqkv[:T, v_c], s.vw[rs, :])
        ).astype(BF16)

    tiles(D, TILE, body)
    scatter_start(6, s.send_a, s.recv3)
    s.outsh[...] = scatter_sum(3, s.send_b, s.recv2, s.resid[...]).astype(BF16)
    grad_first = scatter_sum(6, s.send_a, s.recv3, jnp.zeros((S, D), F32))
    tokshare = s.tokshare[...]
    scale = rms(tokshare)
    normed = tokshare * scale
    s.gains[:, :D] = jnp.sum(grad_first * normed, axis=0, keepdims=True)
    scaled = grad_first * g1[...]
    inner = jnp.mean(scaled * normed, axis=-1, keepdims=True)
    s.tgsh[...] = (s.gresid[...] + scale * (scaled - normed * inner)).astype(BF16)
    for j in range(1, nt):
        remote(s.gains, s.gains_p.at[j - 1], s.pl_s.at[8, j - 1], s.pl_r.at[8, j - 1], tensor=t ^ j).start()
    spread_start(7, s.tgsh, tgrad_hbm, 1)
    mirror_qkv().wait_recv()
    job_dp(3)
    job_dp_wait_all(jobs[3], 3)
    chain_step(jobs[3], 3, 0)
    for step in range(1, nl - 1):
        for k, job in enumerate(jobs):
            chain_step(job, k, step)

    columns_wait_recv(2, s.gm, s.gmc)
    share_start(2, s.gmc)
    spread_start(5, s.outsh, out_hbm, 0)
    for j in range(1, nt):
        remote(s.gains, s.gains_p.at[j - 1], s.pl_s.at[8, j - 1], s.pl_r.at[8, j - 1], tensor=t ^ j).wait()
    total = s.gains[...]
    for j in range(1, nt):
        total = total + s.gains_p[j - 1]
    s.gains2[...] = total

    def gain_copy(e, d):
        i = e * n + d
        return remote(
            s.gains2, s.gains_x.at[i - 1], s.ga_s.at[i], s.ga_r.at[i], dp=dp ^ e, ctx=lax.rem(z + d, n)
        )

    for e in range(2):
        for d in range(n):
            if e or d:
                gain_copy(e, d).start()
    stage = s.gh2.at[pl.ds(0, R), pl.ds(0, QH * H + 2 * KV)]

    def gate_copy():
        return pltpu.make_async_copy(s.gh.at[pl.ds(0, R)], gate_out, s.load_sem.at[2])

    def up_copy():
        return pltpu.make_async_copy(s.gh.at[pl.ds(0, R)], up_out, s.load_sem.at[3])

    def qkv_copies():
        parts = [(q_out, 0, QH * H), (k_out, QH * H, KV), (v_out, QH * H + KV, KV)]
        return [
            pltpu.make_async_copy(stage.at[:, pl.ds(a, w)], ref, s.load_sem.at[6 + i])
            for i, (ref, a, w) in enumerate(parts)
        ]

    rows = pl.ds(0, R)
    chain_final(jobs[0], 0, s.gh.at[rows])
    width = min(256, F)
    flip = s.gh2.at[:, pl.ds(QH * H + 2 * KV, 2 * R)]

    def down_copy(i):
        return pltpu.make_async_copy(
            flip.at[pl.ds(0, width), pl.ds((i % 2) * R, R)],
            down_out.at[pl.ds(i * width, width)],
            s.load_sem.at[4 + i % 2],
        )

    count = F // width
    for i in range(count):
        if i >= 2:
            down_copy(i - 2).wait()
        flip[:width, (i % 2) * R : (i % 2 + 1) * R] = s.gh[rows, i * width : (i + 1) * width].T
        down_copy(i).start()
    for i in range(max(0, count - 2), count):
        down_copy(i).wait()
    for step in range(3, n):
        gather_line_step(2, att_all, step)
    gather_line_finish(2, s.attt, att_all)
    share_wait(2, s.gmc)

    def load(i):
        slot = lax.rem(i, 2)
        return pltpu.make_async_copy(
            att_all.at[i // n, lax.rem(i, n)],
            s.dw.at[pl.ds(pl.multiple_of(slot * QH * H, QH * H), QH * H), pl.ds(0, T)],
            s.stage_sem.at[slot],
        )

    load(0).start()
    outw_out[...] = jnp.zeros(outw_out.shape, F32)

    def step(i, _):
        @pl.when(i + 1 < 2 * n)
        def _():
            load(i + 1).start()

        load(i).wait()
        slot = lax.rem(i, 2)
        left = s.dw[pl.ds(pl.multiple_of(slot * QH * H, QH * H), QH * H), pl.ds(0, T)]
        outw_out[...] += dot(left, s.gmc[:, i].reshape(T, R))
        return 0

    lax.fori_loop(0, 2 * n, step, 0)
    chain_final(jobs[1], 1, s.gh.at[rows])
    gate_copy().start()
    chain_final(jobs[3], 3, stage)
    for copy in qkv_copies():
        copy.start()
    gate_copy().wait()
    chain_final(jobs[2], 2, s.gh.at[rows])
    up_copy().start()
    for e in range(2):
        for d in range(n):
            if e or d:
                gain_copy(e, d).wait()
    total = s.gains2[...]
    for i in range(2 * n - 1):
        total = total + s.gains_x[i]
    gains_out[...] = total

    columns_wait_send(2, s.gm, s.gmc)
    mirror(0, s.cot, s.cot2).wait_send()
    mirror_qkv().wait_send()
    for d in range(2):
        mirror_x1(d).wait_send()
    for b in order:
        job_dp_wait_send(jobs[-1], len(jobs) - 1, b)
    for st in range(nl - 1):
        for k, job in enumerate(jobs):
            chain_wait_send(job, k, st)
    for r in range(1, reach + 1):

        @pl.when((z < n - 1) & (z >= r - 1))
        def _(r=r):
            for c in range(KH):
                kv_copy(r, c).wait_send()

    for i in range(reach):

        @pl.when(z >= reach - i)
        def _():
            dkv_copy(i).wait_send()

    spread_wait(5, s.outsh, out_hbm, 0)
    spread_wait(7, s.tgsh, tgrad_hbm, 1)
    up_copy().wait()
    for copy in qkv_copies():
        copy.wait()


def run_layer(dm, *operands):
    T, D, H, F, n, nt, reach, S, R = dm.T, dm.D, dm.H, dm.F, dm.n, dm.nt, dm.reach, dm.S, dm.R
    QC, KV = dm.QH * H, dm.KH * H
    span = (reach + 1) * T
    G = 2 * D + 2 * H
    dma = pltpu.SemaphoreType.DMA
    scratch = dict(
        tok=((T, D), BF16), x1=((T, D), BF16), send_b=((T, D), BF16), cot=((T, D), BF16), x2=((T, D), BF16),
        outsh=((S, D), BF16), tgsh=((S, D), BF16), xt=((D // 2, 2 * T), BF16), cott=((D // 2, 2 * T), BF16),
        cot2=((T, D), BF16), x2b=((T, D), BF16),
        qw=((D, QC), BF16), kw=((D, KV), BF16), vw=((D, KV), BF16), ow=((QC, D), BF16),
        gw=((D, F), BF16), uw=((D, F), BF16), dw=((F, D), BF16),
        tokshare=((S, D), F32), cotshare=((S, D), F32), resid=((S, D), F32), gresid=((S, D), F32),
        k_raw=((T, KV), F32), q_raw=((T, QC), F32), q_rot=((T, QC), BF16), kv=((span, 2 * KV), BF16),
        mask=((T, span), F32), tot=((T, QC), F32), att=((T, QC), F32), att_low=((T, QC), BF16),
        attt=((QC, T), BF16), gq_acc=((1, H), F32),
        recv0=((nt - 1, S, D), BF16), recv1=((nt - 1, S, D), BF16),
        gh=((T, F), F32), hid=((2 * T, F), BF16), gg=((2 * T, F), BF16), gu=((2 * T, F), BF16),
        dkv=((span, 2 * KV), BF16), dkv_in=((reach, T, 2 * KV), BF16), dqkv=((2 * T, QC + 2 * KV), BF16),
        chain=((4, 1 if n == 4 else 2, n // 2 - 1, R, F), BF16),

        gmc=((nt, 2 * n, S, R), BF16), x1b=((T, D // 2), BF16), x1t=((D // 2, 2 * T), BF16), gh2=((T, F), F32),
        cos=((T, H), F32), sin=((T, H), F32), segs=((1, reach * T + dm.L), jnp.int32),
        gain_in=((1, G), F32), gains=((1, G), F32), gains2=((1, G), F32), gains_p=((nt - 1, 1, G), F32),
        gains_x=((2 * n - 1, 1, G), F32),
    )
    sems = dict(
        load_sem=(9,), own_sem=(3,), pl_s=(13, nt - 1), pl_r=(13, nt - 1), ag_s=(3, 2, n - 1), ag_r=(3, 2, n - 1),
        agx_s=(3, 2 * n - 1), agx_r=(3, 2 * n - 1), aa_s=(3, 2 * n), aa_r=(3, 2 * n), stage_sem=(2,),
        dp_s=(4, n // 2), dp_r=(4, n // 2), ch_s=(4, 2, n // 2 - 1, 2), ch_r=(4, 2, n // 2 - 1, 2), mi_s=(5,), mi_r=(5,), kv_s=(reach, KV // H), kv_r=(reach, KV // H), pl2_s=(11,), pl2_r=(11,),
        dkv_s=(reach,), dkv_r=(reach,), ga_s=(2 * n,), ga_r=(2 * n,),
    )
    names = list(scratch) + list(sems) + ["credit"]
    shapes = [pltpu.VMEM(*v) for v in scratch.values()] + [dma(v) for v in sems.values()]
    shapes.append(pltpu.SemaphoreType.REGULAR)

    def body(*refs):
        fixed = len(refs) - len(names)
        s = Dims()
        for name, ref in zip(names, refs[fixed:]):
            setattr(s, name, ref)
        for alias, of in dm.alias.items():
            setattr(s, alias, getattr(s, of))
        layer_kernel(dm, *refs[:fixed], s)

    hbm = pl.BlockSpec(memory_space=pl.ANY)
    vmem = pl.BlockSpec(memory_space=pltpu.VMEM)
    return pl.pallas_call(
        body,
        out_shape=(
            jax.ShapeDtypeStruct((T, D), BF16),
            jax.ShapeDtypeStruct((T, D), BF16),
            jax.ShapeDtypeStruct((R, F), F32),
            jax.ShapeDtypeStruct((R, F), F32),
            jax.ShapeDtypeStruct((F, R), F32),
            jax.ShapeDtypeStruct((R, QC), F32),
            jax.ShapeDtypeStruct((R, KV), F32),
            jax.ShapeDtypeStruct((R, KV), F32),
            jax.ShapeDtypeStruct((QC, R), F32),
            jax.ShapeDtypeStruct((1, G), F32),
            jax.ShapeDtypeStruct((2, n, QC, T), BF16),
        ),
        in_specs=[hbm] * 2 + [vmem] * 6 + [hbm] * 7,
        out_specs=[hbm] * 8 + [vmem] * 2 + [hbm],
        scratch_shapes=shapes,
        compiler_params=pltpu.CompilerParams(
            collective_id=0, has_side_effects=True, vmem_limit_bytes=67043328
        ),
        name="layer",
    )(*operands)


def finish_kernel(dm, *refs):
    count = len(dm.finish)
    ins, gains, outs = refs[:count], refs[count], refs[count + 1 : 2 * count + 1]
    gain_outs = refs[2 * count + 1 : 2 * count + 5]
    bufs, load_sem, store_sem = refs[2 * count + 5 : 3 * count + 5], refs[-2], refs[-1]
    loads = [pltpu.make_async_copy(a, b, load_sem.at[i]) for i, (a, b) in enumerate(zip(ins, bufs))]
    stores = [pltpu.make_async_copy(b, c, store_sem.at[i]) for i, (b, c) in enumerate(zip(bufs, outs))]
    for load in loads:
        load.start()
    place = 0
    for ref in gain_outs:
        ref[...] = gains[:, place : place + ref.shape[1]]
        place += ref.shape[1]
    for load, store in zip(loads, stores):
        load.wait()
        store.start()
    for store in stores:
        store.wait()


def finish(dm, arrays, gains):
    dm.finish = arrays
    hbm = pl.BlockSpec(memory_space=pl.ANY)
    vmem = pl.BlockSpec(memory_space=pltpu.VMEM)
    shapes = [jax.ShapeDtypeStruct(a.shape, a.dtype) for a in arrays]
    gain_shapes = [jax.ShapeDtypeStruct((1, w), F32) for w in (dm.D, dm.D, dm.H, dm.H)]
    dma = pltpu.SemaphoreType.DMA((len(arrays),))
    return pl.pallas_call(
        functools.partial(finish_kernel, dm),
        out_shape=tuple(shapes + gain_shapes),
        in_specs=[hbm] * len(arrays) + [vmem],
        out_specs=tuple([hbm] * len(arrays) + [vmem] * 4),
        scratch_shapes=[pltpu.VMEM(a.shape, a.dtype) for a in arrays] + [dma, dma],
        compiler_params=pltpu.CompilerParams(vmem_limit_bytes=67043328),
        name="finish",
    )(*arrays, gains)


def per_device(
    tokens,
    segments,
    first_gain,
    query_weight,
    key_matrix,
    value_matrix,
    query_norm_gain,
    key_gain,
    output_weight,
    second_gain,
    gate_weight,
    up_weight,
    down_weight,
    cotangent,
):
    _, T, D = tokens.shape
    dm = Dims()
    dm.T, dm.D, dm.H, dm.F = T, D, query_norm_gain.shape[0], gate_weight.shape[1]
    dm.QH, dm.KH = query_weight.shape[1] // dm.H, key_matrix.shape[1] // dm.H
    dm.n, dm.nt = lax.axis_size("ctx"), lax.axis_size("tensor")
    length = segments.shape[1]
    dm.reach = -(-(length // 2 - 1) // T)
    dm.S, dm.R = T // dm.nt, D // (2 * dm.n)
    dm.alias = {"send_a": "tok", "gm": "x2", "recv2": "recv0", "recv3": "recv1"}
    H = dm.H
    dm.L = length
    inverse = (1.0 / rope_base ** (np.arange(0, H, 2, dtype=np.float32) / np.float32(H))).astype(np.float32)
    inverse = np.concatenate([inverse, inverse])[None]
    out, tgrad, gate_g, up_g, down_g, q_g, k_g, v_g, out_g, gains = run_layer(
        dm,
        tokens.reshape(T, D),
        cotangent.reshape(T, D),
        first_gain.reshape(-1, H),
        second_gain.reshape(-1, H),
        query_norm_gain.reshape(1, H),
        key_gain.reshape(1, H),
        inverse,
        segments,
        query_weight,
        key_matrix,
        value_matrix,
        output_weight,
        gate_weight,
        up_weight,
        down_weight,
    )[:10]
    out, tgrad, gate_g, up_g, down_g, q_g, k_g, v_g, out_g, first_g, second_g, qn_g, kn_g = finish(
        dm, (out, tgrad, gate_g, up_g, down_g, q_g, k_g, v_g, out_g), gains
    )
    return (
        out.reshape(tokens.shape),
        tgrad.reshape(tokens.shape),
        first_g.reshape(D),
        q_g,
        k_g,
        v_g,
        qn_g.reshape(H),
        kn_g.reshape(H),
        out_g,
        second_g.reshape(D),
        gate_g,
        up_g,
        down_g,
    )


def solution(mesh):
    return jax.shard_map(
        per_device,
        mesh=mesh,
        in_specs=(
            P("dp", "ctx", None),
            P("dp", None),
            P(),
            P(None, "tensor"),
            P(None, "tensor"),
            P(None, "tensor"),
            P(),
            P(),
            P("tensor", None),
            P(),
            P(None, "tensor"),
            P(None, "tensor"),
            P("tensor", None),
            P("dp", "ctx", None),
        ),
        out_specs=(
            P("dp", "ctx", None),
            P("dp", "ctx", None),
            P(),
            P(("dp", "ctx"), "tensor"),
            P(("dp", "ctx"), "tensor"),
            P(("dp", "ctx"), "tensor"),
            P(),
            P(),
            P("tensor", ("dp", "ctx")),
            P(),
            P(("dp", "ctx"), "tensor"),
            P(("dp", "ctx"), "tensor"),
            P("tensor", ("dp", "ctx")),
        ),
        check_vma=False,
    )
```

```python
import functools
import math

import jax
import jax.numpy as jnp
import numpy as np
from jax import lax
from jax.experimental import pallas as pl
from jax.experimental.pallas import tpu as pltpu
from jax.sharding import PartitionSpec as P

epsilon = 1e-06
rope_base = 1000000.0
F32 = jnp.float32
BF16 = jnp.bfloat16
MESH = pl.DeviceIdType.MESH
TILE = 256


def dot(a, b):
    return jnp.dot(a, b, preferred_element_type=F32)


def dot_nt(a, b):
    return lax.dot_general(a, b, (((1,), (1,)), ((), ())), preferred_element_type=F32)


def dot_tn(a, b):
    return lax.dot_general(a, b, (((0,), (0,)), ((), ())), preferred_element_type=F32)


def remote(src, dst, send_sem, recv_sem, **device):
    return pltpu.make_async_remote_copy(
        src_ref=src,
        dst_ref=dst,
        send_sem=send_sem,
        recv_sem=recv_sem,
        device_id=device,
        device_id_type=MESH,
    )


def tiles(total, size, body):
    size = min(size, total)

    def step(i, _):
        body(pl.multiple_of(i * size, size), size)
        return 0

    lax.fori_loop(0, total // size, step, 0)


class Dims:
    pass


def layer_kernel(
    dm,
    tok_hbm,
    cot_hbm,
    first_in,
    second_in,
    query_in,
    key_in,
    inverse,
    seg_row,
    qw_hbm,
    kw_hbm,
    vw_hbm,
    ow_hbm,
    gw_hbm,
    uw_hbm,
    dw_hbm,
    out_hbm,
    tgrad_hbm,
    gate_out,
    up_out,
    down_out,
    q_out,
    k_out,
    v_out,
    outw_out,
    gains_out,
    att_all,
    s,
):
    T, D, H, QH, KH, F, n, nt, reach, S, R = (
        dm.T, dm.D, dm.H, dm.QH, dm.KH, dm.F, dm.n, dm.nt, dm.reach, dm.S, dm.R,
    )
    group = QH // KH
    span = (reach + 1) * T
    KV = KH * H
    inv_root = 1.0 / math.sqrt(H)
    C = R // nt
    gain_in = s.gain_in
    for place, ref in ((0, first_in), (D, second_in), (2 * D, query_in), (2 * D + H, key_in)):
        for i in range(ref.shape[0]):
            gain_in[:, place + i * H : place + (i + 1) * H] = ref[i : i + 1, :].astype(F32)
    g1 = gain_in.at[:, pl.ds(0, D)]
    g2 = gain_in.at[:, pl.ds(D, D)]
    gq = gain_in.at[:, pl.ds(2 * D, H)]
    gk = gain_in.at[:, pl.ds(2 * D + H, H)]
    cos, sin = s.cos, s.sin
    dp, z, t = lax.axis_index("dp"), lax.axis_index("ctx"), lax.axis_index("tensor")
    zz = n - 1 - z
    nl = n // 2
    zh, zl = z // nl, lax.rem(z, nl)
    zzl = nl - 1 - zl

    barrier = pltpu.get_barrier_semaphore()
    for j in range(1, nt):
        pl.semaphore_signal(barrier, inc=1, device_id={"tensor": t ^ j}, device_id_type=MESH)
    for e in range(2):
        for d in range(n):
            if e or d:
                pl.semaphore_signal(
                    barrier,
                    inc=1,
                    device_id={"dp": dp ^ e, "ctx": lax.rem(z + d, n)},
                    device_id_type=MESH,
                )

    loads = [
        (tok_hbm, s.tok), (cot_hbm, s.cot), (kw_hbm, s.kw), (vw_hbm, s.vw), (qw_hbm, s.qw),
        (ow_hbm, s.ow), (dw_hbm, s.dw), (gw_hbm, s.gw), (uw_hbm, s.uw),
    ]
    loads = [pltpu.make_async_copy(a, b, s.load_sem.at[i]) for i, (a, b) in enumerate(loads)]
    for load in loads:
        load.start()
    (l_tok, l_cot, l_kw, l_vw, l_qw, l_ow, l_dw, l_gw, l_uw) = loads

    def scatter_direct(k, buf, recv, j):
        peer = t ^ j
        return remote(
            buf.at[pl.ds(pl.multiple_of(peer * S, S), S)], recv.at[j - 1],
            s.pl_s.at[k, j - 1], s.pl_r.at[k, j - 1], tensor=peer,
        )

    def scatter_first(k, buf, recv, slot):
        to = t ^ (1 if slot < 2 else 2)
        rows = pl.ds(pl.multiple_of((to if slot % 2 == 0 else t ^ 3) * S, S), S)
        cols = pl.ds(0 if slot < 2 else D // 2, D // 2)
        return remote(buf.at[rows, cols], recv.at[slot], s.rs_s.at[k, slot], s.rs_r.at[k, slot], tensor=to)

    def scatter_second(k, recv, slot):
        to = t ^ (2 if slot == 4 else 1)
        return remote(s.pair.at[slot - 4], recv.at[slot], s.rs_s.at[k, slot], s.rs_r.at[k, slot], tensor=to)

    def scatter_start(k, buf, recv):
        if nt == 4:
            for slot in (1, 3, 0, 2):
                scatter_first(k, buf, recv, slot).start()
        else:
            for j in range(1, nt):
                scatter_direct(k, buf, recv, j).start()

    def scatter_sum(k, buf, recv, base):
        own = pl.ds(pl.multiple_of(t * S, S), S)
        if nt == 4:
            for slot, peer, cols in ((1, t ^ 2, slice(0, D // 2)), (3, t ^ 1, slice(D // 2, D))):
                scatter_first(k, buf, recv, slot).wait_recv()
                rows = pl.ds(pl.multiple_of(peer * S, S), S)
                both = buf[rows, cols].astype(F32) + recv[slot].astype(F32)
                s.pair[slot // 2] = both.astype(BF16)
                scatter_second(k, recv, 4 + slot // 2).start()
            for slot in (0, 2):
                scatter_first(k, buf, recv, slot).wait_recv()
            for slot in range(4):
                scatter_first(k, buf, recv, slot).wait_send()
            for slot in (4, 5):
                scatter_second(k, recv, slot).wait()
            left = buf[own, 0 : D // 2].astype(F32) + recv[0].astype(F32) + recv[4].astype(F32)
            right = buf[own, D // 2 : D].astype(F32) + recv[2].astype(F32) + recv[5].astype(F32)
            return base + jnp.concatenate([left, right], axis=1)
        for j in range(1, nt):
            scatter_direct(k, buf, recv, j).wait()
        total = base + buf[own, :].astype(F32)
        for j in range(1, nt):
            total = total + recv[j - 1].astype(F32)
        return total

    def rows_of(peer, half=None):
        if half is None:
            return pl.ds(pl.multiple_of(peer * S, S), S)
        return pl.ds(pl.multiple_of(peer * S + half * (S // 2), S // 2), S // 2)

    def gather_copy(k, full, j):
        rows = rows_of(t)
        return remote(full.at[rows], full.at[rows], s.pl_s.at[k, j - 1], s.pl_r.at[k, j - 1], tensor=t ^ j)

    def gather_arrived(k, full, j):
        rows = rows_of(t ^ j)
        return remote(full.at[rows], full.at[rows], s.pl_s.at[k, j - 1], s.pl_r.at[k, j - 1], tensor=t ^ j)

    def relay_copy(k, full, origin, half, to):
        rows = rows_of(origin, half)
        sems = (s.pl2_s.at[k], s.pl2_r.at[k]) if half else (s.pl_s.at[k, 2], s.pl_r.at[k, 2])
        return remote(full.at[rows], full.at[rows], *sems, tensor=to)

    def gather_start(k, full):
        for j in range(1, nt) if nt != 4 else (1, 2):
            gather_copy(k, full, j).start()

    def gather_forward(k, full):
        if nt == 4:
            gather_arrived(k, full, 1).wait_recv()
            relay_copy(k, full, t ^ 1, 0, t ^ 2).start()
            gather_arrived(k, full, 2).wait_recv()
            relay_copy(k, full, t ^ 2, 1, t ^ 1).start()

    def gather_wait(k, full):
        for j in range(1, nt) if nt != 4 else (1, 2):
            gather_copy(k, full, j).wait_send()
            if nt != 4:
                gather_arrived(k, full, j).wait_recv()
        if nt == 4:
            relay_copy(k, full, t ^ 1, 0, t ^ 2).wait_send()
            relay_copy(k, full, t ^ 2, 1, t ^ 1).wait_send()
            relay_copy(k, full, t ^ 3, 0, t ^ 2).wait_recv()
            relay_copy(k, full, t ^ 3, 1, t ^ 1).wait_recv()

    mine = pl.ds(pl.multiple_of(t * S, S), S)

    def spread_start(k, share, full, own):
        own_copy(share, full, own).start()
        for j in range(1, nt):
            remote(
                share, full.at[mine], s.pl_s.at[k, j - 1], s.pl_r.at[k, j - 1], tensor=t ^ j
            ).start()

    def own_copy(share, full, own):
        return pltpu.make_async_copy(share, full.at[mine], s.load_sem.at[own])

    def spread_wait(k, share, full, own):
        own_copy(share, full, own).wait()
        for j in range(1, nt):
            peer = t ^ j
            theirs = pl.ds(pl.multiple_of(peer * S, S), S)
            copy = remote(share, full.at[theirs], s.pl_s.at[k, j - 1], s.pl_r.at[k, j - 1], tensor=peer)
            copy.wait_send()
            copy.wait_recv()

    def mirror(i, src, dst):
        return remote(src.at[mine], dst.at[mine], s.mi_s.at[i], s.mi_r.at[i], ctx=zz)

    def mirror_x1(d):
        cols = pl.ds(pl.multiple_of((d * n + (1 - zh) * nl) * R, 128), nl * R)
        return remote(
            s.x1.at[:, cols], s.x1b.at[:, pl.ds(d * nl * R, nl * R)], s.mi_s.at[2 + d], s.mi_r.at[2 + d], ctx=zz
        )

    def mirror_qkv():
        return remote(
            s.dqkv.at[pl.ds(0, T)], s.dqkv.at[pl.ds(T, T)], s.mi_s.at[4], s.mi_r.at[4], ctx=zz
        )

    def line_copy(k, all_ref, up, step, src=None):
        idx = (z - step) if up else (z + step)
        ref = all_ref.at[dp, idx]
        return remote(
            ref if src is None else src, ref,
            s.ag_s.at[k, 0 if up else 1, step], s.ag_r.at[k, 0 if up else 1, step],
            ctx=(z + 1) if up else (z - 1),
        )

    def core_copy(k, all_ref, slot, idx, src=None):
        ref = all_ref.at[dp, idx]
        return remote(
            ref if src is None else src, ref, s.agx_s.at[k, slot], s.agx_r.at[k, slot], dp=1 - dp
        )

    def gather_line_start(k, src, all_ref):
        pltpu.make_async_copy(src, all_ref.at[dp, z], s.own_sem.at[k]).start()

        @pl.when(z < n - 1)
        def _():
            line_copy(k, all_ref, True, 0, src).start()

        @pl.when(z > 0)
        def _():
            line_copy(k, all_ref, False, 0, src).start()

        core_copy(k, all_ref, 0, z, src).start()

    def gather_line_step(k, all_ref, step):
        @pl.when(z >= step)
        def _():
            ref = all_ref.at[dp, z - step]
            remote(ref, ref, s.ag_s.at[k, 0, step - 1], s.ag_r.at[k, 0, step - 1], ctx=z - 1).wait_recv()
            if step < n - 1:

                @pl.when(z < n - 1)
                def _():
                    line_copy(k, all_ref, True, step).start()

            core_copy(k, all_ref, step, z - step).start()

        @pl.when(zz >= step)
        def _():
            ref = all_ref.at[dp, z + step]
            remote(ref, ref, s.ag_s.at[k, 1, step - 1], s.ag_r.at[k, 1, step - 1], ctx=z + 1).wait_recv()
            if step < n - 1:

                @pl.when(z > 0)
                def _():
                    line_copy(k, all_ref, False, step).start()

            core_copy(k, all_ref, n - 1 + step, z + step).start()

    def gather_line_finish(k, src, all_ref):
        pltpu.make_async_copy(src, all_ref.at[dp, z], s.own_sem.at[k]).wait()
        for step in range(n - 1):

            @pl.when((z >= step) & (z < n - 1))
            def _():
                line_copy(k, all_ref, True, step, src).wait_send()

            @pl.when((zz >= step) & (z > 0))
            def _():
                line_copy(k, all_ref, False, step, src).wait_send()

        def both(slot, idx):
            ref = all_ref.at[1 - dp, idx]
            copy = remote(src, ref, s.agx_s.at[k, slot], s.agx_r.at[k, slot], dp=1 - dp)
            copy.wait_send()
            copy.wait_recv()

        both(0, z)
        for step in range(1, n):

            @pl.when(z >= step)
            def _():
                both(step, z - step)

            @pl.when(zz >= step)
            def _():
                both(n - 1 + step, z + step)

    me = dp * n + z

    def columns_src(k, src, block):
        if k < 2:
            rows = pl.ds(pl.multiple_of(lax.rem(block, n) * R + t * C, C), C)
            return src.at[rows, pl.ds(pl.multiple_of(block // n * T, T), T)]
        return src.at[mine, pl.ds(pl.multiple_of(block * R, R), R)]

    def columns_copy(k, src, all_ref, e, d):
        to_dp, to_z = dp ^ e, lax.rem(z + d, n)
        return remote(
            columns_src(k, src, to_dp * n + to_z), all_ref.at[t, me],
            s.aa_s.at[k, e * n + d], s.aa_r.at[k, e * n + d], dp=to_dp, ctx=to_z,
        )

    def columns_own(k, src, all_ref):
        return pltpu.make_async_copy(columns_src(k, src, me), all_ref.at[t, me], s.aa_s.at[k, 0])

    def columns_start(k, src, all_ref):
        columns_own(k, src, all_ref).start()
        for d in range(n):
            for e in range(2):
                if e or d:
                    columns_copy(k, src, all_ref, e, d).start()

    def columns_wait_send(k, src, all_ref):
        for e in range(2):
            for d in range(n):
                if e or d:
                    columns_copy(k, src, all_ref, e, d).wait_send()

    def columns_wait_recv(k, src, all_ref):
        columns_own(k, src, all_ref).wait()
        for e in range(2):
            for d in range(n):
                if e or d:
                    ref = all_ref.at[t, (dp ^ e) * n + lax.rem(z - d + n, n)]
                    remote(
                        columns_src(k, src, me), ref, s.aa_s.at[k, e * n + d], s.aa_r.at[k, e * n + d],
                        dp=dp ^ e, ctx=lax.rem(z - d + n, n),
                    ).wait_recv()

    def share_start(k, all_ref):
        for j in range(1, nt):
            remote(
                all_ref.at[t], all_ref.at[t], s.pl_s.at[10 + k, j - 1], s.pl_r.at[10 + k, j - 1], tensor=t ^ j
            ).start()

    def share_wait(k, all_ref):
        for j in range(1, nt):
            copy = remote(
                all_ref.at[t], all_ref.at[t ^ j], s.pl_s.at[10 + k, j - 1], s.pl_r.at[10 + k, j - 1], tensor=t ^ j
            )
            copy.wait_send()
            copy.wait_recv()

    def job_dp_start(job, k, b):
        slot = job.dp_slot(b)

        def body(c, w):
            slot[:, pl.ds(c, w)] = job.part((1 - dp) * nl + b, c, w).astype(BF16)

        tiles(job.cols, 512, body)
        remote(slot, job.dp_recv(b), s.dp_s.at[k, b], s.dp_r.at[k, b], dp=1 - dp).start()

    def job_dp_wait_send(job, k, b):
        remote(job.dp_slot(b), job.dp_recv(b), s.dp_s.at[k, b], s.dp_r.at[k, b], dp=1 - dp).wait_send()

    def job_dp_wait_all(job, k):
        for b in range(nl):
            remote(job.dp_slot(b), job.dp_recv(b), s.dp_s.at[k, b], s.dp_r.at[k, b], dp=1 - dp).wait_recv()

    def chain_copy(job, k, up, step, part):
        i = 0 if up else 1
        width = job.cols // 2
        cols = pl.ds(part * width, width)
        return remote(
            job.chain_slot(up, step).at[:, cols], job.chain(up, step).at[:, cols],
            s.ch_s.at[k, i, step, part], s.ch_r.at[k, i, step, part],
            ctx=(z + 1) if up else (z - 1),
        )

    def chain_step(job, k, step, ways=(True, False), parts=(0, 1)):
        width = job.cols // 2
        for part in parts:
            for up in ways:
                pos = zl if up else zzl

                @pl.when((pos <= step) & (pos < nl - 1))
                def _(up=up, pos=pos, part=part):
                    target = (zl + nl - 1 - step) if up else (zl - (nl - 1 - step))
                    slot = job.chain_slot(up, step)
                    if step:

                        @pl.when(pos >= 1)
                        def _():
                            chain_copy(job, k, up, step - 1, part).wait_recv()

                    def body(c, w):
                        cs = pl.ds(pl.multiple_of(part * width + c, 128), w)
                        total = job.part(dp * nl + target, cs.start, w)
                        total = total + job.dp_recv(target)[:, cs].astype(F32)
                        if step:
                            prev = job.chain(up, step - 1)[:, cs].astype(F32)
                            total = total + jnp.where(pos >= 1, prev, 0.0)
                        slot[:, cs] = total.astype(BF16)

                    tiles(width, 256 if width % 256 == 0 else 128, body)
                    chain_copy(job, k, up, step, part).start()

    def chain_wait_send(job, k, step):
        for up in (True, False):
            pos = zl if up else zzl

            @pl.when((pos <= step) & (pos < nl - 1))
            def _(up=up):
                for part in range(2):
                    chain_copy(job, k, up, step, part).wait_send()

    def chain_final(job, k, out_ref):
        width = job.cols // 2
        for part in range(2):
            for up in (True, False):
                pos = zl if up else zzl

                @pl.when(pos >= 1)
                def _(up=up, part=part):
                    chain_copy(job, k, up, nl - 2, part).wait_recv()

            def body(c, w):
                cs = pl.ds(pl.multiple_of(part * width + c, 128), w)
                total = job.part(dp * nl + zl, cs.start, w) + job.dp_recv(zl)[:, cs].astype(F32)
                a = job.chain(True, nl - 2)[:, cs].astype(F32)
                b = job.chain(False, nl - 2)[:, cs].astype(F32)
                out_ref[:, cs] = total + jnp.where(zl >= 1, a, 0.0) + jnp.where(zzl >= 1, b, 0.0)

            tiles(width, 256 if width % 256 == 0 else 128, body)

    L = seg_row.shape[1]
    s.segs[:, : reach * T] = jnp.full((1, reach * T), -1, jnp.int32)
    s.segs[:, reach * T :] = seg_row[...]
    row = seg_row[...]
    at_me = lax.broadcasted_iota(jnp.int32, (T, L), 1) == lax.broadcasted_iota(jnp.int32, (T, L), 0) + z * T
    row_f = jnp.broadcast_to(row.astype(F32), (T, L))
    qseg_f = jnp.sum(jnp.where(at_me, row_f, 0.0), axis=1, keepdims=True)
    begins = jnp.sum(jnp.where(row_f < qseg_f, 1.0, 0.0), axis=1, keepdims=True)
    position = (lax.broadcasted_iota(jnp.int32, (T, H), 0) + z * T).astype(F32) - begins
    angles = position * inverse[...]
    cos[...] = jnp.cos(angles)
    lane = lax.broadcasted_iota(jnp.int32, (T, H), 1)
    turned = jnp.sin(angles)
    sin[...] = jnp.where(lane < H // 2, -turned, turned)

    rows_i = lax.broadcasted_iota(jnp.int32, (T, span), 0) + reach * T
    cols_i = lax.broadcasted_iota(jnp.int32, (T, span), 1)
    kseg_f = s.segs[:, pl.ds(pl.multiple_of(z * T, T), span)].astype(F32)
    allowed = (cols_i <= rows_i) & (qseg_f == kseg_f)
    s.mask[...] = jnp.where(allowed, 1.0, 0.0).astype(F32)

    l_tok.wait()
    x = s.tok[...].astype(F32)
    scale = lax.rsqrt(jnp.mean(x * x, axis=-1, keepdims=True) + epsilon)
    s.x1[...] = (x * scale * g1[...]).astype(BF16)
    s.tokshare[...] = s.tok[mine, :].astype(F32)

    def rms(v):
        return lax.rsqrt(jnp.mean(v * v, axis=-1, keepdims=True) + epsilon)

    def rope(v):
        return v * cos[...] + pltpu.roll(v, H // 2, 1) * sin[...]

    def rope_back(g):
        return g * cos[...] + pltpu.roll(g * sin[...], H // 2, 1)

    own_rows = pl.ds(reach * T, T)
    l_kw.wait()
    l_vw.wait()
    def kv_copy(r, c):
        lanes = pl.ds(c * 2 * H, 2 * H)
        return remote(
            s.kv.at[pl.ds((reach - r + 1) * T, T), lanes], s.kv.at[pl.ds((reach - r) * T, T), lanes],
            s.kv_s.at[r - 1, c], s.kv_r.at[r - 1, c], ctx=z + 1,
        )

    def kv_send(r, c):
        @pl.when((z < n - 1) & (z >= r - 1))
        def _():
            kv_copy(r, c).start()

    for h in range(KH):
        hs = pl.ds(h * H, H)
        raw = dot(s.x1[...], s.kw[:, hs])
        s.k_raw[:, hs] = raw
        s.kv[own_rows, 2 * h * H : (2 * h + 1) * H] = rope(raw * rms(raw) * gk[...]).astype(BF16)
        s.kv[own_rows, (2 * h + 1) * H : (2 * h + 2) * H] = dot(s.x1[...], s.vw[:, hs]).astype(BF16)
        if h == 0:
            pl.semaphore_wait(barrier, (nt - 1) + (2 * n - 1))
        kv_send(1, h)
    l_cot.wait()
    pl.when(zh == 1)(lambda: mirror(0, s.cot, s.cot2).start())
    for r in range(1, reach + 1):

        @pl.when(z < r)
        def _():
            s.kv[pl.ds((reach - r) * T, T), :] = jnp.zeros((T, 2 * KV), BF16)

    l_qw.wait()
    s.q_raw[...] = dot(s.x1[...], s.qw[...])
    for h in range(QH):
        raw = s.q_raw[:, h * H : (h + 1) * H]
        s.q_rot[:, h * H : (h + 1) * H] = rope(raw * rms(raw) * gq[...]).astype(BF16)
    for r in range(1, reach + 1):
        for c in range(KH):

            @pl.when(z >= r)
            def _(r=r, c=c):
                kv_copy(r, c).wait_recv()

            if r < reach:
                kv_send(r + 1, c)
    def weights_of(h, g):
        hs = pl.ds(pl.multiple_of(h * H, H), H)
        q = s.q_rot[:, hs]
        k = s.kv[:, pl.ds(pl.multiple_of(2 * g * H, H), H)]
        return q, k, jnp.where(s.mask[...] > 0.0, jnp.exp(dot_nt(q, k) * inv_root), 0.0)

    def attend(h, _):
        g = h // group
        hs = pl.ds(pl.multiple_of(h * H, H), H)
        _q, _k, w = weights_of(h, g)
        v = s.kv[:, pl.ds(pl.multiple_of((2 * g + 1) * H, H), H)]
        total = jnp.sum(w, axis=-1, keepdims=True)
        att = dot(w.astype(BF16), v) / total
        s.tot[:, hs] = jnp.broadcast_to(total, (T, H))
        s.att[:, hs] = att
        s.att_low[:, hs] = att.astype(BF16)
        s.attt[hs, :] = att.T.astype(BF16)
        return 0

    lax.fori_loop(0, QH, attend, 0)

    l_ow.wait()

    def body(c, w):
        s.send_a[:, pl.ds(c, w)] = dot(s.att_low[...], s.ow[:, pl.ds(c, w)]).astype(BF16)

    tiles(D, TILE, body)
    scatter_start(0, s.send_a, s.recv0)

    def transpose_half(src, dst, place):
        for d in range(2):

            def body(c, w):
                cs = pl.ds(pl.multiple_of((d * n + zh * nl) * R + c, 128), w)
                rows = pl.ds(pl.multiple_of(d * nl * R + c, 128), w)
                dst[rows, place * T : (place + 1) * T] = src[:, cs].astype(F32).T.astype(BF16)

            tiles(nl * R, TILE, body)

    s.cotshare[...] = s.cot[mine, :].astype(F32)

    transpose_half(s.x1, s.x1t, 0)
    transpose_half(s.cot, s.cott, 0)
    l_dw.wait()

    def hidden_grad(cot, out):
        def body(c, w):
            out[:, pl.ds(c, w)] = dot_nt(cot[...], s.dw[pl.ds(c, w), :])

        tiles(F, TILE, body)

    def cot_share():
        mirror(0, s.cot, s.cot2).wait_recv()
        gather_start(9, s.cot2)

    hidden_grad(s.cot, s.gh)
    pl.when(z == nl - 1)(lambda: mirror(0, s.cot, s.cot2).start())

    s.resid[...] = scatter_sum(0, s.send_a, s.recv0, s.tokshare[...])
    resid = s.resid[...]
    s.x2[mine, :] = (resid * rms(resid) * g2[...]).astype(BF16)
    gather_start(1, s.x2)
    mirror(1, s.x2, s.x2b).start()
    l_gw.wait()
    l_uw.wait()
    gather_forward(1, s.x2)
    gather_wait(1, s.x2)

    def mirrored_share():
        mirror(1, s.x2, s.x2b).wait_recv()
        gather_start(10, s.x2b)

    pl.when(zh == 1)(mirrored_share)
    pl.when(zh == 0)(cot_share)

    def feed(x, grad_hidden, place):
        rows = pl.ds(place * T, T)

        def body(c, w):
            cs = pl.ds(c, w)
            gate = dot(x[...], s.gw[:, cs])
            up = dot(x[...], s.uw[:, cs])
            gh = grad_hidden[:, cs]
            sig = jax.nn.sigmoid(gate)
            act = gate * sig
            s.hid[rows, cs] = (act * up).astype(BF16)
            s.gg[rows, cs] = (gh * up * (sig * (1.0 + gate * (1.0 - sig)))).astype(BF16)
            s.gu[rows, cs] = (gh * act).astype(BF16)

        tiles(F, TILE, body)

    feed(s.x2, s.gh, 0)
    pl.when(z < nl - 1)(lambda: mirror(0, s.cot, s.cot2).start())
    pl.when(zh == 0)(mirrored_share)
    pl.when(zh == 1)(cot_share)
    pl.when(zh == 0)(lambda: gather_forward(9, s.cot2))
    pl.when(zh == 1)(lambda: gather_forward(10, s.x2b))
    gather_line_start(2, s.attt, att_all)
    own_part = pl.ds(0, T)

    def body(c, w):
        rs = pl.ds(c, w)
        s.send_a[:, rs] = (
            dot_nt(s.gg[own_part, :], s.gw[rs, :]) + dot_nt(s.gu[own_part, :], s.uw[rs, :])
        ).astype(BF16)

    tiles(D, TILE, body)
    transpose_half(s.x2, s.xt, 0)
    pl.when(zh == 0)(lambda: gather_forward(10, s.x2b))
    pl.when(zh == 1)(lambda: gather_forward(9, s.cot2))
    mirror(1, s.x2, s.x2b).wait_send()
    scatter_start(2, s.send_a, s.recv1)
    for d in range(2):
        mirror_x1(d).start()

    def body(c, w):
        s.send_b[:, pl.ds(c, w)] = dot(s.hid[own_part, :], s.dw[:, pl.ds(c, w)]).astype(BF16)

    tiles(D, TILE, body)
    gather_wait(9, s.cot2)
    hidden_grad(s.cot2, s.gh2)
    transpose_half(s.cot2, s.cott, 1)
    gather_wait(10, s.x2b)
    feed(s.x2b, s.gh2, 1)
    transpose_half(s.x2b, s.xt, 1)
    gather_line_step(2, att_all, 1)
    pl.semaphore_signal(s.credit, inc=1, device_id={"dp": 1 - dp}, device_id_type=MESH)

    grad_second = scatter_sum(2, s.send_a, s.recv1, jnp.zeros((S, D), F32))
    resid = s.resid[...]
    scale = rms(resid)
    normed = resid * scale
    s.gains[:, D : 2 * D] = jnp.sum(grad_second * normed, axis=0, keepdims=True)
    scaled = grad_second * g2[...]
    inner = jnp.mean(scaled * normed, axis=-1, keepdims=True)
    s.gresid[...] = s.cotshare[...] + scale * (scaled - normed * inner)
    s.gm[mine, :] = s.gresid[...].astype(BF16)
    gather_start(4, s.gm)
    columns_start(2, s.gm, s.gmc)

    class WeightJob:
        def __init__(self, k, left, grad):
            self.k, self.left, self.grad, self.cols = k, left, grad, grad.shape[1]

        def part(self, block, c, w):
            rows = pl.ds(pl.multiple_of(block * R, R), R)
            return dot(self.left[rows, :], self.grad[:, pl.ds(c, w)])

        def dp_slot(self, b):
            return s.gw.at[pl.ds(b * R, R), pl.ds(0, self.cols)]

        def dp_recv(self, b):
            return s.uw.at[pl.ds(pl.multiple_of((self.k * nl + b) * R, R), R), pl.ds(0, self.cols)]

        def chain_slot(self, up, step):
            i = nl + self.k * (nl - 1) + (step if up else nl - 2 - step)
            return s.gw.at[pl.ds(i * R, R), pl.ds(0, self.cols)]

        def chain(self, up, step):
            return s.chain.at[self.k, 0 if up or nl == 2 else 1, step, :, pl.ds(0, self.cols)]

    jobs = [
        WeightJob(0, s.cott, s.hid),
        WeightJob(1, s.xt, s.gg),
        WeightJob(2, s.xt, s.gu),
        WeightJob(3, s.x1t, s.dqkv),
    ]
    order = [b for i in range((nl + 1) // 2) for b in dict.fromkeys((nl - 1 - i, i))]

    def job_dp(k):
        for b in order:
            if k:
                job_dp_wait_send(jobs[k - 1], k - 1, b)
            job_dp_start(jobs[k], k, b)

    pl.semaphore_wait(s.credit, 1)
    job_dp(0)
    job_dp_wait_all(jobs[0], 0)
    chain_step(jobs[0], 0, 0)
    gather_forward(4, s.gm)
    job_dp(1)
    gather_wait(4, s.gm)
    scatter_start(3, s.send_b, s.recv2)
    for d in range(2):
        mirror_x1(d).wait_recv()

    def body(c, w):
        s.x1t[pl.ds(c, w), T : 2 * T] = s.x1b[:, pl.ds(c, w)].astype(F32).T.astype(BF16)

    tiles(D // 2, TILE, body)

    gatt = s.gh.at[:, pl.ds(0, QH * H)]

    def body(c, w):
        gatt[:, pl.ds(c, w)] = dot_nt(s.gm[...], s.ow[pl.ds(c, w), :])

    tiles(QH * H, TILE, body)
    s.gq_acc[...] = jnp.zeros((1, H), F32)

    def back(g, _):
        ks = pl.ds(pl.multiple_of(g * H, H), H)
        vs = pl.ds(pl.multiple_of(KV + g * H, H), H)
        v = s.kv[:, pl.ds(pl.multiple_of((2 * g + 1) * H, H), H)]
        grad_k = jnp.zeros((span, H), F32)
        grad_v = jnp.zeros((span, H), F32)
        for i in range(group):
            h = g * group + i
            hs = pl.ds(pl.multiple_of(h * H, H), H)
            q, k, w = weights_of(h, g)
            ga, total = gatt[:, hs], s.tot[:, hs]
            gs = (ga / total).astype(BF16)
            delta = jnp.sum(ga * s.att[:, hs], axis=-1, keepdims=True) / total[:, :1]
            ds = (w * (dot_nt(gs, v) - delta)).astype(BF16)
            grad_k = grad_k + dot_tn(ds, q) * inv_root
            grad_v = grad_v + dot_tn(w.astype(BF16), gs)
            gr = rope_back(dot(ds, k) * inv_root)
            raw = s.q_raw[:, hs]
            r = rms(raw)
            nq = raw * r
            s.gq_acc[...] += jnp.sum(gr * nq, axis=0, keepdims=True)
            sc = gr * gq[...]
            s.dqkv[:T, hs] = (r * (sc - nq * jnp.mean(sc * nq, axis=-1, keepdims=True))).astype(BF16)
        s.dkv[:, ks] = grad_k.astype(BF16)
        s.dkv[:, vs] = grad_v.astype(BF16)
        return 0

    lax.fori_loop(0, KH, back, 0)
    s.gains[:, 2 * D : 2 * D + H] = s.gq_acc[...]

    def dkv_copy(i):
        return remote(
            s.dkv.at[pl.ds(i * T, T)], s.dkv_in.at[i], s.dkv_s.at[i], s.dkv_r.at[i], ctx=z - 1
        )

    for i in range(reach):
        if i:

            @pl.when((z < n - 1) & (z + 1 >= reach - i + 1))
            def _():
                dkv_copy(i - 1).wait_recv()
                rows = pl.ds(i * T, T)
                s.dkv[rows, :] = (s.dkv[rows, :].astype(F32) + s.dkv_in[i - 1].astype(F32)).astype(BF16)

        @pl.when(z >= reach - i)
        def _():
            dkv_copy(i).start()

        if i == 0:
            job_dp_wait_all(jobs[1], 1)
            chain_step(jobs[1], 1, 0, (True,))
            pl.when(zh == 0)(lambda: chain_step(jobs[1], 1, 0, (False,), (0,)))
            job_dp(2)

    pl.when(zh == 0)(lambda: chain_step(jobs[1], 1, 0, (False,), (1,)))

    @pl.when(z < n - 1)
    def _():
        dkv_copy(reach - 1).wait_recv()

    own = s.dkv[pl.ds(reach * T, T), :].astype(F32)
    own = own + jnp.where(z < n - 1, s.dkv_in[reach - 1].astype(F32), 0.0)
    s.dqkv[:T, QH * H + KV :] = own[:, KV:].astype(BF16)
    gk_sum = jnp.zeros((1, H), F32)
    for h in range(KH):
        gr = rope_back(own[:, h * H : (h + 1) * H])
        raw = s.k_raw[:, h * H : (h + 1) * H]
        r = rms(raw)
        nk = raw * r
        gk_sum = gk_sum + jnp.sum(gr * nk, axis=0, keepdims=True)
        sc = gr * gk[...]
        s.dqkv[:T, QH * H + h * H : QH * H + (h + 1) * H] = (
            r * (sc - nk * jnp.mean(sc * nk, axis=-1, keepdims=True))
        ).astype(BF16)
    s.gains[:, 2 * D + H :] = gk_sum
    pl.when(zh == 1)(lambda: chain_step(jobs[1], 1, 0, (False,)))
    mirror_qkv().start()
    gather_line_step(2, att_all, 2)
    job_dp_wait_all(jobs[2], 2)
    chain_step(jobs[2], 2, 0)

    s.outsh[...] = scatter_sum(3, s.send_b, s.recv2, s.resid[...]).astype(BF16)
    q_c, k_c, v_c = pl.ds(0, QH * H), pl.ds(QH * H, KV), pl.ds(QH * H + KV, KV)

    def body(c, w):
        rs = pl.ds(c, w)
        s.send_a[:, rs] = (
            dot_nt(s.dqkv[:T, q_c], s.qw[rs, :])
            + dot_nt(s.dqkv[:T, k_c], s.kw[rs, :])
            + dot_nt(s.dqkv[:T, v_c], s.vw[rs, :])
        ).astype(BF16)

    tiles(D, TILE, body)
    scatter_start(6, s.send_a, s.recv3)
    grad_first = scatter_sum(6, s.send_a, s.recv3, jnp.zeros((S, D), F32))
    tokshare = s.tokshare[...]
    scale = rms(tokshare)
    normed = tokshare * scale
    s.gains[:, :D] = jnp.sum(grad_first * normed, axis=0, keepdims=True)
    scaled = grad_first * g1[...]
    inner = jnp.mean(scaled * normed, axis=-1, keepdims=True)
    s.tgsh[...] = (s.gresid[...] + scale * (scaled - normed * inner)).astype(BF16)
    for j in range(1, nt):
        remote(s.gains, s.gains_p.at[j - 1], s.pl_s.at[8, j - 1], s.pl_r.at[8, j - 1], tensor=t ^ j).start()
    spread_start(7, s.tgsh, tgrad_hbm, 1)
    for j in range(1, nt):
        remote(s.gains, s.gains_p.at[j - 1], s.pl_s.at[8, j - 1], s.pl_r.at[8, j - 1], tensor=t ^ j).wait()
    total = s.gains[...]
    for j in range(1, nt):
        total = total + s.gains_p[j - 1]
    s.gains2[...] = total

    def gain_copy(e, d):
        i = e * n + d
        return remote(
            s.gains2, s.gains_x.at[i - 1], s.ga_s.at[i], s.ga_r.at[i], dp=dp ^ e, ctx=lax.rem(z + d, n)
        )

    for e in range(2):
        for d in range(n):
            if e or d:
                gain_copy(e, d).start()
    columns_wait_recv(2, s.gm, s.gmc)
    share_start(2, s.gmc)
    spread_start(5, s.outsh, out_hbm, 0)
    stage = s.gh2.at[pl.ds(0, R), pl.ds(0, QH * H + 2 * KV)]

    def gate_copy():
        return pltpu.make_async_copy(s.gh.at[pl.ds(0, R)], gate_out, s.load_sem.at[2])

    def up_copy():
        return pltpu.make_async_copy(s.gh.at[pl.ds(0, R)], up_out, s.load_sem.at[3])

    def qkv_copies():
        parts = [(q_out, 0, QH * H), (k_out, QH * H, KV), (v_out, QH * H + KV, KV)]
        return [
            pltpu.make_async_copy(stage.at[:, pl.ds(a, w)], ref, s.load_sem.at[6 + i])
            for i, (ref, a, w) in enumerate(parts)
        ]

    for step in range(1, nl - 1):
        for k in range(3):
            chain_step(jobs[k], k, step)
    rows = pl.ds(0, R)
    chain_final(jobs[0], 0, s.gh.at[rows])
    width = min(256, F)
    flip = s.gh2.at[:, pl.ds(QH * H + 2 * KV, 2 * R)]

    def down_copy(i):
        return pltpu.make_async_copy(
            flip.at[pl.ds(0, width), pl.ds((i % 2) * R, R)],
            down_out.at[pl.ds(i * width, width)],
            s.load_sem.at[4 + i % 2],
        )

    count = F // width
    for i in range(count):
        if i >= 2:
            down_copy(i - 2).wait()
        flip[:width, (i % 2) * R : (i % 2 + 1) * R] = s.gh[rows, i * width : (i + 1) * width].T
        down_copy(i).start()
    for i in range(max(0, count - 2), count):
        down_copy(i).wait()
    mirror_qkv().wait_recv()
    job_dp(3)
    job_dp_wait_all(jobs[3], 3)
    chain_step(jobs[3], 3, 0)
    for step in range(1, nl - 1):
        chain_step(jobs[3], 3, step)


    chain_final(jobs[1], 1, s.gh.at[rows])
    gate_copy().start()
    for step in range(3, n):
        gather_line_step(2, att_all, step)
    gather_line_finish(2, s.attt, att_all)
    share_wait(2, s.gmc)

    def load(i):
        slot = lax.rem(i, 2)
        return pltpu.make_async_copy(
            att_all.at[i // n, lax.rem(i, n)],
            s.dw.at[pl.ds(pl.multiple_of(slot * QH * H, QH * H), QH * H), pl.ds(0, T)],
            s.stage_sem.at[slot],
        )

    load(0).start()
    s.outw[...] = jnp.zeros(s.outw.shape, F32)

    def step(i, _):
        @pl.when(i + 1 < 2 * n)
        def _():
            load(i + 1).start()

        load(i).wait()
        slot = lax.rem(i, 2)
        left = s.dw[pl.ds(pl.multiple_of(slot * QH * H, QH * H), QH * H), pl.ds(0, T)]
        s.outw[...] += dot(left, s.gmc[:, i].reshape(T, R))
        return 0

    lax.fori_loop(0, 2 * n, step, 0)

    def outw_copy():
        return pltpu.make_async_copy(s.outw, outw_out, s.load_sem.at[4])

    outw_copy().start()
    gate_copy().wait()
    chain_final(jobs[2], 2, s.gh.at[rows])
    up_copy().start()
    chain_final(jobs[3], 3, stage)
    for copy in qkv_copies():
        copy.start()
    for e in range(2):
        for d in range(n):
            if e or d:
                gain_copy(e, d).wait()
    total = s.gains2[...]
    for i in range(2 * n - 1):
        total = total + s.gains_x[i]
    gains_out[...] = total

    columns_wait_send(2, s.gm, s.gmc)
    mirror(0, s.cot, s.cot2).wait_send()
    mirror_qkv().wait_send()
    for d in range(2):
        mirror_x1(d).wait_send()
    for b in order:
        job_dp_wait_send(jobs[-1], len(jobs) - 1, b)
    for st in range(nl - 1):
        for k, job in enumerate(jobs):
            chain_wait_send(job, k, st)
    for r in range(1, reach + 1):

        @pl.when((z < n - 1) & (z >= r - 1))
        def _(r=r):
            for c in range(KH):
                kv_copy(r, c).wait_send()

    for i in range(reach):

        @pl.when(z >= reach - i)
        def _():
            dkv_copy(i).wait_send()

    spread_wait(5, s.outsh, out_hbm, 0)
    spread_wait(7, s.tgsh, tgrad_hbm, 1)
    up_copy().wait()
    outw_copy().wait()
    for copy in qkv_copies():
        copy.wait()


def run_layer(dm, *operands):
    T, D, H, F, n, nt, reach, S, R = dm.T, dm.D, dm.H, dm.F, dm.n, dm.nt, dm.reach, dm.S, dm.R
    QC, KV = dm.QH * H, dm.KH * H
    span = (reach + 1) * T
    G = 2 * D + 2 * H
    dma = pltpu.SemaphoreType.DMA
    scratch = dict(
        tok=((T, D), BF16), x1=((T, D), BF16), send_b=((T, D), BF16), cot=((T, D), BF16), x2=((T, D), BF16),
        outsh=((S, D), BF16), tgsh=((S, D), BF16), xt=((D // 2, 2 * T), BF16), cott=((D // 2, 2 * T), BF16),
        cot2=((T, D), BF16), x2b=((T, D), BF16),
        qw=((D, QC), BF16), kw=((D, KV), BF16), vw=((D, KV), BF16), ow=((QC, D), BF16),
        gw=((D, F), BF16), uw=((D, F), BF16), dw=((F, D), BF16),
        tokshare=((S, D), F32), cotshare=((S, D), F32), resid=((S, D), F32), gresid=((S, D), F32),
        k_raw=((T, KV), F32), q_raw=((T, QC), F32), q_rot=((T, QC), BF16), kv=((span, 2 * KV), BF16),
        mask=((T, span), F32), tot=((T, QC), F32), att=((T, QC), F32), att_low=((T, QC), BF16),
        attt=((QC, T), BF16), gq_acc=((1, H), F32),
        recv0=((6, S, D // 2) if nt == 4 else (nt - 1, S, D), BF16),
        recv1=((6, S, D // 2) if nt == 4 else (nt - 1, S, D), BF16), pair=((2, S, D // 2), BF16),
        gh=((T, F), F32), hid=((2 * T, F), BF16), gg=((2 * T, F), BF16), gu=((2 * T, F), BF16),
        dkv=((span, 2 * KV), BF16), dkv_in=((reach, T, 2 * KV), BF16), dqkv=((2 * T, QC + 2 * KV), BF16),
        chain=((4, 1 if n == 4 else 2, n // 2 - 1, R, F), BF16),

        gmc=((nt, 2 * n, S, R), BF16), x1b=((T, D // 2), BF16), x1t=((D // 2, 2 * T), BF16), gh2=((T, F), F32),
        cos=((T, H), F32), sin=((T, H), F32), segs=((1, reach * T + dm.L), jnp.int32),
        outw=((QC, R), F32), gain_in=((1, G), F32), gains=((1, G), F32), gains2=((1, G), F32), gains_p=((nt - 1, 1, G), F32),
        gains_x=((2 * n - 1, 1, G), F32),
    )
    sems = dict(
        load_sem=(9,), own_sem=(3,), pl_s=(13, nt - 1), pl_r=(13, nt - 1), ag_s=(3, 2, n - 1), ag_r=(3, 2, n - 1),
        agx_s=(3, 2 * n - 1), agx_r=(3, 2 * n - 1), aa_s=(3, 2 * n), aa_r=(3, 2 * n), stage_sem=(2,),
        dp_s=(4, n // 2), dp_r=(4, n // 2), ch_s=(4, 2, n // 2 - 1, 2), ch_r=(4, 2, n // 2 - 1, 2), mi_s=(5,), mi_r=(5,), kv_s=(reach, KV // H), kv_r=(reach, KV // H), pl2_s=(11,), pl2_r=(11,), rs_s=(7, 6), rs_r=(7, 6),
        dkv_s=(reach,), dkv_r=(reach,), ga_s=(2 * n,), ga_r=(2 * n,),
    )
    names = list(scratch) + list(sems) + ["credit"]
    shapes = [pltpu.VMEM(*v) for v in scratch.values()] + [dma(v) for v in sems.values()]
    shapes.append(pltpu.SemaphoreType.REGULAR)

    def body(*refs):
        fixed = len(refs) - len(names)
        s = Dims()
        for name, ref in zip(names, refs[fixed:]):
            setattr(s, name, ref)
        for alias, of in dm.alias.items():
            setattr(s, alias, getattr(s, of))
        layer_kernel(dm, *refs[:fixed], s)

    hbm = pl.BlockSpec(memory_space=pl.ANY)
    vmem = pl.BlockSpec(memory_space=pltpu.VMEM)
    return pl.pallas_call(
        body,
        out_shape=(
            jax.ShapeDtypeStruct((T, D), BF16),
            jax.ShapeDtypeStruct((T, D), BF16),
            jax.ShapeDtypeStruct((R, F), F32),
            jax.ShapeDtypeStruct((R, F), F32),
            jax.ShapeDtypeStruct((F, R), F32),
            jax.ShapeDtypeStruct((R, QC), F32),
            jax.ShapeDtypeStruct((R, KV), F32),
            jax.ShapeDtypeStruct((R, KV), F32),
            jax.ShapeDtypeStruct((QC, R), F32),
            jax.ShapeDtypeStruct((1, G), F32),
            jax.ShapeDtypeStruct((2, n, QC, T), BF16),
        ),
        in_specs=[hbm] * 2 + [vmem] * 6 + [hbm] * 7,
        out_specs=[hbm] * 9 + [vmem] + [hbm],
        scratch_shapes=shapes,
        compiler_params=pltpu.CompilerParams(
            collective_id=0, has_side_effects=True, vmem_limit_bytes=67043328
        ),
        name="layer",
    )(*operands)


FINISH_WINDOW = 64


def finish_pieces(shape):
    rows = shape[0]
    step = rows // 2 if rows % 32 == 0 else rows
    return [(r, step) for r in range(0, rows, step)]


def finish_kernel(dm, *refs):
    count = len(dm.finish)
    ins, gains, outs = refs[:count], refs[count], refs[count + 1 : 2 * count + 1]
    gain_outs = refs[2 * count + 1 : 2 * count + 5]
    bufs, load_sem, store_sem = refs[2 * count + 5 : 3 * count + 5], refs[-2], refs[-1]
    loads, stores = [], []
    for a, b, c in zip(ins, bufs, outs):
        for start, size in finish_pieces(a.shape):
            rows, i = pl.ds(start, size), len(loads)
            loads.append(pltpu.make_async_copy(a.at[rows], b.at[rows], load_sem.at[i]))
            stores.append(pltpu.make_async_copy(b.at[rows], c.at[rows], store_sem.at[i]))
    for load in loads[:FINISH_WINDOW]:
        load.start()
    place = 0
    for ref in gain_outs:
        ref[...] = gains[:, place : place + ref.shape[1]]
        place += ref.shape[1]
    for i, (load, store) in enumerate(zip(loads, stores)):
        load.wait()
        store.start()
        if i + FINISH_WINDOW < len(loads):
            loads[i + FINISH_WINDOW].start()
    for store in stores:
        store.wait()


def finish(dm, arrays, gains):
    dm.finish = arrays
    hbm = pl.BlockSpec(memory_space=pl.ANY)
    vmem = pl.BlockSpec(memory_space=pltpu.VMEM)
    shapes = [jax.ShapeDtypeStruct(a.shape, a.dtype) for a in arrays]
    gain_shapes = [jax.ShapeDtypeStruct((1, w), F32) for w in (dm.D, dm.D, dm.H, dm.H)]
    dma = pltpu.SemaphoreType.DMA((sum(len(finish_pieces(a.shape)) for a in arrays),))
    return pl.pallas_call(
        functools.partial(finish_kernel, dm),
        out_shape=tuple(shapes + gain_shapes),
        in_specs=[hbm] * len(arrays) + [vmem],
        out_specs=tuple([hbm] * len(arrays) + [vmem] * 4),
        scratch_shapes=[pltpu.VMEM(a.shape, a.dtype) for a in arrays] + [dma, dma],
        compiler_params=pltpu.CompilerParams(vmem_limit_bytes=67043328),
        name="finish",
    )(*arrays, gains)


def per_device(
    tokens,
    segments,
    first_gain,
    query_weight,
    key_matrix,
    value_matrix,
    query_norm_gain,
    key_gain,
    output_weight,
    second_gain,
    gate_weight,
    up_weight,
    down_weight,
    cotangent,
):
    _, T, D = tokens.shape
    dm = Dims()
    dm.T, dm.D, dm.H, dm.F = T, D, query_norm_gain.shape[0], gate_weight.shape[1]
    dm.QH, dm.KH = query_weight.shape[1] // dm.H, key_matrix.shape[1] // dm.H
    dm.n, dm.nt = lax.axis_size("ctx"), lax.axis_size("tensor")
    length = segments.shape[1]
    dm.reach = -(-(length // 2 - 1) // T)
    dm.S, dm.R = T // dm.nt, D // (2 * dm.n)
    dm.alias = {"send_a": "tok", "gm": "x2", "recv2": "recv0", "recv3": "recv1"}
    H = dm.H
    dm.L = length
    inverse = (1.0 / rope_base ** (np.arange(0, H, 2, dtype=np.float32) / np.float32(H))).astype(np.float32)
    inverse = np.concatenate([inverse, inverse])[None]
    out, tgrad, gate_g, up_g, down_g, q_g, k_g, v_g, out_g, gains = run_layer(
        dm,
        tokens.reshape(T, D),
        cotangent.reshape(T, D),
        first_gain.reshape(-1, H),
        second_gain.reshape(-1, H),
        query_norm_gain.reshape(1, H),
        key_gain.reshape(1, H),
        inverse,
        segments,
        query_weight,
        key_matrix,
        value_matrix,
        output_weight,
        gate_weight,
        up_weight,
        down_weight,
    )[:10]
    out, tgrad, gate_g, up_g, down_g, q_g, k_g, v_g, out_g, first_g, second_g, qn_g, kn_g = finish(
        dm, (out, tgrad, gate_g, up_g, down_g, q_g, k_g, v_g, out_g), gains
    )
    return (
        out.reshape(tokens.shape),
        tgrad.reshape(tokens.shape),
        first_g.reshape(D),
        q_g,
        k_g,
        v_g,
        qn_g.reshape(H),
        kn_g.reshape(H),
        out_g,
        second_g.reshape(D),
        gate_g,
        up_g,
        down_g,
    )


def solution(mesh):
    return jax.shard_map(
        per_device,
        mesh=mesh,
        in_specs=(
            P("dp", "ctx", None),
            P("dp", None),
            P(),
            P(None, "tensor"),
            P(None, "tensor"),
            P(None, "tensor"),
            P(),
            P(),
            P("tensor", None),
            P(),
            P(None, "tensor"),
            P(None, "tensor"),
            P("tensor", None),
            P("dp", "ctx", None),
        ),
        out_specs=(
            P("dp", "ctx", None),
            P("dp", "ctx", None),
            P(),
            P(("dp", "ctx"), "tensor"),
            P(("dp", "ctx"), "tensor"),
            P(("dp", "ctx"), "tensor"),
            P(),
            P(),
            P("tensor", ("dp", "ctx")),
            P(),
            P(("dp", "ctx"), "tensor"),
            P(("dp", "ctx"), "tensor"),
            P("tensor", ("dp", "ctx")),
        ),
        check_vma=False,
    )
```

```python
import functools
import math

import jax
import jax.numpy as jnp
import numpy as np
from jax import lax
from jax.experimental import pallas as pl
from jax.experimental.pallas import tpu as pltpu
from jax.sharding import PartitionSpec as P

epsilon = 1e-06
rope_base = 1000000.0
F32 = jnp.float32
BF16 = jnp.bfloat16
MESH = pl.DeviceIdType.MESH
TILE = 256


def dot(a, b):
    return jnp.dot(a, b, preferred_element_type=F32)


def dot_nt(a, b):
    return lax.dot_general(a, b, (((1,), (1,)), ((), ())), preferred_element_type=F32)


def dot_tn(a, b):
    return lax.dot_general(a, b, (((0,), (0,)), ((), ())), preferred_element_type=F32)


def remote(src, dst, send_sem, recv_sem, **device):
    return pltpu.make_async_remote_copy(
        src_ref=src,
        dst_ref=dst,
        send_sem=send_sem,
        recv_sem=recv_sem,
        device_id=device,
        device_id_type=MESH,
    )


def tiles(total, size, body):
    size = min(size, total)

    def step(i, _):
        body(pl.multiple_of(i * size, size), size)
        return 0

    lax.fori_loop(0, total // size, step, 0)


class Dims:
    pass


def layer_kernel(
    dm,
    tok_hbm,
    cot_hbm,
    first_in,
    second_in,
    query_in,
    key_in,
    inverse,
    seg_row,
    qw_hbm,
    kw_hbm,
    vw_hbm,
    ow_hbm,
    gw_hbm,
    uw_hbm,
    dw_hbm,
    out_hbm,
    tgrad_hbm,
    gate_out,
    up_out,
    down_out,
    q_out,
    k_out,
    v_out,
    outw_out,
    gains_out,
    att_all,
    s,
):
    T, D, H, QH, KH, F, n, nt, reach, S, R = (
        dm.T, dm.D, dm.H, dm.QH, dm.KH, dm.F, dm.n, dm.nt, dm.reach, dm.S, dm.R,
    )
    group = QH // KH
    span = (reach + 1) * T
    KV = KH * H
    inv_root = 1.0 / math.sqrt(H)
    C = R // nt
    gain_in = s.gain_in
    for place, ref in ((0, first_in), (D, second_in), (2 * D, query_in), (2 * D + H, key_in)):
        for i in range(ref.shape[0]):
            gain_in[:, place + i * H : place + (i + 1) * H] = ref[i : i + 1, :].astype(F32)
    g1 = gain_in.at[:, pl.ds(0, D)]
    g2 = gain_in.at[:, pl.ds(D, D)]
    gq = gain_in.at[:, pl.ds(2 * D, H)]
    gk = gain_in.at[:, pl.ds(2 * D + H, H)]
    cos, sin = s.cos, s.sin
    dp, z, t = lax.axis_index("dp"), lax.axis_index("ctx"), lax.axis_index("tensor")
    zz = n - 1 - z
    nl = n // 2
    zh, zl = z // nl, lax.rem(z, nl)
    zzl = nl - 1 - zl

    barrier = pltpu.get_barrier_semaphore()
    for j in range(1, nt):
        pl.semaphore_signal(barrier, inc=1, device_id={"tensor": t ^ j}, device_id_type=MESH)
    for e in range(2):
        for d in range(n):
            if e or d:
                pl.semaphore_signal(
                    barrier,
                    inc=1,
                    device_id={"dp": dp ^ e, "ctx": lax.rem(z + d, n)},
                    device_id_type=MESH,
                )

    loads = [
        (tok_hbm, s.tok), (cot_hbm, s.cot), (kw_hbm, s.kw), (vw_hbm, s.vw), (qw_hbm, s.qw),
        (ow_hbm, s.ow), (dw_hbm, s.dw), (gw_hbm, s.gw), (uw_hbm, s.uw),
    ]
    loads = [pltpu.make_async_copy(a, b, s.load_sem.at[i]) for i, (a, b) in enumerate(loads)]
    for load in loads:
        load.start()
    (l_tok, l_cot, l_kw, l_vw, l_qw, l_ow, l_dw, l_gw, l_uw) = loads

    def scatter_direct(k, buf, recv, j):
        peer = t ^ j
        return remote(
            buf.at[pl.ds(pl.multiple_of(peer * S, S), S)], recv.at[j - 1],
            s.pl_s.at[k, j - 1], s.pl_r.at[k, j - 1], tensor=peer,
        )

    def scatter_first(k, buf, recv, slot):
        to = t ^ (1 if slot < 2 else 2)
        rows = pl.ds(pl.multiple_of((to if slot % 2 == 0 else t ^ 3) * S, S), S)
        cols = pl.ds(0 if slot < 2 else D // 2, D // 2)
        return remote(buf.at[rows, cols], recv.at[slot], s.rs_s.at[k, slot], s.rs_r.at[k, slot], tensor=to)

    def scatter_second(k, recv, slot):
        to = t ^ (2 if slot == 4 else 1)
        return remote(s.pair.at[slot - 4], recv.at[slot], s.rs_s.at[k, slot], s.rs_r.at[k, slot], tensor=to)

    def scatter_start(k, buf, recv):
        if nt == 4:
            for slot in (1, 3, 0, 2):
                scatter_first(k, buf, recv, slot).start()
        else:
            for j in range(1, nt):
                scatter_direct(k, buf, recv, j).start()

    def scatter_sum(k, buf, recv, base):
        own = pl.ds(pl.multiple_of(t * S, S), S)
        if nt == 4:
            for slot, peer, cols in ((1, t ^ 2, slice(0, D // 2)), (3, t ^ 1, slice(D // 2, D))):
                scatter_first(k, buf, recv, slot).wait_recv()
                rows = pl.ds(pl.multiple_of(peer * S, S), S)
                both = buf[rows, cols].astype(F32) + recv[slot].astype(F32)
                s.pair[slot // 2] = both.astype(BF16)
                scatter_second(k, recv, 4 + slot // 2).start()
            for slot in (0, 2):
                scatter_first(k, buf, recv, slot).wait_recv()
            for slot in range(4):
                scatter_first(k, buf, recv, slot).wait_send()
            for slot in (4, 5):
                scatter_second(k, recv, slot).wait()
            left = buf[own, 0 : D // 2].astype(F32) + recv[0].astype(F32) + recv[4].astype(F32)
            right = buf[own, D // 2 : D].astype(F32) + recv[2].astype(F32) + recv[5].astype(F32)
            return base + jnp.concatenate([left, right], axis=1)
        for j in range(1, nt):
            scatter_direct(k, buf, recv, j).wait()
        total = base + buf[own, :].astype(F32)
        for j in range(1, nt):
            total = total + recv[j - 1].astype(F32)
        return total

    def rows_of(peer, half=None):
        if half is None:
            return pl.ds(pl.multiple_of(peer * S, S), S)
        return pl.ds(pl.multiple_of(peer * S + half * (S // 2), S // 2), S // 2)

    def gather_copy(k, full, j):
        rows = rows_of(t)
        return remote(full.at[rows], full.at[rows], s.pl_s.at[k, j - 1], s.pl_r.at[k, j - 1], tensor=t ^ j)

    def gather_arrived(k, full, j):
        rows = rows_of(t ^ j)
        return remote(full.at[rows], full.at[rows], s.pl_s.at[k, j - 1], s.pl_r.at[k, j - 1], tensor=t ^ j)

    def relay_copy(k, full, origin, half, to):
        rows = rows_of(origin, half)
        sems = (s.pl2_s.at[k], s.pl2_r.at[k]) if half else (s.pl_s.at[k, 2], s.pl_r.at[k, 2])
        return remote(full.at[rows], full.at[rows], *sems, tensor=to)

    def gather_start(k, full):
        for j in range(1, nt) if nt != 4 else (1, 2):
            gather_copy(k, full, j).start()

    def gather_forward(k, full):
        if nt == 4:
            gather_arrived(k, full, 1).wait_recv()
            relay_copy(k, full, t ^ 1, 0, t ^ 2).start()
            gather_arrived(k, full, 2).wait_recv()
            relay_copy(k, full, t ^ 2, 1, t ^ 1).start()

    def gather_wait(k, full):
        for j in range(1, nt) if nt != 4 else (1, 2):
            gather_copy(k, full, j).wait_send()
            if nt != 4:
                gather_arrived(k, full, j).wait_recv()
        if nt == 4:
            relay_copy(k, full, t ^ 1, 0, t ^ 2).wait_send()
            relay_copy(k, full, t ^ 2, 1, t ^ 1).wait_send()
            relay_copy(k, full, t ^ 3, 0, t ^ 2).wait_recv()
            relay_copy(k, full, t ^ 3, 1, t ^ 1).wait_recv()

    mine = pl.ds(pl.multiple_of(t * S, S), S)

    def spread_start(k, share, full, own):
        own_copy(share, full, own).start()
        for j in range(1, nt):
            remote(
                share, full.at[mine], s.pl_s.at[k, j - 1], s.pl_r.at[k, j - 1], tensor=t ^ j
            ).start()

    def own_copy(share, full, own):
        return pltpu.make_async_copy(share, full.at[mine], s.load_sem.at[own])

    def spread_wait(k, share, full, own):
        own_copy(share, full, own).wait()
        for j in range(1, nt):
            peer = t ^ j
            theirs = pl.ds(pl.multiple_of(peer * S, S), S)
            copy = remote(share, full.at[theirs], s.pl_s.at[k, j - 1], s.pl_r.at[k, j - 1], tensor=peer)
            copy.wait_send()
            copy.wait_recv()

    def mirror(i, src, dst):
        return remote(src.at[mine], dst.at[mine], s.mi_s.at[i], s.mi_r.at[i], ctx=zz)

    def mirror_x1(d):
        cols = pl.ds(pl.multiple_of((d * n + (1 - zh) * nl) * R, 128), nl * R)
        return remote(
            s.x1.at[:, cols], s.x1b.at[:, pl.ds(d * nl * R, nl * R)], s.mi_s.at[2 + d], s.mi_r.at[2 + d], ctx=zz
        )

    def mirror_qkv():
        return remote(
            s.dqkv.at[pl.ds(0, T)], s.dqkv.at[pl.ds(T, T)], s.mi_s.at[4], s.mi_r.at[4], ctx=zz
        )

    def line_copy(k, all_ref, up, step, src=None):
        idx = (z - step) if up else (z + step)
        ref = all_ref.at[dp, idx]
        return remote(
            ref if src is None else src, ref,
            s.ag_s.at[k, 0 if up else 1, step], s.ag_r.at[k, 0 if up else 1, step],
            ctx=(z + 1) if up else (z - 1),
        )

    def core_copy(k, all_ref, slot, idx, src=None):
        ref = all_ref.at[dp, idx]
        return remote(
            ref if src is None else src, ref, s.agx_s.at[k, slot], s.agx_r.at[k, slot], dp=1 - dp
        )

    def gather_line_start(k, src, all_ref):
        pltpu.make_async_copy(src, all_ref.at[dp, z], s.own_sem.at[k]).start()

        @pl.when(z < n - 1)
        def _():
            line_copy(k, all_ref, True, 0, src).start()

        @pl.when(z > 0)
        def _():
            line_copy(k, all_ref, False, 0, src).start()

        core_copy(k, all_ref, 0, z, src).start()

    def gather_line_step(k, all_ref, step):
        @pl.when(z >= step)
        def _():
            ref = all_ref.at[dp, z - step]
            remote(ref, ref, s.ag_s.at[k, 0, step - 1], s.ag_r.at[k, 0, step - 1], ctx=z - 1).wait_recv()
            if step < n - 1:

                @pl.when(z < n - 1)
                def _():
                    line_copy(k, all_ref, True, step).start()

            core_copy(k, all_ref, step, z - step).start()

        @pl.when(zz >= step)
        def _():
            ref = all_ref.at[dp, z + step]
            remote(ref, ref, s.ag_s.at[k, 1, step - 1], s.ag_r.at[k, 1, step - 1], ctx=z + 1).wait_recv()
            if step < n - 1:

                @pl.when(z > 0)
                def _():
                    line_copy(k, all_ref, False, step).start()

            core_copy(k, all_ref, n - 1 + step, z + step).start()

    def gather_line_finish(k, src, all_ref):
        pltpu.make_async_copy(src, all_ref.at[dp, z], s.own_sem.at[k]).wait()
        for step in range(n - 1):

            @pl.when((z >= step) & (z < n - 1))
            def _():
                line_copy(k, all_ref, True, step, src).wait_send()

            @pl.when((zz >= step) & (z > 0))
            def _():
                line_copy(k, all_ref, False, step, src).wait_send()

        def both(slot, idx):
            ref = all_ref.at[1 - dp, idx]
            copy = remote(src, ref, s.agx_s.at[k, slot], s.agx_r.at[k, slot], dp=1 - dp)
            copy.wait_send()
            copy.wait_recv()

        both(0, z)
        for step in range(1, n):

            @pl.when(z >= step)
            def _():
                both(step, z - step)

            @pl.when(zz >= step)
            def _():
                both(n - 1 + step, z + step)

    me = dp * n + z

    def columns_src(k, src, block):
        if k < 2:
            rows = pl.ds(pl.multiple_of(lax.rem(block, n) * R + t * C, C), C)
            return src.at[rows, pl.ds(pl.multiple_of(block // n * T, T), T)]
        return src.at[mine, pl.ds(pl.multiple_of(block * R, R), R)]

    def columns_copy(k, src, all_ref, e, d):
        to_dp, to_z = dp ^ e, lax.rem(z + d, n)
        return remote(
            columns_src(k, src, to_dp * n + to_z), all_ref.at[t, me],
            s.aa_s.at[k, e * n + d], s.aa_r.at[k, e * n + d], dp=to_dp, ctx=to_z,
        )

    def columns_own(k, src, all_ref):
        return pltpu.make_async_copy(columns_src(k, src, me), all_ref.at[t, me], s.aa_s.at[k, 0])

    def columns_start(k, src, all_ref):
        columns_own(k, src, all_ref).start()
        for d in range(n):
            for e in range(2):
                if e or d:
                    columns_copy(k, src, all_ref, e, d).start()

    def columns_wait_send(k, src, all_ref):
        for e in range(2):
            for d in range(n):
                if e or d:
                    columns_copy(k, src, all_ref, e, d).wait_send()

    def columns_wait_recv(k, src, all_ref):
        columns_own(k, src, all_ref).wait()
        for e in range(2):
            for d in range(n):
                if e or d:
                    ref = all_ref.at[t, (dp ^ e) * n + lax.rem(z - d + n, n)]
                    remote(
                        columns_src(k, src, me), ref, s.aa_s.at[k, e * n + d], s.aa_r.at[k, e * n + d],
                        dp=dp ^ e, ctx=lax.rem(z - d + n, n),
                    ).wait_recv()

    def share_start(k, all_ref):
        for j in range(1, nt):
            remote(
                all_ref.at[t], all_ref.at[t], s.pl_s.at[10 + k, j - 1], s.pl_r.at[10 + k, j - 1], tensor=t ^ j
            ).start()

    def share_wait(k, all_ref):
        for j in range(1, nt):
            copy = remote(
                all_ref.at[t], all_ref.at[t ^ j], s.pl_s.at[10 + k, j - 1], s.pl_r.at[10 + k, j - 1], tensor=t ^ j
            )
            copy.wait_send()
            copy.wait_recv()

    def job_dp_start(job, k, b):
        slot = job.dp_slot(b)

        def body(c, w):
            slot[:, pl.ds(c, w)] = job.part((1 - dp) * nl + b, c, w).astype(BF16)

        tiles(job.cols, 512, body)
        remote(slot, job.dp_recv(b), s.dp_s.at[k, b], s.dp_r.at[k, b], dp=1 - dp).start()

    def job_dp_wait_send(job, k, b):
        remote(job.dp_slot(b), job.dp_recv(b), s.dp_s.at[k, b], s.dp_r.at[k, b], dp=1 - dp).wait_send()

    def job_dp_wait_all(job, k):
        for b in range(nl):
            remote(job.dp_slot(b), job.dp_recv(b), s.dp_s.at[k, b], s.dp_r.at[k, b], dp=1 - dp).wait_recv()

    def chain_copy(job, k, up, step, part):
        i = 0 if up else 1
        width = job.cols // 2
        cols = pl.ds(part * width, width)
        return remote(
            job.chain_slot(up, step).at[:, cols], job.chain(up, step).at[:, cols],
            s.ch_s.at[k, i, step, part], s.ch_r.at[k, i, step, part],
            ctx=(z + 1) if up else (z - 1),
        )

    def chain_step(job, k, step, ways=(True, False), parts=(0, 1)):
        width = job.cols // 2
        for part in parts:
            for up in ways:
                pos = zl if up else zzl

                @pl.when((pos <= step) & (pos < nl - 1))
                def _(up=up, pos=pos, part=part):
                    target = (zl + nl - 1 - step) if up else (zl - (nl - 1 - step))
                    slot = job.chain_slot(up, step)
                    if step:

                        @pl.when(pos >= 1)
                        def _():
                            chain_copy(job, k, up, step - 1, part).wait_recv()

                    def body(c, w):
                        cs = pl.ds(pl.multiple_of(part * width + c, 128), w)
                        total = job.part(dp * nl + target, cs.start, w)
                        total = total + job.dp_recv(target)[:, cs].astype(F32)
                        if step:
                            prev = job.chain(up, step - 1)[:, cs].astype(F32)
                            total = total + jnp.where(pos >= 1, prev, 0.0)
                        slot[:, cs] = total.astype(BF16)

                    tiles(width, 256 if width % 256 == 0 else 128, body)
                    chain_copy(job, k, up, step, part).start()

    def chain_wait_send(job, k, step):
        for up in (True, False):
            pos = zl if up else zzl

            @pl.when((pos <= step) & (pos < nl - 1))
            def _(up=up):
                for part in range(2):
                    chain_copy(job, k, up, step, part).wait_send()

    def chain_final(job, k, out_ref):
        width = job.cols // 2
        for part in range(2):
            for up in (True, False):
                pos = zl if up else zzl

                @pl.when(pos >= 1)
                def _(up=up, part=part):
                    chain_copy(job, k, up, nl - 2, part).wait_recv()

            def body(c, w):
                cs = pl.ds(pl.multiple_of(part * width + c, 128), w)
                total = job.part(dp * nl + zl, cs.start, w) + job.dp_recv(zl)[:, cs].astype(F32)
                a = job.chain(True, nl - 2)[:, cs].astype(F32)
                b = job.chain(False, nl - 2)[:, cs].astype(F32)
                out_ref[:, cs] = total + jnp.where(zl >= 1, a, 0.0) + jnp.where(zzl >= 1, b, 0.0)

            tiles(width, 256 if width % 256 == 0 else 128, body)

    L = seg_row.shape[1]
    s.segs[:, : reach * T] = jnp.full((1, reach * T), -1, jnp.int32)
    s.segs[:, reach * T :] = seg_row[...]
    row = seg_row[...]
    at_me = lax.broadcasted_iota(jnp.int32, (T, L), 1) == lax.broadcasted_iota(jnp.int32, (T, L), 0) + z * T
    row_f = jnp.broadcast_to(row.astype(F32), (T, L))
    qseg_f = jnp.sum(jnp.where(at_me, row_f, 0.0), axis=1, keepdims=True)
    begins = jnp.sum(jnp.where(row_f < qseg_f, 1.0, 0.0), axis=1, keepdims=True)
    position = (lax.broadcasted_iota(jnp.int32, (T, H), 0) + z * T).astype(F32) - begins
    angles = position * inverse[...]
    cos[...] = jnp.cos(angles)
    lane = lax.broadcasted_iota(jnp.int32, (T, H), 1)
    turned = jnp.sin(angles)
    sin[...] = jnp.where(lane < H // 2, -turned, turned)

    rows_i = lax.broadcasted_iota(jnp.int32, (T, span), 0) + reach * T
    cols_i = lax.broadcasted_iota(jnp.int32, (T, span), 1)
    kseg_f = s.segs[:, pl.ds(pl.multiple_of(z * T, T), span)].astype(F32)
    allowed = (cols_i <= rows_i) & (qseg_f == kseg_f)
    s.mask[...] = jnp.where(allowed, 1.0, 0.0).astype(F32)

    l_tok.wait()
    x = s.tok[...].astype(F32)
    scale = lax.rsqrt(jnp.mean(x * x, axis=-1, keepdims=True) + epsilon)
    s.x1[...] = (x * scale * g1[...]).astype(BF16)
    s.tokshare[...] = s.tok[mine, :].astype(F32)

    def rms(v):
        return lax.rsqrt(jnp.mean(v * v, axis=-1, keepdims=True) + epsilon)

    def rope(v):
        return v * cos[...] + pltpu.roll(v, H // 2, 1) * sin[...]

    def rope_back(g):
        return g * cos[...] + pltpu.roll(g * sin[...], H // 2, 1)

    own_rows = pl.ds(reach * T, T)
    l_kw.wait()
    l_vw.wait()
    def kv_copy(r, c):
        lanes = pl.ds(c * 2 * H, 2 * H)
        return remote(
            s.kv.at[pl.ds((reach - r + 1) * T, T), lanes], s.kv.at[pl.ds((reach - r) * T, T), lanes],
            s.kv_s.at[r - 1, c], s.kv_r.at[r - 1, c], ctx=z + 1,
        )

    def kv_send(r, c):
        @pl.when((z < n - 1) & (z >= r - 1))
        def _():
            kv_copy(r, c).start()

    for h in range(KH):
        hs = pl.ds(h * H, H)
        raw = dot(s.x1[...], s.kw[:, hs])
        s.k_raw[:, hs] = raw
        s.kv[own_rows, 2 * h * H : (2 * h + 1) * H] = rope(raw * rms(raw) * gk[...]).astype(BF16)
        s.kv[own_rows, (2 * h + 1) * H : (2 * h + 2) * H] = dot(s.x1[...], s.vw[:, hs]).astype(BF16)
        if h == 0:
            pl.semaphore_wait(barrier, (nt - 1) + (2 * n - 1))
        kv_send(1, h)
    l_cot.wait()
    pl.when(zh == 1)(lambda: mirror(0, s.cot, s.cot2).start())
    for r in range(1, reach + 1):

        @pl.when(z < r)
        def _():
            s.kv[pl.ds((reach - r) * T, T), :] = jnp.zeros((T, 2 * KV), BF16)

    l_qw.wait()
    s.q_raw[...] = dot(s.x1[...], s.qw[...])
    for h in range(QH):
        raw = s.q_raw[:, h * H : (h + 1) * H]
        s.q_rot[:, h * H : (h + 1) * H] = rope(raw * rms(raw) * gq[...]).astype(BF16)
    for r in range(1, reach + 1):
        for c in range(KH):

            @pl.when(z >= r)
            def _(r=r, c=c):
                kv_copy(r, c).wait_recv()

            if r < reach:
                kv_send(r + 1, c)
    def weights_of(h, g):
        hs = pl.ds(pl.multiple_of(h * H, H), H)
        q = s.q_rot[:, hs]
        k = s.kv[:, pl.ds(pl.multiple_of(2 * g * H, H), H)]
        return q, k, jnp.where(s.mask[...] > 0.0, jnp.exp(dot_nt(q, k) * inv_root), 0.0)

    def attend(h, _):
        g = h // group
        hs = pl.ds(pl.multiple_of(h * H, H), H)
        _q, _k, w = weights_of(h, g)
        v = s.kv[:, pl.ds(pl.multiple_of((2 * g + 1) * H, H), H)]
        total = jnp.sum(w, axis=-1, keepdims=True)
        att = dot(w.astype(BF16), v) / total
        s.tot[:, hs] = jnp.broadcast_to(total, (T, H))
        s.att[:, hs] = att
        s.att_low[:, hs] = att.astype(BF16)
        s.attt[hs, :] = att.T.astype(BF16)
        return 0

    lax.fori_loop(0, QH, attend, 0)

    l_ow.wait()

    def body(c, w):
        s.send_a[:, pl.ds(c, w)] = dot(s.att_low[...], s.ow[:, pl.ds(c, w)]).astype(BF16)

    tiles(D, TILE, body)
    scatter_start(0, s.send_a, s.recv0)

    def transpose_half(src, dst, place):
        for d in range(2):

            def body(c, w):
                cs = pl.ds(pl.multiple_of((d * n + zh * nl) * R + c, 128), w)
                rows = pl.ds(pl.multiple_of(d * nl * R + c, 128), w)
                dst[rows, place * T : (place + 1) * T] = src[:, cs].astype(F32).T.astype(BF16)

            tiles(nl * R, TILE, body)

    s.cotshare[...] = s.cot[mine, :].astype(F32)

    transpose_half(s.x1, s.x1t, 0)
    transpose_half(s.cot, s.cott, 0)
    l_dw.wait()

    def hidden_grad(cot, out):
        def body(c, w):
            out[:, pl.ds(c, w)] = dot_nt(cot[...], s.dw[pl.ds(c, w), :])

        tiles(F, TILE, body)

    def cot_share():
        mirror(0, s.cot, s.cot2).wait_recv()
        gather_start(9, s.cot2)

    hidden_grad(s.cot, s.gh)
    pl.when(z == nl - 1)(lambda: mirror(0, s.cot, s.cot2).start())

    s.resid[...] = scatter_sum(0, s.send_a, s.recv0, s.tokshare[...])
    resid = s.resid[...]
    s.x2[mine, :] = (resid * rms(resid) * g2[...]).astype(BF16)
    gather_start(1, s.x2)
    mirror(1, s.x2, s.x2b).start()
    l_gw.wait()
    l_uw.wait()
    gather_forward(1, s.x2)
    pl.when(z < nl - 1)(lambda: mirror(0, s.cot, s.cot2).start())
    gather_wait(1, s.x2)

    def mirrored_share():
        mirror(1, s.x2, s.x2b).wait_recv()
        gather_start(10, s.x2b)

    cot_share()

    def feed(x, grad_hidden, place):
        rows = pl.ds(place * T, T)

        def body(c, w):
            cs = pl.ds(c, w)
            gate = dot(x[...], s.gw[:, cs])
            up = dot(x[...], s.uw[:, cs])
            gh = grad_hidden[:, cs]
            sig = jax.nn.sigmoid(gate)
            act = gate * sig
            s.hid[rows, cs] = (act * up).astype(BF16)
            s.gg[rows, cs] = (gh * up * (sig * (1.0 + gate * (1.0 - sig)))).astype(BF16)
            s.gu[rows, cs] = (gh * act).astype(BF16)

        tiles(F, TILE, body)

    feed(s.x2, s.gh, 0)
    mirrored_share()
    gather_forward(9, s.cot2)
    gather_line_start(2, s.attt, att_all)
    own_part = pl.ds(0, T)

    def body(c, w):
        rs = pl.ds(c, w)
        s.send_a[:, rs] = (
            dot_nt(s.gg[own_part, :], s.gw[rs, :]) + dot_nt(s.gu[own_part, :], s.uw[rs, :])
        ).astype(BF16)

    tiles(D, TILE, body)
    transpose_half(s.x2, s.xt, 0)
    gather_forward(10, s.x2b)
    mirror(1, s.x2, s.x2b).wait_send()
    scatter_start(2, s.send_a, s.recv1)
    for d in range(2):
        mirror_x1(d).start()

    def body(c, w):
        s.send_b[:, pl.ds(c, w)] = dot(s.hid[own_part, :], s.dw[:, pl.ds(c, w)]).astype(BF16)

    tiles(D, TILE, body)
    gather_wait(9, s.cot2)
    hidden_grad(s.cot2, s.gh2)
    transpose_half(s.cot2, s.cott, 1)
    gather_wait(10, s.x2b)
    feed(s.x2b, s.gh2, 1)
    transpose_half(s.x2b, s.xt, 1)
    pl.semaphore_signal(s.credit, inc=1, device_id={"dp": 1 - dp}, device_id_type=MESH)

    grad_second = scatter_sum(2, s.send_a, s.recv1, jnp.zeros((S, D), F32))
    resid = s.resid[...]
    scale = rms(resid)
    normed = resid * scale
    s.gains[:, D : 2 * D] = jnp.sum(grad_second * normed, axis=0, keepdims=True)
    scaled = grad_second * g2[...]
    inner = jnp.mean(scaled * normed, axis=-1, keepdims=True)
    s.gresid[...] = s.cotshare[...] + scale * (scaled - normed * inner)
    s.gm[mine, :] = s.gresid[...].astype(BF16)
    gather_start(4, s.gm)
    columns_start(2, s.gm, s.gmc)

    class WeightJob:
        def __init__(self, k, left, grad):
            self.k, self.left, self.grad, self.cols = k, left, grad, grad.shape[1]

        def part(self, block, c, w):
            rows = pl.ds(pl.multiple_of(block * R, R), R)
            return dot(self.left[rows, :], self.grad[:, pl.ds(c, w)])

        def dp_slot(self, b):
            return s.gw.at[pl.ds(b * R, R), pl.ds(0, self.cols)]

        def dp_recv(self, b):
            return s.uw.at[pl.ds(pl.multiple_of((self.k * nl + b) * R, R), R), pl.ds(0, self.cols)]

        def chain_slot(self, up, step):
            i = nl + self.k * (nl - 1) + (step if up else nl - 2 - step)
            return s.gw.at[pl.ds(i * R, R), pl.ds(0, self.cols)]

        def chain(self, up, step):
            return s.chain.at[self.k, 0 if up or nl == 2 else 1, step, :, pl.ds(0, self.cols)]

    jobs = [
        WeightJob(0, s.cott, s.hid),
        WeightJob(1, s.xt, s.gg),
        WeightJob(2, s.xt, s.gu),
        WeightJob(3, s.x1t, s.dqkv),
    ]
    order = [b for i in range((nl + 1) // 2) for b in dict.fromkeys((nl - 1 - i, i))]

    def job_dp(k):
        for b in order:
            if k:
                job_dp_wait_send(jobs[k - 1], k - 1, b)
            job_dp_start(jobs[k], k, b)

    pl.semaphore_wait(s.credit, 1)
    job_dp(0)
    job_dp_wait_all(jobs[0], 0)
    chain_step(jobs[0], 0, 0)
    gather_forward(4, s.gm)
    gather_line_step(2, att_all, 1)
    job_dp(1)
    gather_wait(4, s.gm)
    scatter_start(3, s.send_b, s.recv2)
    for d in range(2):
        mirror_x1(d).wait_recv()

    def body(c, w):
        s.x1t[pl.ds(c, w), T : 2 * T] = s.x1b[:, pl.ds(c, w)].astype(F32).T.astype(BF16)

    tiles(D // 2, TILE, body)

    gatt = s.gh.at[:, pl.ds(0, QH * H)]

    def body(c, w):
        gatt[:, pl.ds(c, w)] = dot_nt(s.gm[...], s.ow[pl.ds(c, w), :])

    tiles(QH * H, TILE, body)
    s.gq_acc[...] = jnp.zeros((1, H), F32)

    def back(g, _):
        ks = pl.ds(pl.multiple_of(g * H, H), H)
        vs = pl.ds(pl.multiple_of(KV + g * H, H), H)
        v = s.kv[:, pl.ds(pl.multiple_of((2 * g + 1) * H, H), H)]
        grad_k = jnp.zeros((span, H), F32)
        grad_v = jnp.zeros((span, H), F32)
        for i in range(group):
            h = g * group + i
            hs = pl.ds(pl.multiple_of(h * H, H), H)
            q, k, w = weights_of(h, g)
            ga, total = gatt[:, hs], s.tot[:, hs]
            gs = (ga / total).astype(BF16)
            delta = jnp.sum(ga * s.att[:, hs], axis=-1, keepdims=True) / total[:, :1]
            ds = (w * (dot_nt(gs, v) - delta)).astype(BF16)
            grad_k = grad_k + dot_tn(ds, q) * inv_root
            grad_v = grad_v + dot_tn(w.astype(BF16), gs)
            gr = rope_back(dot(ds, k) * inv_root)
            raw = s.q_raw[:, hs]
            r = rms(raw)
            nq = raw * r
            s.gq_acc[...] += jnp.sum(gr * nq, axis=0, keepdims=True)
            sc = gr * gq[...]
            s.dqkv[:T, hs] = (r * (sc - nq * jnp.mean(sc * nq, axis=-1, keepdims=True))).astype(BF16)
        s.dkv[:, ks] = grad_k.astype(BF16)
        s.dkv[:, vs] = grad_v.astype(BF16)
        return 0

    lax.fori_loop(0, KH, back, 0)
    s.gains[:, 2 * D : 2 * D + H] = s.gq_acc[...]

    def dkv_copy(i):
        return remote(
            s.dkv.at[pl.ds(i * T, T)], s.dkv_in.at[i], s.dkv_s.at[i], s.dkv_r.at[i], ctx=z - 1
        )

    for i in range(reach):
        if i:

            @pl.when((z < n - 1) & (z + 1 >= reach - i + 1))
            def _():
                dkv_copy(i - 1).wait_recv()
                rows = pl.ds(i * T, T)
                s.dkv[rows, :] = (s.dkv[rows, :].astype(F32) + s.dkv_in[i - 1].astype(F32)).astype(BF16)

        @pl.when(z >= reach - i)
        def _():
            dkv_copy(i).start()

        if i == 0:
            job_dp_wait_all(jobs[1], 1)
            chain_step(jobs[1], 1, 0, (True,))
            pl.when(zh == 0)(lambda: chain_step(jobs[1], 1, 0, (False,), (0,)))
            job_dp(2)

    pl.when(zh == 0)(lambda: chain_step(jobs[1], 1, 0, (False,), (1,)))

    @pl.when(z < n - 1)
    def _():
        dkv_copy(reach - 1).wait_recv()

    own = s.dkv[pl.ds(reach * T, T), :].astype(F32)
    own = own + jnp.where(z < n - 1, s.dkv_in[reach - 1].astype(F32), 0.0)
    s.dqkv[:T, QH * H + KV :] = own[:, KV:].astype(BF16)
    gk_sum = jnp.zeros((1, H), F32)
    for h in range(KH):
        gr = rope_back(own[:, h * H : (h + 1) * H])
        raw = s.k_raw[:, h * H : (h + 1) * H]
        r = rms(raw)
        nk = raw * r
        gk_sum = gk_sum + jnp.sum(gr * nk, axis=0, keepdims=True)
        sc = gr * gk[...]
        s.dqkv[:T, QH * H + h * H : QH * H + (h + 1) * H] = (
            r * (sc - nk * jnp.mean(sc * nk, axis=-1, keepdims=True))
        ).astype(BF16)
    s.gains[:, 2 * D + H :] = gk_sum
    pl.when(zh == 1)(lambda: chain_step(jobs[1], 1, 0, (False,)))
    mirror_qkv().start()
    gather_line_step(2, att_all, 2)
    job_dp_wait_all(jobs[2], 2)
    chain_step(jobs[2], 2, 0)

    s.outsh[...] = scatter_sum(3, s.send_b, s.recv2, s.resid[...]).astype(BF16)
    q_c, k_c, v_c = pl.ds(0, QH * H), pl.ds(QH * H, KV), pl.ds(QH * H + KV, KV)

    def body(c, w):
        rs = pl.ds(c, w)
        s.send_a[:, rs] = (
            dot_nt(s.dqkv[:T, q_c], s.qw[rs, :])
            + dot_nt(s.dqkv[:T, k_c], s.kw[rs, :])
            + dot_nt(s.dqkv[:T, v_c], s.vw[rs, :])
        ).astype(BF16)

    tiles(D, TILE, body)
    scatter_start(6, s.send_a, s.recv3)
    grad_first = scatter_sum(6, s.send_a, s.recv3, jnp.zeros((S, D), F32))
    tokshare = s.tokshare[...]
    scale = rms(tokshare)
    normed = tokshare * scale
    s.gains[:, :D] = jnp.sum(grad_first * normed, axis=0, keepdims=True)
    scaled = grad_first * g1[...]
    inner = jnp.mean(scaled * normed, axis=-1, keepdims=True)
    s.tgsh[...] = (s.gresid[...] + scale * (scaled - normed * inner)).astype(BF16)
    for j in range(1, nt):
        remote(s.gains, s.gains_p.at[j - 1], s.pl_s.at[8, j - 1], s.pl_r.at[8, j - 1], tensor=t ^ j).start()
    spread_start(7, s.tgsh, tgrad_hbm, 1)
    for j in range(1, nt):
        remote(s.gains, s.gains_p.at[j - 1], s.pl_s.at[8, j - 1], s.pl_r.at[8, j - 1], tensor=t ^ j).wait()
    total = s.gains[...]
    for j in range(1, nt):
        total = total + s.gains_p[j - 1]
    s.gains2[...] = total

    def gain_copy(e, d):
        i = e * n + d
        return remote(
            s.gains2, s.gains_x.at[i - 1], s.ga_s.at[i], s.ga_r.at[i], dp=dp ^ e, ctx=lax.rem(z + d, n)
        )

    for e in range(2):
        for d in range(n):
            if e or d:
                gain_copy(e, d).start()
    columns_wait_recv(2, s.gm, s.gmc)
    share_start(2, s.gmc)
    spread_start(5, s.outsh, out_hbm, 0)
    stage = s.gh2.at[pl.ds(0, R), pl.ds(0, QH * H + 2 * KV)]

    def gate_copy():
        return pltpu.make_async_copy(s.gh.at[pl.ds(0, R)], gate_out, s.load_sem.at[2])

    def up_copy():
        return pltpu.make_async_copy(s.gh.at[pl.ds(0, R)], up_out, s.load_sem.at[3])

    def qkv_copies():
        parts = [(q_out, 0, QH * H), (k_out, QH * H, KV), (v_out, QH * H + KV, KV)]
        return [
            pltpu.make_async_copy(stage.at[:, pl.ds(a, w)], ref, s.load_sem.at[6 + i])
            for i, (ref, a, w) in enumerate(parts)
        ]

    for step in range(1, nl - 1):
        for k in range(3):
            chain_step(jobs[k], k, step)
    rows = pl.ds(0, R)
    chain_final(jobs[0], 0, s.gh.at[rows])
    width = min(256, F)
    flip = s.gh2.at[:, pl.ds(QH * H + 2 * KV, 2 * R)]

    def down_copy(i):
        return pltpu.make_async_copy(
            flip.at[pl.ds(0, width), pl.ds((i % 2) * R, R)],
            down_out.at[pl.ds(i * width, width)],
            s.load_sem.at[4 + i % 2],
        )

    count = F // width
    for i in range(count):
        if i >= 2:
            down_copy(i - 2).wait()
        flip[:width, (i % 2) * R : (i % 2 + 1) * R] = s.gh[rows, i * width : (i + 1) * width].T
        down_copy(i).start()
    for i in range(max(0, count - 2), count):
        down_copy(i).wait()
    mirror_qkv().wait_recv()
    job_dp(3)
    job_dp_wait_all(jobs[3], 3)
    chain_step(jobs[3], 3, 0)
    for step in range(1, nl - 1):
        chain_step(jobs[3], 3, step)


    chain_final(jobs[1], 1, s.gh.at[rows])
    gate_copy().start()
    for step in range(3, n):
        gather_line_step(2, att_all, step)
    gather_line_finish(2, s.attt, att_all)
    share_wait(2, s.gmc)

    def load(i):
        slot = lax.rem(i, 2)
        return pltpu.make_async_copy(
            att_all.at[i // n, lax.rem(i, n)],
            s.dw.at[pl.ds(pl.multiple_of(slot * QH * H, QH * H), QH * H), pl.ds(0, T)],
            s.stage_sem.at[slot],
        )

    load(0).start()
    s.outw[...] = jnp.zeros(s.outw.shape, F32)

    def step(i, _):
        @pl.when(i + 1 < 2 * n)
        def _():
            load(i + 1).start()

        load(i).wait()
        slot = lax.rem(i, 2)
        left = s.dw[pl.ds(pl.multiple_of(slot * QH * H, QH * H), QH * H), pl.ds(0, T)]
        s.outw[...] += dot(left, s.gmc[:, i].reshape(T, R))
        return 0

    lax.fori_loop(0, 2 * n, step, 0)

    def outw_copy():
        return pltpu.make_async_copy(s.outw, outw_out, s.load_sem.at[4])

    outw_copy().start()
    gate_copy().wait()
    chain_final(jobs[2], 2, s.gh.at[rows])
    up_copy().start()
    chain_final(jobs[3], 3, stage)
    for copy in qkv_copies():
        copy.start()
    for e in range(2):
        for d in range(n):
            if e or d:
                gain_copy(e, d).wait()
    total = s.gains2[...]
    for i in range(2 * n - 1):
        total = total + s.gains_x[i]
    s.gains[...] = total

    def gains_copy():
        return pltpu.make_async_copy(s.gains, gains_out, s.load_sem.at[2])

    gains_copy().start()

    columns_wait_send(2, s.gm, s.gmc)
    mirror(0, s.cot, s.cot2).wait_send()
    mirror_qkv().wait_send()
    for d in range(2):
        mirror_x1(d).wait_send()
    for b in order:
        job_dp_wait_send(jobs[-1], len(jobs) - 1, b)
    for st in range(nl - 1):
        for k, job in enumerate(jobs):
            chain_wait_send(job, k, st)
    for r in range(1, reach + 1):

        @pl.when((z < n - 1) & (z >= r - 1))
        def _(r=r):
            for c in range(KH):
                kv_copy(r, c).wait_send()

    for i in range(reach):

        @pl.when(z >= reach - i)
        def _():
            dkv_copy(i).wait_send()

    spread_wait(5, s.outsh, out_hbm, 0)
    spread_wait(7, s.tgsh, tgrad_hbm, 1)
    gains_copy().wait()
    up_copy().wait()
    outw_copy().wait()
    for copy in qkv_copies():
        copy.wait()


def run_layer(dm, *operands):
    T, D, H, F, n, nt, reach, S, R = dm.T, dm.D, dm.H, dm.F, dm.n, dm.nt, dm.reach, dm.S, dm.R
    QC, KV = dm.QH * H, dm.KH * H
    span = (reach + 1) * T
    G = 2 * D + 2 * H
    dma = pltpu.SemaphoreType.DMA
    scratch = dict(
        tok=((T, D), BF16), x1=((T, D), BF16), send_b=((T, D), BF16), cot=((T, D), BF16), x2=((T, D), BF16),
        outsh=((S, D), BF16), tgsh=((S, D), BF16), xt=((D // 2, 2 * T), BF16), cott=((D // 2, 2 * T), BF16),
        cot2=((T, D), BF16), x2b=((T, D), BF16),
        qw=((D, QC), BF16), kw=((D, KV), BF16), vw=((D, KV), BF16), ow=((QC, D), BF16),
        gw=((D, F), BF16), uw=((D, F), BF16), dw=((F, D), BF16),
        tokshare=((S, D), F32), cotshare=((S, D), F32), resid=((S, D), F32), gresid=((S, D), F32),
        k_raw=((T, KV), F32), q_raw=((T, QC), F32), q_rot=((T, QC), BF16), kv=((span, 2 * KV), BF16),
        mask=((T, span), F32), tot=((T, QC), F32), att=((T, QC), F32), att_low=((T, QC), BF16),
        attt=((QC, T), BF16), gq_acc=((1, H), F32),
        recv0=((6, S, D // 2) if nt == 4 else (nt - 1, S, D), BF16),
        recv1=((6, S, D // 2) if nt == 4 else (nt - 1, S, D), BF16), pair=((2, S, D // 2), BF16),
        gh=((T, F), F32), hid=((2 * T, F), BF16), gg=((2 * T, F), BF16), gu=((2 * T, F), BF16),
        dkv=((span, 2 * KV), BF16), dkv_in=((reach, T, 2 * KV), BF16), dqkv=((2 * T, QC + 2 * KV), BF16),
        chain=((4, 1 if n == 4 else 2, n // 2 - 1, R, F), BF16),

        gmc=((nt, 2 * n, S, R), BF16), x1b=((T, D // 2), BF16), x1t=((D // 2, 2 * T), BF16), gh2=((T, F), F32),
        cos=((T, H), F32), sin=((T, H), F32), segs=((1, reach * T + dm.L), jnp.int32),
        outw=((QC, R), F32), gain_in=((1, G), F32), gains=((1, G), F32), gains2=((1, G), F32), gains_p=((nt - 1, 1, G), F32),
        gains_x=((2 * n - 1, 1, G), F32),
    )
    sems = dict(
        load_sem=(9,), own_sem=(3,), pl_s=(13, nt - 1), pl_r=(13, nt - 1), ag_s=(3, 2, n - 1), ag_r=(3, 2, n - 1),
        agx_s=(3, 2 * n - 1), agx_r=(3, 2 * n - 1), aa_s=(3, 2 * n), aa_r=(3, 2 * n), stage_sem=(2,),
        dp_s=(4, n // 2), dp_r=(4, n // 2), ch_s=(4, 2, n // 2 - 1, 2), ch_r=(4, 2, n // 2 - 1, 2), mi_s=(5,), mi_r=(5,), kv_s=(reach, KV // H), kv_r=(reach, KV // H), pl2_s=(11,), pl2_r=(11,), rs_s=(7, 6), rs_r=(7, 6),
        dkv_s=(reach,), dkv_r=(reach,), ga_s=(2 * n,), ga_r=(2 * n,),
    )
    names = list(scratch) + list(sems) + ["credit"]
    shapes = [pltpu.VMEM(*v) for v in scratch.values()] + [dma(v) for v in sems.values()]
    shapes.append(pltpu.SemaphoreType.REGULAR)

    def body(*refs):
        fixed = len(refs) - len(names)
        s = Dims()
        for name, ref in zip(names, refs[fixed:]):
            setattr(s, name, ref)
        for alias, of in dm.alias.items():
            setattr(s, alias, getattr(s, of))
        layer_kernel(dm, *refs[:fixed], s)

    hbm = pl.BlockSpec(memory_space=pl.ANY)
    vmem = pl.BlockSpec(memory_space=pltpu.VMEM)
    return pl.pallas_call(
        body,
        out_shape=(
            jax.ShapeDtypeStruct((T, D), BF16),
            jax.ShapeDtypeStruct((T, D), BF16),
            jax.ShapeDtypeStruct((R, F), F32),
            jax.ShapeDtypeStruct((R, F), F32),
            jax.ShapeDtypeStruct((F, R), F32),
            jax.ShapeDtypeStruct((R, QC), F32),
            jax.ShapeDtypeStruct((R, KV), F32),
            jax.ShapeDtypeStruct((R, KV), F32),
            jax.ShapeDtypeStruct((QC, R), F32),
            jax.ShapeDtypeStruct((1, G), F32),
            jax.ShapeDtypeStruct((2, n, QC, T), BF16),
        ),
        in_specs=[hbm] * 2 + [vmem] * 6 + [hbm] * 7,
        out_specs=[hbm] * 11,
        scratch_shapes=shapes,
        compiler_params=pltpu.CompilerParams(
            collective_id=0, has_side_effects=True, vmem_limit_bytes=67043328
        ),
        name="layer",
    )(*operands)


FINISH_WINDOW = 64


def finish_pieces(shape):
    rows = shape[0]
    step = rows // 2 if rows % 32 == 0 else rows
    return [(r, step) for r in range(0, rows, step)]


def finish_kernel(dm, *refs):
    count = len(dm.finish)
    ins, gains, outs = refs[:count], refs[count], refs[count + 1 : 2 * count + 1]
    gain_outs = refs[2 * count + 1 : 2 * count + 5]
    bufs, load_sem, store_sem = refs[2 * count + 5 : 3 * count + 5], refs[-2], refs[-1]
    loads, stores = [], []
    for a, b, c in zip(ins, bufs, outs):
        for start, size in finish_pieces(a.shape):
            rows, i = pl.ds(start, size), len(loads)
            loads.append(pltpu.make_async_copy(a.at[rows], b.at[rows], load_sem.at[i]))
            stores.append(pltpu.make_async_copy(b.at[rows], c.at[rows], store_sem.at[i]))
    for load in loads[:FINISH_WINDOW]:
        load.start()
    place = 0
    for ref in gain_outs:
        ref[...] = gains[:, place : place + ref.shape[1]]
        place += ref.shape[1]
    for i, (load, store) in enumerate(zip(loads, stores)):
        load.wait()
        store.start()
        if i + FINISH_WINDOW < len(loads):
            loads[i + FINISH_WINDOW].start()
    for store in stores:
        store.wait()


def finish(dm, arrays, gains):
    dm.finish = arrays
    hbm = pl.BlockSpec(memory_space=pl.ANY)
    vmem = pl.BlockSpec(memory_space=pltpu.VMEM)
    shapes = [jax.ShapeDtypeStruct(a.shape, a.dtype) for a in arrays]
    gain_shapes = [jax.ShapeDtypeStruct((1, w), F32) for w in (dm.D, dm.D, dm.H, dm.H)]
    dma = pltpu.SemaphoreType.DMA((sum(len(finish_pieces(a.shape)) for a in arrays),))
    return pl.pallas_call(
        functools.partial(finish_kernel, dm),
        out_shape=tuple(shapes + gain_shapes),
        in_specs=[hbm] * len(arrays) + [vmem],
        out_specs=tuple([hbm] * len(arrays) + [vmem] * 4),
        scratch_shapes=[pltpu.VMEM(a.shape, a.dtype) for a in arrays] + [dma, dma],
        compiler_params=pltpu.CompilerParams(vmem_limit_bytes=67043328),
        name="finish",
    )(*arrays, gains)


def per_device(
    tokens,
    segments,
    first_gain,
    query_weight,
    key_matrix,
    value_matrix,
    query_norm_gain,
    key_gain,
    output_weight,
    second_gain,
    gate_weight,
    up_weight,
    down_weight,
    cotangent,
):
    _, T, D = tokens.shape
    dm = Dims()
    dm.T, dm.D, dm.H, dm.F = T, D, query_norm_gain.shape[0], gate_weight.shape[1]
    dm.QH, dm.KH = query_weight.shape[1] // dm.H, key_matrix.shape[1] // dm.H
    dm.n, dm.nt = lax.axis_size("ctx"), lax.axis_size("tensor")
    length = segments.shape[1]
    dm.reach = -(-(length // 2 - 1) // T)
    dm.S, dm.R = T // dm.nt, D // (2 * dm.n)
    dm.alias = {"send_a": "tok", "gm": "x2", "recv2": "recv0", "recv3": "recv1"}
    H = dm.H
    dm.L = length
    inverse = (1.0 / rope_base ** (np.arange(0, H, 2, dtype=np.float32) / np.float32(H))).astype(np.float32)
    inverse = np.concatenate([inverse, inverse])[None]
    out, tgrad, gate_g, up_g, down_g, q_g, k_g, v_g, out_g, gains = run_layer(
        dm,
        tokens.reshape(T, D),
        cotangent.reshape(T, D),
        first_gain.reshape(-1, H),
        second_gain.reshape(-1, H),
        query_norm_gain.reshape(1, H),
        key_gain.reshape(1, H),
        inverse,
        segments,
        query_weight,
        key_matrix,
        value_matrix,
        output_weight,
        gate_weight,
        up_weight,
        down_weight,
    )[:10]
    out, tgrad, gate_g, up_g, down_g, q_g, k_g, v_g, out_g, first_g, second_g, qn_g, kn_g = finish(
        dm, (out, tgrad, gate_g, up_g, down_g, q_g, k_g, v_g, out_g), gains
    )
    return (
        out.reshape(tokens.shape),
        tgrad.reshape(tokens.shape),
        first_g.reshape(D),
        q_g,
        k_g,
        v_g,
        qn_g.reshape(H),
        kn_g.reshape(H),
        out_g,
        second_g.reshape(D),
        gate_g,
        up_g,
        down_g,
    )


def solution(mesh):
    return jax.shard_map(
        per_device,
        mesh=mesh,
        in_specs=(
            P("dp", "ctx", None),
            P("dp", None),
            P(),
            P(None, "tensor"),
            P(None, "tensor"),
            P(None, "tensor"),
            P(),
            P(),
            P("tensor", None),
            P(),
            P(None, "tensor"),
            P(None, "tensor"),
            P("tensor", None),
            P("dp", "ctx", None),
        ),
        out_specs=(
            P("dp", "ctx", None),
            P("dp", "ctx", None),
            P(),
            P(("dp", "ctx"), "tensor"),
            P(("dp", "ctx"), "tensor"),
            P(("dp", "ctx"), "tensor"),
            P(),
            P(),
            P("tensor", ("dp", "ctx")),
            P(),
            P(("dp", "ctx"), "tensor"),
            P(("dp", "ctx"), "tensor"),
            P("tensor", ("dp", "ctx")),
        ),
        check_vma=False,
    )
```

```python
import functools
import math

import jax
import jax.numpy as jnp
import numpy as np
from jax import lax
from jax.experimental import pallas as pl
from jax.experimental.pallas import tpu as pltpu
from jax.sharding import PartitionSpec as P

epsilon = 1e-06
rope_base = 1000000.0
F32 = jnp.float32
BF16 = jnp.bfloat16
MESH = pl.DeviceIdType.MESH
TILE = 256


def dot(a, b):
    return jnp.dot(a, b, preferred_element_type=F32)


def dot_nt(a, b):
    return lax.dot_general(a, b, (((1,), (1,)), ((), ())), preferred_element_type=F32)


def dot_tn(a, b):
    return lax.dot_general(a, b, (((0,), (0,)), ((), ())), preferred_element_type=F32)


def remote(src, dst, send_sem, recv_sem, **device):
    return pltpu.make_async_remote_copy(
        src_ref=src,
        dst_ref=dst,
        send_sem=send_sem,
        recv_sem=recv_sem,
        device_id=device,
        device_id_type=MESH,
    )


def tiles(total, size, body):
    size = min(size, total)

    def step(i, _):
        body(pl.multiple_of(i * size, size), size)
        return 0

    lax.fori_loop(0, total // size, step, 0)


class Dims:
    pass


def layer_kernel(
    dm,
    tok_hbm,
    cot_hbm,
    first_in,
    second_in,
    query_in,
    key_in,
    inverse,
    seg_row,
    qw_hbm,
    kw_hbm,
    vw_hbm,
    ow_hbm,
    gw_hbm,
    uw_hbm,
    dw_hbm,
    out_hbm,
    tgrad_hbm,
    gate_out,
    up_out,
    down_out,
    q_out,
    k_out,
    v_out,
    outw_out,
    gains_out,
    att_all,
    s,
):
    T, D, H, QH, KH, F, n, nt, reach, S, R = (
        dm.T, dm.D, dm.H, dm.QH, dm.KH, dm.F, dm.n, dm.nt, dm.reach, dm.S, dm.R,
    )
    group = QH // KH
    span = (reach + 1) * T
    KV = KH * H
    inv_root = 1.0 / math.sqrt(H)
    C = R // nt
    gain_in = s.gain_in
    for place, ref in ((0, first_in), (D, second_in), (2 * D, query_in), (2 * D + H, key_in)):
        for i in range(ref.shape[0]):
            gain_in[:, place + i * H : place + (i + 1) * H] = ref[i : i + 1, :].astype(F32)
    g1 = gain_in.at[:, pl.ds(0, D)]
    g2 = gain_in.at[:, pl.ds(D, D)]
    gq = gain_in.at[:, pl.ds(2 * D, H)]
    gk = gain_in.at[:, pl.ds(2 * D + H, H)]
    cos, sin = s.cos, s.sin
    dp, z, t = lax.axis_index("dp"), lax.axis_index("ctx"), lax.axis_index("tensor")
    zz = n - 1 - z
    nl = n // 2
    zh, zl = z // nl, lax.rem(z, nl)
    zzl = nl - 1 - zl

    barrier = pltpu.get_barrier_semaphore()
    for j in range(1, nt):
        pl.semaphore_signal(barrier, inc=1, device_id={"tensor": t ^ j}, device_id_type=MESH)
    for e in range(2):
        for d in range(n):
            if e or d:
                pl.semaphore_signal(
                    barrier,
                    inc=1,
                    device_id={"dp": dp ^ e, "ctx": lax.rem(z + d, n)},
                    device_id_type=MESH,
                )

    loads = [
        (tok_hbm, s.tok), (cot_hbm, s.cot), (kw_hbm, s.kw), (vw_hbm, s.vw), (qw_hbm, s.qw),
        (ow_hbm, s.ow), (dw_hbm, s.dw), (gw_hbm, s.gw), (uw_hbm, s.uw),
    ]
    loads = [pltpu.make_async_copy(a, b, s.load_sem.at[i]) for i, (a, b) in enumerate(loads)]
    for load in loads:
        load.start()
    (l_tok, l_cot, l_kw, l_vw, l_qw, l_ow, l_dw, l_gw, l_uw) = loads

    def scatter_direct(k, buf, recv, j):
        peer = t ^ j
        return remote(
            buf.at[pl.ds(pl.multiple_of(peer * S, S), S)], recv.at[j - 1],
            s.pl_s.at[k, j - 1], s.pl_r.at[k, j - 1], tensor=peer,
        )

    def scatter_first(k, buf, recv, slot):
        to = t ^ (1 if slot < 2 else 2)
        rows = pl.ds(pl.multiple_of((to if slot % 2 == 0 else t ^ 3) * S, S), S)
        cols = pl.ds(0 if slot < 2 else D // 2, D // 2)
        return remote(buf.at[rows, cols], recv.at[slot], s.rs_s.at[k, slot], s.rs_r.at[k, slot], tensor=to)

    def scatter_second(k, recv, slot):
        to = t ^ (2 if slot == 4 else 1)
        return remote(s.pair.at[slot - 4], recv.at[slot], s.rs_s.at[k, slot], s.rs_r.at[k, slot], tensor=to)

    def scatter_start(k, buf, recv):
        if nt == 4:
            for slot in (1, 3, 0, 2):
                scatter_first(k, buf, recv, slot).start()
        else:
            for j in range(1, nt):
                scatter_direct(k, buf, recv, j).start()

    def scatter_sum(k, buf, recv, base):
        own = pl.ds(pl.multiple_of(t * S, S), S)
        if nt == 4:
            for slot, peer, cols in ((1, t ^ 2, slice(0, D // 2)), (3, t ^ 1, slice(D // 2, D))):
                scatter_first(k, buf, recv, slot).wait_recv()
                rows = pl.ds(pl.multiple_of(peer * S, S), S)
                both = buf[rows, cols].astype(F32) + recv[slot].astype(F32)
                s.pair[slot // 2] = both.astype(BF16)
                scatter_second(k, recv, 4 + slot // 2).start()
            for slot in (0, 2):
                scatter_first(k, buf, recv, slot).wait_recv()
            for slot in range(4):
                scatter_first(k, buf, recv, slot).wait_send()
            for slot in (4, 5):
                scatter_second(k, recv, slot).wait()
            left = buf[own, 0 : D // 2].astype(F32) + recv[0].astype(F32) + recv[4].astype(F32)
            right = buf[own, D // 2 : D].astype(F32) + recv[2].astype(F32) + recv[5].astype(F32)
            return base + jnp.concatenate([left, right], axis=1)
        for j in range(1, nt):
            scatter_direct(k, buf, recv, j).wait()
        total = base + buf[own, :].astype(F32)
        for j in range(1, nt):
            total = total + recv[j - 1].astype(F32)
        return total

    def rows_of(peer, half=None):
        if half is None:
            return pl.ds(pl.multiple_of(peer * S, S), S)
        return pl.ds(pl.multiple_of(peer * S + half * (S // 2), S // 2), S // 2)

    def gather_copy(k, full, j):
        rows = rows_of(t)
        return remote(full.at[rows], full.at[rows], s.pl_s.at[k, j - 1], s.pl_r.at[k, j - 1], tensor=t ^ j)

    def gather_arrived(k, full, j):
        rows = rows_of(t ^ j)
        return remote(full.at[rows], full.at[rows], s.pl_s.at[k, j - 1], s.pl_r.at[k, j - 1], tensor=t ^ j)

    def relay_copy(k, full, origin, half, to):
        rows = rows_of(origin, half)
        sems = (s.pl2_s.at[k], s.pl2_r.at[k]) if half else (s.pl_s.at[k, 2], s.pl_r.at[k, 2])
        return remote(full.at[rows], full.at[rows], *sems, tensor=to)

    def gather_start(k, full):
        for j in range(1, nt) if nt != 4 else (1, 2):
            gather_copy(k, full, j).start()

    def gather_forward(k, full):
        if nt == 4:
            gather_arrived(k, full, 1).wait_recv()
            relay_copy(k, full, t ^ 1, 0, t ^ 2).start()
            gather_arrived(k, full, 2).wait_recv()
            relay_copy(k, full, t ^ 2, 1, t ^ 1).start()

    def gather_wait(k, full):
        for j in range(1, nt) if nt != 4 else (1, 2):
            gather_copy(k, full, j).wait_send()
            if nt != 4:
                gather_arrived(k, full, j).wait_recv()
        if nt == 4:
            relay_copy(k, full, t ^ 1, 0, t ^ 2).wait_send()
            relay_copy(k, full, t ^ 2, 1, t ^ 1).wait_send()
            relay_copy(k, full, t ^ 3, 0, t ^ 2).wait_recv()
            relay_copy(k, full, t ^ 3, 1, t ^ 1).wait_recv()

    mine = pl.ds(pl.multiple_of(t * S, S), S)

    def spread_start(k, share, full, own):
        own_copy(share, full, own).start()
        for j in range(1, nt):
            remote(
                share, full.at[mine], s.pl_s.at[k, j - 1], s.pl_r.at[k, j - 1], tensor=t ^ j
            ).start()

    def own_copy(share, full, own):
        return pltpu.make_async_copy(share, full.at[mine], s.load_sem.at[own])

    def spread_wait(k, share, full, own):
        own_copy(share, full, own).wait()
        for j in range(1, nt):
            peer = t ^ j
            theirs = pl.ds(pl.multiple_of(peer * S, S), S)
            copy = remote(share, full.at[theirs], s.pl_s.at[k, j - 1], s.pl_r.at[k, j - 1], tensor=peer)
            copy.wait_send()
            copy.wait_recv()

    def mirror(i, src, dst):
        return remote(src.at[mine], dst.at[mine], s.mi_s.at[i], s.mi_r.at[i], ctx=zz)

    def mirror_x1(d):
        cols = pl.ds(pl.multiple_of((d * n + (1 - zh) * nl) * R, 128), nl * R)
        return remote(
            s.x1.at[:, cols], s.x1b.at[:, pl.ds(d * nl * R, nl * R)], s.mi_s.at[2 + d], s.mi_r.at[2 + d], ctx=zz
        )

    def mirror_qkv():
        return remote(
            s.dqkv.at[pl.ds(0, T)], s.dqkv.at[pl.ds(T, T)], s.mi_s.at[4], s.mi_r.at[4], ctx=zz
        )

    def line_copy(k, all_ref, up, step, src=None):
        idx = (z - step) if up else (z + step)
        ref = all_ref.at[dp, idx]
        return remote(
            ref if src is None else src, ref,
            s.ag_s.at[k, 0 if up else 1, step], s.ag_r.at[k, 0 if up else 1, step],
            ctx=(z + 1) if up else (z - 1),
        )

    def core_copy(k, all_ref, slot, idx, src=None):
        ref = all_ref.at[dp, idx]
        return remote(
            ref if src is None else src, ref, s.agx_s.at[k, slot], s.agx_r.at[k, slot], dp=1 - dp
        )

    def gather_line_start(k, src, all_ref, ways, own):
        if own:
            pltpu.make_async_copy(src, all_ref.at[dp, z], s.own_sem.at[k]).start()
        for up in ways:

            @pl.when((z < n - 1) if up else (z > 0))
            def _(up=up):
                line_copy(k, all_ref, up, 0, src).start()

        if own:
            core_copy(k, all_ref, 0, z, src).start()

    def gather_line_step(k, all_ref, step, ways=(True, False)):
        for up in ways:

            @pl.when((z >= step) if up else (zz >= step))
            def _(up=up):
                idx = (z - step) if up else (z + step)
                ref = all_ref.at[dp, idx]
                i = 0 if up else 1
                remote(
                    ref, ref, s.ag_s.at[k, i, step - 1], s.ag_r.at[k, i, step - 1],
                    ctx=(z - 1) if up else (z + 1),
                ).wait_recv()
                if step < n - 1:

                    @pl.when((z < n - 1) if up else (z > 0))
                    def _():
                        line_copy(k, all_ref, up, step).start()

                core_copy(k, all_ref, step if up else n - 1 + step, idx).start()

    def gather_line_finish(k, src, all_ref):
        pltpu.make_async_copy(src, all_ref.at[dp, z], s.own_sem.at[k]).wait()
        for step in range(n - 1):

            @pl.when((z >= step) & (z < n - 1))
            def _():
                line_copy(k, all_ref, True, step, src).wait_send()

            @pl.when((zz >= step) & (z > 0))
            def _():
                line_copy(k, all_ref, False, step, src).wait_send()

        def both(slot, idx):
            ref = all_ref.at[1 - dp, idx]
            copy = remote(src, ref, s.agx_s.at[k, slot], s.agx_r.at[k, slot], dp=1 - dp)
            copy.wait_send()
            copy.wait_recv()

        both(0, z)
        for step in range(1, n):

            @pl.when(z >= step)
            def _():
                both(step, z - step)

            @pl.when(zz >= step)
            def _():
                both(n - 1 + step, z + step)

    me = dp * n + z

    def columns_src(k, src, block):
        if k < 2:
            rows = pl.ds(pl.multiple_of(lax.rem(block, n) * R + t * C, C), C)
            return src.at[rows, pl.ds(pl.multiple_of(block // n * T, T), T)]
        return src.at[mine, pl.ds(pl.multiple_of(block * R, R), R)]

    def columns_copy(k, src, all_ref, e, d):
        to_dp, to_z = dp ^ e, lax.rem(z + d, n)
        return remote(
            columns_src(k, src, to_dp * n + to_z), all_ref.at[t, me],
            s.aa_s.at[k, e * n + d], s.aa_r.at[k, e * n + d], dp=to_dp, ctx=to_z,
        )

    def columns_own(k, src, all_ref):
        return pltpu.make_async_copy(columns_src(k, src, me), all_ref.at[t, me], s.aa_s.at[k, 0])

    def columns_start(k, src, all_ref):
        columns_own(k, src, all_ref).start()
        for d in range(n):
            for e in range(2):
                if e or d:
                    columns_copy(k, src, all_ref, e, d).start()

    def columns_wait_send(k, src, all_ref):
        for e in range(2):
            for d in range(n):
                if e or d:
                    columns_copy(k, src, all_ref, e, d).wait_send()

    def columns_wait_recv(k, src, all_ref):
        columns_own(k, src, all_ref).wait()
        for e in range(2):
            for d in range(n):
                if e or d:
                    ref = all_ref.at[t, (dp ^ e) * n + lax.rem(z - d + n, n)]
                    remote(
                        columns_src(k, src, me), ref, s.aa_s.at[k, e * n + d], s.aa_r.at[k, e * n + d],
                        dp=dp ^ e, ctx=lax.rem(z - d + n, n),
                    ).wait_recv()

    def share_start(k, all_ref):
        for j in range(1, nt):
            remote(
                all_ref.at[t], all_ref.at[t], s.pl_s.at[10 + k, j - 1], s.pl_r.at[10 + k, j - 1], tensor=t ^ j
            ).start()

    def share_wait(k, all_ref):
        for j in range(1, nt):
            copy = remote(
                all_ref.at[t], all_ref.at[t ^ j], s.pl_s.at[10 + k, j - 1], s.pl_r.at[10 + k, j - 1], tensor=t ^ j
            )
            copy.wait_send()
            copy.wait_recv()

    def job_dp_start(job, k, b):
        slot = job.dp_slot(b)

        def body(c, w):
            slot[:, pl.ds(c, w)] = job.part((1 - dp) * nl + b, c, w).astype(BF16)

        tiles(job.cols, 512, body)
        remote(slot, job.dp_recv(b), s.dp_s.at[k, b], s.dp_r.at[k, b], dp=1 - dp).start()

    def job_dp_wait_send(job, k, b):
        remote(job.dp_slot(b), job.dp_recv(b), s.dp_s.at[k, b], s.dp_r.at[k, b], dp=1 - dp).wait_send()

    def job_dp_wait_all(job, k):
        for b in range(nl):
            remote(job.dp_slot(b), job.dp_recv(b), s.dp_s.at[k, b], s.dp_r.at[k, b], dp=1 - dp).wait_recv()

    def chain_copy(job, k, up, step, part):
        i = 0 if up else 1
        width = job.cols // 2
        cols = pl.ds(part * width, width)
        return remote(
            job.chain_slot(up, step).at[:, cols], job.chain(up, step).at[:, cols],
            s.ch_s.at[k, i, step, part], s.ch_r.at[k, i, step, part],
            ctx=(z + 1) if up else (z - 1),
        )

    def chain_step(job, k, step, ways=(True, False), parts=(0, 1)):
        width = job.cols // 2
        for part in parts:
            for up in ways:
                pos = zl if up else zzl

                @pl.when((pos <= step) & (pos < nl - 1))
                def _(up=up, pos=pos, part=part):
                    target = (zl + nl - 1 - step) if up else (zl - (nl - 1 - step))
                    slot = job.chain_slot(up, step)
                    if step:

                        @pl.when(pos >= 1)
                        def _():
                            chain_copy(job, k, up, step - 1, part).wait_recv()

                    def body(c, w):
                        cs = pl.ds(pl.multiple_of(part * width + c, 128), w)
                        total = job.part(dp * nl + target, cs.start, w)
                        total = total + job.dp_recv(target)[:, cs].astype(F32)
                        if step:
                            prev = job.chain(up, step - 1)[:, cs].astype(F32)
                            total = total + jnp.where(pos >= 1, prev, 0.0)
                        slot[:, cs] = total.astype(BF16)

                    tiles(width, 256 if width % 256 == 0 else 128, body)
                    chain_copy(job, k, up, step, part).start()

    def chain_wait_send(job, k, step):
        for up in (True, False):
            pos = zl if up else zzl

            @pl.when((pos <= step) & (pos < nl - 1))
            def _(up=up):
                for part in range(2):
                    chain_copy(job, k, up, step, part).wait_send()

    def chain_final(job, k, out_ref):
        width = job.cols // 2
        for part in range(2):
            for up in (True, False):
                pos = zl if up else zzl

                @pl.when(pos >= 1)
                def _(up=up, part=part):
                    chain_copy(job, k, up, nl - 2, part).wait_recv()

            def body(c, w):
                cs = pl.ds(pl.multiple_of(part * width + c, 128), w)
                total = job.part(dp * nl + zl, cs.start, w) + job.dp_recv(zl)[:, cs].astype(F32)
                a = job.chain(True, nl - 2)[:, cs].astype(F32)
                b = job.chain(False, nl - 2)[:, cs].astype(F32)
                out_ref[:, cs] = total + jnp.where(zl >= 1, a, 0.0) + jnp.where(zzl >= 1, b, 0.0)

            tiles(width, 256 if width % 256 == 0 else 128, body)

    L = seg_row.shape[1]
    s.segs[:, : reach * T] = jnp.full((1, reach * T), -1, jnp.int32)
    s.segs[:, reach * T :] = seg_row[...]
    row = seg_row[...]
    at_me = lax.broadcasted_iota(jnp.int32, (T, L), 1) == lax.broadcasted_iota(jnp.int32, (T, L), 0) + z * T
    row_f = jnp.broadcast_to(row.astype(F32), (T, L))
    qseg_f = jnp.sum(jnp.where(at_me, row_f, 0.0), axis=1, keepdims=True)
    begins = jnp.sum(jnp.where(row_f < qseg_f, 1.0, 0.0), axis=1, keepdims=True)
    position = (lax.broadcasted_iota(jnp.int32, (T, H), 0) + z * T).astype(F32) - begins
    angles = position * inverse[...]
    cos[...] = jnp.cos(angles)
    lane = lax.broadcasted_iota(jnp.int32, (T, H), 1)
    turned = jnp.sin(angles)
    sin[...] = jnp.where(lane < H // 2, -turned, turned)

    rows_i = lax.broadcasted_iota(jnp.int32, (T, span), 0) + reach * T
    cols_i = lax.broadcasted_iota(jnp.int32, (T, span), 1)
    kseg_f = s.segs[:, pl.ds(pl.multiple_of(z * T, T), span)].astype(F32)
    allowed = (cols_i <= rows_i) & (qseg_f == kseg_f)
    s.mask[...] = jnp.where(allowed, 1.0, 0.0).astype(F32)

    l_tok.wait()
    x = s.tok[...].astype(F32)
    scale = lax.rsqrt(jnp.mean(x * x, axis=-1, keepdims=True) + epsilon)
    s.x1[...] = (x * scale * g1[...]).astype(BF16)
    s.tokshare[...] = s.tok[mine, :].astype(F32)

    def rms(v):
        return lax.rsqrt(jnp.mean(v * v, axis=-1, keepdims=True) + epsilon)

    def rope(v):
        return v * cos[...] + pltpu.roll(v, H // 2, 1) * sin[...]

    def rope_back(g):
        return g * cos[...] + pltpu.roll(g * sin[...], H // 2, 1)

    own_rows = pl.ds(reach * T, T)
    l_kw.wait()
    l_vw.wait()
    def kv_copy(r, c):
        lanes = pl.ds(c * 2 * H, 2 * H)
        return remote(
            s.kv.at[pl.ds((reach - r + 1) * T, T), lanes], s.kv.at[pl.ds((reach - r) * T, T), lanes],
            s.kv_s.at[r - 1, c], s.kv_r.at[r - 1, c], ctx=z + 1,
        )

    def kv_send(r, c):
        @pl.when((z < n - 1) & (z >= r - 1))
        def _():
            kv_copy(r, c).start()

    for h in range(KH):
        hs = pl.ds(h * H, H)
        raw = dot(s.x1[...], s.kw[:, hs])
        s.k_raw[:, hs] = raw
        s.kv[own_rows, 2 * h * H : (2 * h + 1) * H] = rope(raw * rms(raw) * gk[...]).astype(BF16)
        s.kv[own_rows, (2 * h + 1) * H : (2 * h + 2) * H] = dot(s.x1[...], s.vw[:, hs]).astype(BF16)
        if h == 0:
            pl.semaphore_wait(barrier, (nt - 1) + (2 * n - 1))
        kv_send(1, h)
    l_cot.wait()
    pl.when(zh == 1)(lambda: mirror(0, s.cot, s.cot2).start())
    for r in range(1, reach + 1):

        @pl.when(z < r)
        def _():
            s.kv[pl.ds((reach - r) * T, T), :] = jnp.zeros((T, 2 * KV), BF16)

    l_qw.wait()
    s.q_raw[...] = dot(s.x1[...], s.qw[...])
    for h in range(QH):
        raw = s.q_raw[:, h * H : (h + 1) * H]
        s.q_rot[:, h * H : (h + 1) * H] = rope(raw * rms(raw) * gq[...]).astype(BF16)
    for r in range(1, reach + 1):
        for c in range(KH):

            @pl.when(z >= r)
            def _(r=r, c=c):
                kv_copy(r, c).wait_recv()

            if r < reach:
                kv_send(r + 1, c)
    def weights_of(h, g):
        hs = pl.ds(pl.multiple_of(h * H, H), H)
        q = s.q_rot[:, hs]
        k = s.kv[:, pl.ds(pl.multiple_of(2 * g * H, H), H)]
        return q, k, jnp.where(s.mask[...] > 0.0, jnp.exp(dot_nt(q, k) * inv_root), 0.0)

    def attend(h, _):
        g = h // group
        hs = pl.ds(pl.multiple_of(h * H, H), H)
        _q, _k, w = weights_of(h, g)
        v = s.kv[:, pl.ds(pl.multiple_of((2 * g + 1) * H, H), H)]
        total = jnp.sum(w, axis=-1, keepdims=True)
        att = dot(w.astype(BF16), v) / total
        s.tot[:, hs] = jnp.broadcast_to(total, (T, H))
        s.att[:, hs] = att
        s.att_low[:, hs] = att.astype(BF16)
        s.attt[hs, :] = att.T.astype(BF16)
        return 0

    lax.fori_loop(0, QH, attend, 0)

    l_ow.wait()

    def body(c, w):
        s.send_a[:, pl.ds(c, w)] = dot(s.att_low[...], s.ow[:, pl.ds(c, w)]).astype(BF16)

    tiles(D, TILE, body)
    scatter_start(0, s.send_a, s.recv0)
    gather_line_start(2, s.attt, att_all, (False,), True)

    def transpose_half(src, dst, place):
        for d in range(2):

            def body(c, w):
                cs = pl.ds(pl.multiple_of((d * n + zh * nl) * R + c, 128), w)
                rows = pl.ds(pl.multiple_of(d * nl * R + c, 128), w)
                dst[rows, place * T : (place + 1) * T] = src[:, cs].astype(F32).T.astype(BF16)

            tiles(nl * R, TILE, body)

    s.cotshare[...] = s.cot[mine, :].astype(F32)

    transpose_half(s.x1, s.x1t, 0)
    transpose_half(s.cot, s.cott, 0)
    l_dw.wait()

    def hidden_grad(cot, out):
        def body(c, w):
            out[:, pl.ds(c, w)] = dot_nt(cot[...], s.dw[pl.ds(c, w), :])

        tiles(F, TILE, body)

    def cot_share():
        mirror(0, s.cot, s.cot2).wait_recv()
        gather_start(9, s.cot2)

    hidden_grad(s.cot, s.gh)
    pl.when(z == nl - 1)(lambda: mirror(0, s.cot, s.cot2).start())

    s.resid[...] = scatter_sum(0, s.send_a, s.recv0, s.tokshare[...])
    resid = s.resid[...]
    s.x2[mine, :] = (resid * rms(resid) * g2[...]).astype(BF16)
    gather_start(1, s.x2)
    mirror(1, s.x2, s.x2b).start()
    gather_line_step(2, att_all, 1, (False,))
    l_gw.wait()
    l_uw.wait()
    gather_forward(1, s.x2)
    pl.when(z < nl - 1)(lambda: mirror(0, s.cot, s.cot2).start())
    gather_wait(1, s.x2)

    def mirrored_share():
        mirror(1, s.x2, s.x2b).wait_recv()
        gather_start(10, s.x2b)

    cot_share()

    def feed(x, grad_hidden, place):
        rows = pl.ds(place * T, T)

        def body(c, w):
            cs = pl.ds(c, w)
            gate = dot(x[...], s.gw[:, cs])
            up = dot(x[...], s.uw[:, cs])
            gh = grad_hidden[:, cs]
            sig = jax.nn.sigmoid(gate)
            act = gate * sig
            s.hid[rows, cs] = (act * up).astype(BF16)
            s.gg[rows, cs] = (gh * up * (sig * (1.0 + gate * (1.0 - sig)))).astype(BF16)
            s.gu[rows, cs] = (gh * act).astype(BF16)

        tiles(F, TILE, body)

    feed(s.x2, s.gh, 0)
    mirrored_share()
    gather_forward(9, s.cot2)
    gather_line_start(2, s.attt, att_all, (True,), False)
    gather_line_step(2, att_all, 2, (False,))
    own_part = pl.ds(0, T)

    def body(c, w):
        rs = pl.ds(c, w)
        s.send_a[:, rs] = (
            dot_nt(s.gg[own_part, :], s.gw[rs, :]) + dot_nt(s.gu[own_part, :], s.uw[rs, :])
        ).astype(BF16)

    tiles(D, TILE, body)
    transpose_half(s.x2, s.xt, 0)
    gather_forward(10, s.x2b)
    mirror(1, s.x2, s.x2b).wait_send()
    scatter_start(2, s.send_a, s.recv1)
    for d in range(2):
        mirror_x1(d).start()

    def body(c, w):
        s.send_b[:, pl.ds(c, w)] = dot(s.hid[own_part, :], s.dw[:, pl.ds(c, w)]).astype(BF16)

    tiles(D, TILE, body)
    gather_wait(9, s.cot2)
    hidden_grad(s.cot2, s.gh2)
    transpose_half(s.cot2, s.cott, 1)
    gather_wait(10, s.x2b)
    feed(s.x2b, s.gh2, 1)
    transpose_half(s.x2b, s.xt, 1)
    pl.semaphore_signal(s.credit, inc=1, device_id={"dp": 1 - dp}, device_id_type=MESH)

    grad_second = scatter_sum(2, s.send_a, s.recv1, jnp.zeros((S, D), F32))
    resid = s.resid[...]
    scale = rms(resid)
    normed = resid * scale
    s.gains[:, D : 2 * D] = jnp.sum(grad_second * normed, axis=0, keepdims=True)
    scaled = grad_second * g2[...]
    inner = jnp.mean(scaled * normed, axis=-1, keepdims=True)
    s.gresid[...] = s.cotshare[...] + scale * (scaled - normed * inner)
    s.gm[mine, :] = s.gresid[...].astype(BF16)
    gather_start(4, s.gm)
    columns_start(2, s.gm, s.gmc)

    class WeightJob:
        def __init__(self, k, left, grad):
            self.k, self.left, self.grad, self.cols = k, left, grad, grad.shape[1]

        def part(self, block, c, w):
            rows = pl.ds(pl.multiple_of(block * R, R), R)
            return dot(self.left[rows, :], self.grad[:, pl.ds(c, w)])

        def dp_slot(self, b):
            return s.gw.at[pl.ds(b * R, R), pl.ds(0, self.cols)]

        def dp_recv(self, b):
            return s.uw.at[pl.ds(pl.multiple_of((self.k * nl + b) * R, R), R), pl.ds(0, self.cols)]

        def chain_slot(self, up, step):
            i = nl + self.k * (nl - 1) + (step if up else nl - 2 - step)
            return s.gw.at[pl.ds(i * R, R), pl.ds(0, self.cols)]

        def chain(self, up, step):
            return s.chain.at[self.k, 0 if up or nl == 2 else 1, step, :, pl.ds(0, self.cols)]

    jobs = [
        WeightJob(0, s.cott, s.hid),
        WeightJob(1, s.xt, s.gg),
        WeightJob(2, s.xt, s.gu),
        WeightJob(3, s.x1t, s.dqkv),
    ]
    order = [b for i in range((nl + 1) // 2) for b in dict.fromkeys((nl - 1 - i, i))]

    def job_dp(k):
        for b in order:
            if k:
                job_dp_wait_send(jobs[k - 1], k - 1, b)
            job_dp_start(jobs[k], k, b)

    pl.semaphore_wait(s.credit, 1)
    job_dp(0)
    job_dp_wait_all(jobs[0], 0)
    chain_step(jobs[0], 0, 0)
    gather_forward(4, s.gm)
    gather_line_step(2, att_all, 1, (True,))
    job_dp(1)
    gather_wait(4, s.gm)
    scatter_start(3, s.send_b, s.recv2)
    for d in range(2):
        mirror_x1(d).wait_recv()

    def body(c, w):
        s.x1t[pl.ds(c, w), T : 2 * T] = s.x1b[:, pl.ds(c, w)].astype(F32).T.astype(BF16)

    tiles(D // 2, TILE, body)

    gatt = s.gh.at[:, pl.ds(0, QH * H)]

    def body(c, w):
        gatt[:, pl.ds(c, w)] = dot_nt(s.gm[...], s.ow[pl.ds(c, w), :])

    tiles(QH * H, TILE, body)
    s.gq_acc[...] = jnp.zeros((1, H), F32)

    def back(g, _):
        ks = pl.ds(pl.multiple_of(g * H, H), H)
        vs = pl.ds(pl.multiple_of(KV + g * H, H), H)
        v = s.kv[:, pl.ds(pl.multiple_of((2 * g + 1) * H, H), H)]
        grad_k = jnp.zeros((span, H), F32)
        grad_v = jnp.zeros((span, H), F32)
        for i in range(group):
            h = g * group + i
            hs = pl.ds(pl.multiple_of(h * H, H), H)
            q, k, w = weights_of(h, g)
            ga, total = gatt[:, hs], s.tot[:, hs]
            gs = (ga / total).astype(BF16)
            delta = jnp.sum(ga * s.att[:, hs], axis=-1, keepdims=True) / total[:, :1]
            ds = (w * (dot_nt(gs, v) - delta)).astype(BF16)
            grad_k = grad_k + dot_tn(ds, q) * inv_root
            grad_v = grad_v + dot_tn(w.astype(BF16), gs)
            gr = rope_back(dot(ds, k) * inv_root)
            raw = s.q_raw[:, hs]
            r = rms(raw)
            nq = raw * r
            s.gq_acc[...] += jnp.sum(gr * nq, axis=0, keepdims=True)
            sc = gr * gq[...]
            s.dqkv[:T, hs] = (r * (sc - nq * jnp.mean(sc * nq, axis=-1, keepdims=True))).astype(BF16)
        s.dkv[:, ks] = grad_k.astype(BF16)
        s.dkv[:, vs] = grad_v.astype(BF16)
        return 0

    lax.fori_loop(0, KH, back, 0)
    s.gains[:, 2 * D : 2 * D + H] = s.gq_acc[...]

    def dkv_copy(i):
        return remote(
            s.dkv.at[pl.ds(i * T, T)], s.dkv_in.at[i], s.dkv_s.at[i], s.dkv_r.at[i], ctx=z - 1
        )

    for i in range(reach):
        if i:

            @pl.when((z < n - 1) & (z + 1 >= reach - i + 1))
            def _():
                dkv_copy(i - 1).wait_recv()
                rows = pl.ds(i * T, T)
                s.dkv[rows, :] = (s.dkv[rows, :].astype(F32) + s.dkv_in[i - 1].astype(F32)).astype(BF16)

        @pl.when(z >= reach - i)
        def _():
            dkv_copy(i).start()

        if i == 0:
            job_dp_wait_all(jobs[1], 1)
            chain_step(jobs[1], 1, 0, (True,))
            pl.when(zh == 0)(lambda: chain_step(jobs[1], 1, 0, (False,), (0,)))
            job_dp(2)

    pl.when(zh == 0)(lambda: chain_step(jobs[1], 1, 0, (False,), (1,)))

    @pl.when(z < n - 1)
    def _():
        dkv_copy(reach - 1).wait_recv()

    own = s.dkv[pl.ds(reach * T, T), :].astype(F32)
    own = own + jnp.where(z < n - 1, s.dkv_in[reach - 1].astype(F32), 0.0)
    s.dqkv[:T, QH * H + KV :] = own[:, KV:].astype(BF16)
    gk_sum = jnp.zeros((1, H), F32)
    for h in range(KH):
        gr = rope_back(own[:, h * H : (h + 1) * H])
        raw = s.k_raw[:, h * H : (h + 1) * H]
        r = rms(raw)
        nk = raw * r
        gk_sum = gk_sum + jnp.sum(gr * nk, axis=0, keepdims=True)
        sc = gr * gk[...]
        s.dqkv[:T, QH * H + h * H : QH * H + (h + 1) * H] = (
            r * (sc - nk * jnp.mean(sc * nk, axis=-1, keepdims=True))
        ).astype(BF16)
    s.gains[:, 2 * D + H :] = gk_sum
    pl.when(zh == 1)(lambda: chain_step(jobs[1], 1, 0, (False,)))
    mirror_qkv().start()
    gather_line_step(2, att_all, 2, (True,))
    job_dp_wait_all(jobs[2], 2)
    chain_step(jobs[2], 2, 0)

    s.outsh[...] = scatter_sum(3, s.send_b, s.recv2, s.resid[...]).astype(BF16)
    q_c, k_c, v_c = pl.ds(0, QH * H), pl.ds(QH * H, KV), pl.ds(QH * H + KV, KV)

    def body(c, w):
        rs = pl.ds(c, w)
        s.send_a[:, rs] = (
            dot_nt(s.dqkv[:T, q_c], s.qw[rs, :])
            + dot_nt(s.dqkv[:T, k_c], s.kw[rs, :])
            + dot_nt(s.dqkv[:T, v_c], s.vw[rs, :])
        ).astype(BF16)

    tiles(D, TILE, body)
    scatter_start(6, s.send_a, s.recv3)
    grad_first = scatter_sum(6, s.send_a, s.recv3, jnp.zeros((S, D), F32))
    tokshare = s.tokshare[...]
    scale = rms(tokshare)
    normed = tokshare * scale
    s.gains[:, :D] = jnp.sum(grad_first * normed, axis=0, keepdims=True)
    scaled = grad_first * g1[...]
    inner = jnp.mean(scaled * normed, axis=-1, keepdims=True)
    s.tgsh[...] = (s.gresid[...] + scale * (scaled - normed * inner)).astype(BF16)
    for j in range(1, nt):
        remote(s.gains, s.gains_p.at[j - 1], s.pl_s.at[8, j - 1], s.pl_r.at[8, j - 1], tensor=t ^ j).start()
    spread_start(7, s.tgsh, tgrad_hbm, 1)
    for j in range(1, nt):
        remote(s.gains, s.gains_p.at[j - 1], s.pl_s.at[8, j - 1], s.pl_r.at[8, j - 1], tensor=t ^ j).wait()
    total = s.gains[...]
    for j in range(1, nt):
        total = total + s.gains_p[j - 1]
    s.gains2[...] = total

    def gain_copy(e, d):
        i = e * n + d
        return remote(
            s.gains2, s.gains_x.at[i - 1], s.ga_s.at[i], s.ga_r.at[i], dp=dp ^ e, ctx=lax.rem(z + d, n)
        )

    for e in range(2):
        for d in range(n):
            if e or d:
                gain_copy(e, d).start()
    columns_wait_recv(2, s.gm, s.gmc)
    share_start(2, s.gmc)
    spread_start(5, s.outsh, out_hbm, 0)
    stage = s.gh2.at[pl.ds(0, R), pl.ds(0, QH * H + 2 * KV)]

    def gate_copy():
        return pltpu.make_async_copy(s.gh.at[pl.ds(0, R)], gate_out, s.load_sem.at[2])

    def up_copy():
        return pltpu.make_async_copy(s.gh.at[pl.ds(0, R)], up_out, s.load_sem.at[3])

    def qkv_copies():
        parts = [(q_out, 0, QH * H), (k_out, QH * H, KV), (v_out, QH * H + KV, KV)]
        return [
            pltpu.make_async_copy(stage.at[:, pl.ds(a, w)], ref, s.load_sem.at[6 + i])
            for i, (ref, a, w) in enumerate(parts)
        ]

    for step in range(1, nl - 1):
        for k in range(3):
            chain_step(jobs[k], k, step)
    rows = pl.ds(0, R)
    chain_final(jobs[0], 0, s.gh.at[rows])
    width = min(256, F)
    flip = s.gh2.at[:, pl.ds(QH * H + 2 * KV, 2 * R)]

    def down_copy(i):
        return pltpu.make_async_copy(
            flip.at[pl.ds(0, width), pl.ds((i % 2) * R, R)],
            down_out.at[pl.ds(i * width, width)],
            s.load_sem.at[4 + i % 2],
        )

    count = F // width
    for i in range(count):
        if i >= 2:
            down_copy(i - 2).wait()
        flip[:width, (i % 2) * R : (i % 2 + 1) * R] = s.gh[rows, i * width : (i + 1) * width].T
        down_copy(i).start()
    for i in range(max(0, count - 2), count):
        down_copy(i).wait()
    mirror_qkv().wait_recv()
    job_dp(3)
    job_dp_wait_all(jobs[3], 3)
    chain_step(jobs[3], 3, 0)
    for step in range(1, nl - 1):
        chain_step(jobs[3], 3, step)


    chain_final(jobs[1], 1, s.gh.at[rows])
    gate_copy().start()
    for step in range(3, n):
        gather_line_step(2, att_all, step)
    gather_line_finish(2, s.attt, att_all)
    share_wait(2, s.gmc)

    def load(i):
        slot = lax.rem(i, 2)
        return pltpu.make_async_copy(
            att_all.at[i // n, lax.rem(i, n)],
            s.dw.at[pl.ds(pl.multiple_of(slot * QH * H, QH * H), QH * H), pl.ds(0, T)],
            s.stage_sem.at[slot],
        )

    load(0).start()
    s.outw[...] = jnp.zeros(s.outw.shape, F32)

    def step(i, _):
        @pl.when(i + 1 < 2 * n)
        def _():
            load(i + 1).start()

        load(i).wait()
        slot = lax.rem(i, 2)
        left = s.dw[pl.ds(pl.multiple_of(slot * QH * H, QH * H), QH * H), pl.ds(0, T)]
        s.outw[...] += dot(left, s.gmc[:, i].reshape(T, R))
        return 0

    lax.fori_loop(0, 2 * n, step, 0)

    def outw_copy():
        return pltpu.make_async_copy(s.outw, outw_out, s.load_sem.at[4])

    outw_copy().start()
    gate_copy().wait()
    chain_final(jobs[2], 2, s.gh.at[rows])
    up_copy().start()
    chain_final(jobs[3], 3, stage)
    for copy in qkv_copies():
        copy.start()
    for e in range(2):
        for d in range(n):
            if e or d:
                gain_copy(e, d).wait()
    total = s.gains2[...]
    for i in range(2 * n - 1):
        total = total + s.gains_x[i]
    s.gains[...] = total

    def gains_copy():
        return pltpu.make_async_copy(s.gains, gains_out, s.load_sem.at[2])

    gains_copy().start()

    columns_wait_send(2, s.gm, s.gmc)
    mirror(0, s.cot, s.cot2).wait_send()
    mirror_qkv().wait_send()
    for d in range(2):
        mirror_x1(d).wait_send()
    for b in order:
        job_dp_wait_send(jobs[-1], len(jobs) - 1, b)
    for st in range(nl - 1):
        for k, job in enumerate(jobs):
            chain_wait_send(job, k, st)
    for r in range(1, reach + 1):

        @pl.when((z < n - 1) & (z >= r - 1))
        def _(r=r):
            for c in range(KH):
                kv_copy(r, c).wait_send()

    for i in range(reach):

        @pl.when(z >= reach - i)
        def _():
            dkv_copy(i).wait_send()

    spread_wait(5, s.outsh, out_hbm, 0)
    spread_wait(7, s.tgsh, tgrad_hbm, 1)
    gains_copy().wait()
    up_copy().wait()
    outw_copy().wait()
    for copy in qkv_copies():
        copy.wait()


def run_layer(dm, *operands):
    T, D, H, F, n, nt, reach, S, R = dm.T, dm.D, dm.H, dm.F, dm.n, dm.nt, dm.reach, dm.S, dm.R
    QC, KV = dm.QH * H, dm.KH * H
    span = (reach + 1) * T
    G = 2 * D + 2 * H
    dma = pltpu.SemaphoreType.DMA
    scratch = dict(
        tok=((T, D), BF16), x1=((T, D), BF16), send_b=((T, D), BF16), cot=((T, D), BF16), x2=((T, D), BF16),
        outsh=((S, D), BF16), tgsh=((S, D), BF16), xt=((D // 2, 2 * T), BF16), cott=((D // 2, 2 * T), BF16),
        cot2=((T, D), BF16), x2b=((T, D), BF16),
        qw=((D, QC), BF16), kw=((D, KV), BF16), vw=((D, KV), BF16), ow=((QC, D), BF16),
        gw=((D, F), BF16), uw=((D, F), BF16), dw=((F, D), BF16),
        tokshare=((S, D), F32), cotshare=((S, D), F32), resid=((S, D), F32), gresid=((S, D), F32),
        k_raw=((T, KV), F32), q_raw=((T, QC), F32), q_rot=((T, QC), BF16), kv=((span, 2 * KV), BF16),
        mask=((T, span), F32), tot=((T, QC), F32), att=((T, QC), F32), att_low=((T, QC), BF16),
        attt=((QC, T), BF16), gq_acc=((1, H), F32),
        recv0=((6, S, D // 2) if nt == 4 else (nt - 1, S, D), BF16),
        recv1=((6, S, D // 2) if nt == 4 else (nt - 1, S, D), BF16), pair=((2, S, D // 2), BF16),
        gh=((T, F), F32), hid=((2 * T, F), BF16), gg=((2 * T, F), BF16), gu=((2 * T, F), BF16),
        dkv=((span, 2 * KV), BF16), dkv_in=((reach, T, 2 * KV), BF16), dqkv=((2 * T, QC + 2 * KV), BF16),
        chain=((4, 1 if n == 4 else 2, n // 2 - 1, R, F), BF16),

        gmc=((nt, 2 * n, S, R), BF16), x1b=((T, D // 2), BF16), x1t=((D // 2, 2 * T), BF16), gh2=((T, F), F32),
        cos=((T, H), F32), sin=((T, H), F32), segs=((1, reach * T + dm.L), jnp.int32),
        outw=((QC, R), F32), gain_in=((1, G), F32), gains=((1, G), F32), gains2=((1, G), F32), gains_p=((nt - 1, 1, G), F32),
        gains_x=((2 * n - 1, 1, G), F32),
    )
    sems = dict(
        load_sem=(9,), own_sem=(3,), pl_s=(13, nt - 1), pl_r=(13, nt - 1), ag_s=(3, 2, n - 1), ag_r=(3, 2, n - 1),
        agx_s=(3, 2 * n - 1), agx_r=(3, 2 * n - 1), aa_s=(3, 2 * n), aa_r=(3, 2 * n), stage_sem=(2,),
        dp_s=(4, n // 2), dp_r=(4, n // 2), ch_s=(4, 2, n // 2 - 1, 2), ch_r=(4, 2, n // 2 - 1, 2), mi_s=(5,), mi_r=(5,), kv_s=(reach, KV // H), kv_r=(reach, KV // H), pl2_s=(11,), pl2_r=(11,), rs_s=(7, 6), rs_r=(7, 6),
        dkv_s=(reach,), dkv_r=(reach,), ga_s=(2 * n,), ga_r=(2 * n,),
    )
    names = list(scratch) + list(sems) + ["credit"]
    shapes = [pltpu.VMEM(*v) for v in scratch.values()] + [dma(v) for v in sems.values()]
    shapes.append(pltpu.SemaphoreType.REGULAR)

    def body(*refs):
        fixed = len(refs) - len(names)
        s = Dims()
        for name, ref in zip(names, refs[fixed:]):
            setattr(s, name, ref)
        for alias, of in dm.alias.items():
            setattr(s, alias, getattr(s, of))
        layer_kernel(dm, *refs[:fixed], s)

    hbm = pl.BlockSpec(memory_space=pl.ANY)
    vmem = pl.BlockSpec(memory_space=pltpu.VMEM)
    return pl.pallas_call(
        body,
        out_shape=(
            jax.ShapeDtypeStruct((T, D), BF16),
            jax.ShapeDtypeStruct((T, D), BF16),
            jax.ShapeDtypeStruct((R, F), F32),
            jax.ShapeDtypeStruct((R, F), F32),
            jax.ShapeDtypeStruct((F, R), F32),
            jax.ShapeDtypeStruct((R, QC), F32),
            jax.ShapeDtypeStruct((R, KV), F32),
            jax.ShapeDtypeStruct((R, KV), F32),
            jax.ShapeDtypeStruct((QC, R), F32),
            jax.ShapeDtypeStruct((1, G), F32),
            jax.ShapeDtypeStruct((2, n, QC, T), BF16),
        ),
        in_specs=[hbm] * 2 + [vmem] * 6 + [hbm] * 7,
        out_specs=[hbm] * 11,
        scratch_shapes=shapes,
        compiler_params=pltpu.CompilerParams(
            collective_id=0, has_side_effects=True, vmem_limit_bytes=67043328
        ),
        name="layer",
    )(*operands)


FINISH_WINDOW = 64


def finish_pieces(shape):
    rows = shape[0]
    step = rows // 2 if rows % 32 == 0 else rows
    return [(r, step) for r in range(0, rows, step)]


def finish_kernel(dm, *refs):
    count = len(dm.finish)
    ins, gains, outs = refs[:count], refs[count], refs[count + 1 : 2 * count + 1]
    gain_outs = refs[2 * count + 1 : 2 * count + 5]
    bufs, load_sem, store_sem = refs[2 * count + 5 : 3 * count + 5], refs[-2], refs[-1]
    loads, stores = [], []
    for a, b, c in zip(ins, bufs, outs):
        for start, size in finish_pieces(a.shape):
            rows, i = pl.ds(start, size), len(loads)
            loads.append(pltpu.make_async_copy(a.at[rows], b.at[rows], load_sem.at[i]))
            stores.append(pltpu.make_async_copy(b.at[rows], c.at[rows], store_sem.at[i]))
    for load in loads[:FINISH_WINDOW]:
        load.start()
    place = 0
    for ref in gain_outs:
        ref[...] = gains[:, place : place + ref.shape[1]]
        place += ref.shape[1]
    for i, (load, store) in enumerate(zip(loads, stores)):
        load.wait()
        store.start()
        if i + FINISH_WINDOW < len(loads):
            loads[i + FINISH_WINDOW].start()
    for store in stores:
        store.wait()


def finish(dm, arrays, gains):
    dm.finish = arrays
    hbm = pl.BlockSpec(memory_space=pl.ANY)
    vmem = pl.BlockSpec(memory_space=pltpu.VMEM)
    shapes = [jax.ShapeDtypeStruct(a.shape, a.dtype) for a in arrays]
    gain_shapes = [jax.ShapeDtypeStruct((1, w), F32) for w in (dm.D, dm.D, dm.H, dm.H)]
    dma = pltpu.SemaphoreType.DMA((sum(len(finish_pieces(a.shape)) for a in arrays),))
    return pl.pallas_call(
        functools.partial(finish_kernel, dm),
        out_shape=tuple(shapes + gain_shapes),
        in_specs=[hbm] * len(arrays) + [vmem],
        out_specs=tuple([hbm] * len(arrays) + [vmem] * 4),
        scratch_shapes=[pltpu.VMEM(a.shape, a.dtype) for a in arrays] + [dma, dma],
        compiler_params=pltpu.CompilerParams(vmem_limit_bytes=67043328),
        name="finish",
    )(*arrays, gains)


def per_device(
    tokens,
    segments,
    first_gain,
    query_weight,
    key_matrix,
    value_matrix,
    query_norm_gain,
    key_gain,
    output_weight,
    second_gain,
    gate_weight,
    up_weight,
    down_weight,
    cotangent,
):
    _, T, D = tokens.shape
    dm = Dims()
    dm.T, dm.D, dm.H, dm.F = T, D, query_norm_gain.shape[0], gate_weight.shape[1]
    dm.QH, dm.KH = query_weight.shape[1] // dm.H, key_matrix.shape[1] // dm.H
    dm.n, dm.nt = lax.axis_size("ctx"), lax.axis_size("tensor")
    length = segments.shape[1]
    dm.reach = -(-(length // 2 - 1) // T)
    dm.S, dm.R = T // dm.nt, D // (2 * dm.n)
    dm.alias = {"send_a": "tok", "gm": "x2", "recv2": "recv0", "recv3": "recv1"}
    H = dm.H
    dm.L = length
    inverse = (1.0 / rope_base ** (np.arange(0, H, 2, dtype=np.float32) / np.float32(H))).astype(np.float32)
    inverse = np.concatenate([inverse, inverse])[None]
    out, tgrad, gate_g, up_g, down_g, q_g, k_g, v_g, out_g, gains = run_layer(
        dm,
        tokens.reshape(T, D),
        cotangent.reshape(T, D),
        first_gain.reshape(-1, H),
        second_gain.reshape(-1, H),
        query_norm_gain.reshape(1, H),
        key_gain.reshape(1, H),
        inverse,
        segments,
        query_weight,
        key_matrix,
        value_matrix,
        output_weight,
        gate_weight,
        up_weight,
        down_weight,
    )[:10]
    out, tgrad, gate_g, up_g, down_g, q_g, k_g, v_g, out_g, first_g, second_g, qn_g, kn_g = finish(
        dm, (out, tgrad, gate_g, up_g, down_g, q_g, k_g, v_g, out_g), gains
    )
    return (
        out.reshape(tokens.shape),
        tgrad.reshape(tokens.shape),
        first_g.reshape(D),
        q_g,
        k_g,
        v_g,
        qn_g.reshape(H),
        kn_g.reshape(H),
        out_g,
        second_g.reshape(D),
        gate_g,
        up_g,
        down_g,
    )


def solution(mesh):
    return jax.shard_map(
        per_device,
        mesh=mesh,
        in_specs=(
            P("dp", "ctx", None),
            P("dp", None),
            P(),
            P(None, "tensor"),
            P(None, "tensor"),
            P(None, "tensor"),
            P(),
            P(),
            P("tensor", None),
            P(),
            P(None, "tensor"),
            P(None, "tensor"),
            P("tensor", None),
            P("dp", "ctx", None),
        ),
        out_specs=(
            P("dp", "ctx", None),
            P("dp", "ctx", None),
            P(),
            P(("dp", "ctx"), "tensor"),
            P(("dp", "ctx"), "tensor"),
            P(("dp", "ctx"), "tensor"),
            P(),
            P(),
            P("tensor", ("dp", "ctx")),
            P(),
            P(("dp", "ctx"), "tensor"),
            P(("dp", "ctx"), "tensor"),
            P("tensor", ("dp", "ctx")),
        ),
        check_vma=False,
    )
```

```python
import functools
import math

import jax
import jax.numpy as jnp
import numpy as np
from jax import lax
from jax.experimental import pallas as pl
from jax.experimental.pallas import tpu as pltpu
from jax.sharding import PartitionSpec as P

epsilon = 1e-06
rope_base = 1000000.0
F32 = jnp.float32
BF16 = jnp.bfloat16
MESH = pl.DeviceIdType.MESH
TILE = 256


def dot(a, b):
    return jnp.dot(a, b, preferred_element_type=F32)


def dot_nt(a, b):
    return lax.dot_general(a, b, (((1,), (1,)), ((), ())), preferred_element_type=F32)


def dot_tn(a, b):
    return lax.dot_general(a, b, (((0,), (0,)), ((), ())), preferred_element_type=F32)


def remote(src, dst, send_sem, recv_sem, **device):
    return pltpu.make_async_remote_copy(
        src_ref=src,
        dst_ref=dst,
        send_sem=send_sem,
        recv_sem=recv_sem,
        device_id=device,
        device_id_type=MESH,
    )


def tiles(total, size, body):
    size = min(size, total)

    def step(i, _):
        body(pl.multiple_of(i * size, size), size)
        return 0

    lax.fori_loop(0, total // size, step, 0)


class Dims:
    pass


def layer_kernel(
    dm,
    tok_hbm,
    cot_hbm,
    first_in,
    second_in,
    query_in,
    key_in,
    inverse,
    seg_row,
    qw_hbm,
    kw_hbm,
    vw_hbm,
    ow_hbm,
    gw_hbm,
    uw_hbm,
    dw_hbm,
    out_hbm,
    tgrad_hbm,
    gate_out,
    up_out,
    down_out,
    q_out,
    k_out,
    v_out,
    outw_out,
    gains_out,
    att_all,
    s,
):
    T, D, H, QH, KH, F, n, nt, reach, S, R = (
        dm.T, dm.D, dm.H, dm.QH, dm.KH, dm.F, dm.n, dm.nt, dm.reach, dm.S, dm.R,
    )
    group = QH // KH
    span = (reach + 1) * T
    KV = KH * H
    inv_root = 1.0 / math.sqrt(H)
    C = R // nt
    gain_in = s.gain_in
    for place, ref in ((0, first_in), (D, second_in), (2 * D, query_in), (2 * D + H, key_in)):
        for i in range(ref.shape[0]):
            gain_in[:, place + i * H : place + (i + 1) * H] = ref[i : i + 1, :].astype(F32)
    g1 = gain_in.at[:, pl.ds(0, D)]
    g2 = gain_in.at[:, pl.ds(D, D)]
    gq = gain_in.at[:, pl.ds(2 * D, H)]
    gk = gain_in.at[:, pl.ds(2 * D + H, H)]
    cos, sin = s.cos, s.sin
    dp, z, t = lax.axis_index("dp"), lax.axis_index("ctx"), lax.axis_index("tensor")
    zz = n - 1 - z
    nl = n // 2
    zh, zl = z // nl, lax.rem(z, nl)
    zzl = nl - 1 - zl

    barrier = pltpu.get_barrier_semaphore()
    for j in range(1, nt):
        pl.semaphore_signal(barrier, inc=1, device_id={"tensor": t ^ j}, device_id_type=MESH)
    for e in range(2):
        for d in range(n):
            if e or d:
                pl.semaphore_signal(
                    barrier,
                    inc=1,
                    device_id={"dp": dp ^ e, "ctx": lax.rem(z + d, n)},
                    device_id_type=MESH,
                )

    loads = [
        (tok_hbm, s.tok), (cot_hbm, s.cot), (kw_hbm, s.kw), (vw_hbm, s.vw), (qw_hbm, s.qw),
        (ow_hbm, s.ow), (dw_hbm, s.dw), (gw_hbm, s.gw), (uw_hbm, s.uw),
    ]
    loads = [pltpu.make_async_copy(a, b, s.load_sem.at[i]) for i, (a, b) in enumerate(loads)]
    for load in loads:
        load.start()
    (l_tok, l_cot, l_kw, l_vw, l_qw, l_ow, l_dw, l_gw, l_uw) = loads

    def scatter_direct(k, buf, recv, j):
        peer = t ^ j
        return remote(
            buf.at[pl.ds(pl.multiple_of(peer * S, S), S)], recv.at[j - 1],
            s.pl_s.at[k, j - 1], s.pl_r.at[k, j - 1], tensor=peer,
        )

    def scatter_first(k, buf, recv, slot):
        to = t ^ (1 if slot < 2 else 2)
        rows = pl.ds(pl.multiple_of((to if slot % 2 == 0 else t ^ 3) * S, S), S)
        cols = pl.ds(0 if slot < 2 else D // 2, D // 2)
        return remote(buf.at[rows, cols], recv.at[slot], s.rs_s.at[k, slot], s.rs_r.at[k, slot], tensor=to)

    def scatter_second(k, recv, slot):
        to = t ^ (2 if slot == 4 else 1)
        return remote(s.pair.at[slot - 4], recv.at[slot], s.rs_s.at[k, slot], s.rs_r.at[k, slot], tensor=to)

    def scatter_start(k, buf, recv):
        if nt == 4:
            for slot in (1, 3, 0, 2):
                scatter_first(k, buf, recv, slot).start()
        else:
            for j in range(1, nt):
                scatter_direct(k, buf, recv, j).start()

    def scatter_sum(k, buf, recv, base):
        own = pl.ds(pl.multiple_of(t * S, S), S)
        if nt == 4:
            for slot, peer, cols in ((1, t ^ 2, slice(0, D // 2)), (3, t ^ 1, slice(D // 2, D))):
                scatter_first(k, buf, recv, slot).wait_recv()
                rows = pl.ds(pl.multiple_of(peer * S, S), S)
                both = buf[rows, cols].astype(F32) + recv[slot].astype(F32)
                s.pair[slot // 2] = both.astype(BF16)
                scatter_second(k, recv, 4 + slot // 2).start()
            for slot in (0, 2):
                scatter_first(k, buf, recv, slot).wait_recv()
            for slot in range(4):
                scatter_first(k, buf, recv, slot).wait_send()
            for slot in (4, 5):
                scatter_second(k, recv, slot).wait()
            left = buf[own, 0 : D // 2].astype(F32) + recv[0].astype(F32) + recv[4].astype(F32)
            right = buf[own, D // 2 : D].astype(F32) + recv[2].astype(F32) + recv[5].astype(F32)
            return base + jnp.concatenate([left, right], axis=1)
        for j in range(1, nt):
            scatter_direct(k, buf, recv, j).wait()
        total = base + buf[own, :].astype(F32)
        for j in range(1, nt):
            total = total + recv[j - 1].astype(F32)
        return total

    def rows_of(peer, half=None):
        if half is None:
            return pl.ds(pl.multiple_of(peer * S, S), S)
        return pl.ds(pl.multiple_of(peer * S + half * (S // 2), S // 2), S // 2)

    def gather_copy(k, full, j):
        rows = rows_of(t)
        return remote(full.at[rows], full.at[rows], s.pl_s.at[k, j - 1], s.pl_r.at[k, j - 1], tensor=t ^ j)

    def gather_arrived(k, full, j):
        rows = rows_of(t ^ j)
        return remote(full.at[rows], full.at[rows], s.pl_s.at[k, j - 1], s.pl_r.at[k, j - 1], tensor=t ^ j)

    def relay_copy(k, full, origin, half, to):
        rows = rows_of(origin, half)
        sems = (s.pl2_s.at[k], s.pl2_r.at[k]) if half else (s.pl_s.at[k, 2], s.pl_r.at[k, 2])
        return remote(full.at[rows], full.at[rows], *sems, tensor=to)

    def gather_start(k, full):
        for j in range(1, nt) if nt != 4 else (1, 2):
            gather_copy(k, full, j).start()

    def gather_forward(k, full):
        if nt == 4:
            gather_arrived(k, full, 1).wait_recv()
            relay_copy(k, full, t ^ 1, 0, t ^ 2).start()
            gather_arrived(k, full, 2).wait_recv()
            relay_copy(k, full, t ^ 2, 1, t ^ 1).start()

    def gather_wait(k, full):
        for j in range(1, nt) if nt != 4 else (1, 2):
            gather_copy(k, full, j).wait_send()
            if nt != 4:
                gather_arrived(k, full, j).wait_recv()
        if nt == 4:
            relay_copy(k, full, t ^ 1, 0, t ^ 2).wait_send()
            relay_copy(k, full, t ^ 2, 1, t ^ 1).wait_send()
            relay_copy(k, full, t ^ 3, 0, t ^ 2).wait_recv()
            relay_copy(k, full, t ^ 3, 1, t ^ 1).wait_recv()

    mine = pl.ds(pl.multiple_of(t * S, S), S)

    def spread_start(k, share, full, own):
        own_copy(share, full, own).start()
        for j in range(1, nt):
            remote(
                share, full.at[mine], s.pl_s.at[k, j - 1], s.pl_r.at[k, j - 1], tensor=t ^ j
            ).start()

    def own_copy(share, full, own):
        return pltpu.make_async_copy(share, full.at[mine], s.load_sem.at[own])

    def spread_wait(k, share, full, own):
        own_copy(share, full, own).wait()
        for j in range(1, nt):
            peer = t ^ j
            theirs = pl.ds(pl.multiple_of(peer * S, S), S)
            copy = remote(share, full.at[theirs], s.pl_s.at[k, j - 1], s.pl_r.at[k, j - 1], tensor=peer)
            copy.wait_send()
            copy.wait_recv()

    def mirror(i, src, dst):
        return remote(src.at[mine], dst.at[mine], s.mi_s.at[i], s.mi_r.at[i], ctx=zz)

    def mirror_x1(d):
        cols = pl.ds(pl.multiple_of((d * n + (1 - zh) * nl) * R, 128), nl * R)
        return remote(
            s.x1.at[:, cols], s.x1b.at[:, pl.ds(d * nl * R, nl * R)], s.mi_s.at[2 + d], s.mi_r.at[2 + d], ctx=zz
        )

    def mirror_qkv():
        return remote(
            s.dqkv.at[pl.ds(0, T)], s.dqkv.at[pl.ds(T, T)], s.mi_s.at[4], s.mi_r.at[4], ctx=zz
        )

    def line_copy(k, all_ref, up, step, src=None):
        idx = (z - step) if up else (z + step)
        ref = all_ref.at[dp, idx]
        return remote(
            ref if src is None else src, ref,
            s.ag_s.at[k, 0 if up else 1, step], s.ag_r.at[k, 0 if up else 1, step],
            ctx=(z + 1) if up else (z - 1),
        )

    def core_copy(k, all_ref, slot, idx, src=None):
        ref = all_ref.at[dp, idx]
        return remote(
            ref if src is None else src, ref, s.agx_s.at[k, slot], s.agx_r.at[k, slot], dp=1 - dp
        )

    def gather_line_start(k, src, all_ref, ways, own):
        if own:
            pltpu.make_async_copy(src, all_ref.at[dp, z], s.own_sem.at[k]).start()
        for up in ways:

            @pl.when((z < n - 1) if up else (z > 0))
            def _(up=up):
                line_copy(k, all_ref, up, 0, src).start()

        if own:
            core_copy(k, all_ref, 0, z, src).start()

    def gather_line_step(k, all_ref, step, ways=(True, False)):
        for up in ways:

            @pl.when((z >= step) if up else (zz >= step))
            def _(up=up):
                idx = (z - step) if up else (z + step)
                ref = all_ref.at[dp, idx]
                i = 0 if up else 1
                remote(
                    ref, ref, s.ag_s.at[k, i, step - 1], s.ag_r.at[k, i, step - 1],
                    ctx=(z - 1) if up else (z + 1),
                ).wait_recv()
                if step < n - 1:

                    @pl.when((z < n - 1) if up else (z > 0))
                    def _():
                        line_copy(k, all_ref, up, step).start()

                core_copy(k, all_ref, step if up else n - 1 + step, idx).start()

    def gather_line_finish(k, src, all_ref):
        pltpu.make_async_copy(src, all_ref.at[dp, z], s.own_sem.at[k]).wait()
        for step in range(n - 1):

            @pl.when((z >= step) & (z < n - 1))
            def _():
                line_copy(k, all_ref, True, step, src).wait_send()

            @pl.when((zz >= step) & (z > 0))
            def _():
                line_copy(k, all_ref, False, step, src).wait_send()

        def both(slot, idx):
            ref = all_ref.at[1 - dp, idx]
            copy = remote(src, ref, s.agx_s.at[k, slot], s.agx_r.at[k, slot], dp=1 - dp)
            copy.wait_send()
            copy.wait_recv()

        both(0, z)
        for step in range(1, n):

            @pl.when(z >= step)
            def _():
                both(step, z - step)

            @pl.when(zz >= step)
            def _():
                both(n - 1 + step, z + step)

    me = dp * n + z

    def columns_src(k, src, block):
        if k < 2:
            rows = pl.ds(pl.multiple_of(lax.rem(block, n) * R + t * C, C), C)
            return src.at[rows, pl.ds(pl.multiple_of(block // n * T, T), T)]
        return src.at[mine, pl.ds(pl.multiple_of(block * R, R), R)]

    def columns_copy(k, src, all_ref, e, d):
        to_dp, to_z = dp ^ e, lax.rem(z + d, n)
        return remote(
            columns_src(k, src, to_dp * n + to_z), all_ref.at[t, me],
            s.aa_s.at[k, e * n + d], s.aa_r.at[k, e * n + d], dp=to_dp, ctx=to_z,
        )

    def columns_own(k, src, all_ref):
        return pltpu.make_async_copy(columns_src(k, src, me), all_ref.at[t, me], s.aa_s.at[k, 0])

    def columns_start(k, src, all_ref):
        columns_own(k, src, all_ref).start()
        for d in range(n):
            for e in range(2):
                if e or d:
                    columns_copy(k, src, all_ref, e, d).start()

    def columns_wait_send(k, src, all_ref):
        for e in range(2):
            for d in range(n):
                if e or d:
                    columns_copy(k, src, all_ref, e, d).wait_send()

    def columns_wait_recv(k, src, all_ref):
        columns_own(k, src, all_ref).wait()
        for e in range(2):
            for d in range(n):
                if e or d:
                    ref = all_ref.at[t, (dp ^ e) * n + lax.rem(z - d + n, n)]
                    remote(
                        columns_src(k, src, me), ref, s.aa_s.at[k, e * n + d], s.aa_r.at[k, e * n + d],
                        dp=dp ^ e, ctx=lax.rem(z - d + n, n),
                    ).wait_recv()

    def share_start(k, all_ref):
        for j in range(1, nt):
            remote(
                all_ref.at[t], all_ref.at[t], s.pl_s.at[10 + k, j - 1], s.pl_r.at[10 + k, j - 1], tensor=t ^ j
            ).start()

    def share_wait(k, all_ref):
        for j in range(1, nt):
            copy = remote(
                all_ref.at[t], all_ref.at[t ^ j], s.pl_s.at[10 + k, j - 1], s.pl_r.at[10 + k, j - 1], tensor=t ^ j
            )
            copy.wait_send()
            copy.wait_recv()

    def job_dp_start(job, k, b):
        slot = job.dp_slot(b)

        def body(c, w):
            slot[:, pl.ds(c, w)] = job.part((1 - dp) * nl + b, c, w).astype(BF16)

        tiles(job.cols, 512, body)
        remote(slot, job.dp_recv(b), s.dp_s.at[k, b], s.dp_r.at[k, b], dp=1 - dp).start()

    def job_dp_wait_send(job, k, b):
        remote(job.dp_slot(b), job.dp_recv(b), s.dp_s.at[k, b], s.dp_r.at[k, b], dp=1 - dp).wait_send()

    def job_dp_wait_all(job, k):
        for b in range(nl):
            remote(job.dp_slot(b), job.dp_recv(b), s.dp_s.at[k, b], s.dp_r.at[k, b], dp=1 - dp).wait_recv()

    def chain_copy(job, k, up, step, part):
        i = 0 if up else 1
        width = job.cols // 2
        cols = pl.ds(part * width, width)
        return remote(
            job.chain_slot(up, step).at[:, cols], job.chain(up, step).at[:, cols],
            s.ch_s.at[k, i, step, part], s.ch_r.at[k, i, step, part],
            ctx=(z + 1) if up else (z - 1),
        )

    def chain_step(job, k, step, ways=(True, False), parts=(0, 1)):
        width = job.cols // 2
        for part in parts:
            for up in ways:
                pos = zl if up else zzl

                @pl.when((pos <= step) & (pos < nl - 1))
                def _(up=up, pos=pos, part=part):
                    target = (zl + nl - 1 - step) if up else (zl - (nl - 1 - step))
                    slot = job.chain_slot(up, step)
                    if step:

                        @pl.when(pos >= 1)
                        def _():
                            chain_copy(job, k, up, step - 1, part).wait_recv()

                    def body(c, w):
                        cs = pl.ds(pl.multiple_of(part * width + c, 128), w)
                        total = job.part(dp * nl + target, cs.start, w)
                        total = total + job.dp_recv(target)[:, cs].astype(F32)
                        if step:
                            prev = job.chain(up, step - 1)[:, cs].astype(F32)
                            total = total + jnp.where(pos >= 1, prev, 0.0)
                        slot[:, cs] = total.astype(BF16)

                    tiles(width, 256 if width % 256 == 0 else 128, body)
                    chain_copy(job, k, up, step, part).start()

    def chain_wait_send(job, k, step):
        for up in (True, False):
            pos = zl if up else zzl

            @pl.when((pos <= step) & (pos < nl - 1))
            def _(up=up):
                for part in range(2):
                    chain_copy(job, k, up, step, part).wait_send()

    def chain_final(job, k, out_ref):
        width = job.cols // 2
        for part in range(2):
            for up in (True, False):
                pos = zl if up else zzl

                @pl.when(pos >= 1)
                def _(up=up, part=part):
                    chain_copy(job, k, up, nl - 2, part).wait_recv()

            def body(c, w):
                cs = pl.ds(pl.multiple_of(part * width + c, 128), w)
                total = job.part(dp * nl + zl, cs.start, w) + job.dp_recv(zl)[:, cs].astype(F32)
                a = job.chain(True, nl - 2)[:, cs].astype(F32)
                b = job.chain(False, nl - 2)[:, cs].astype(F32)
                out_ref[:, cs] = total + jnp.where(zl >= 1, a, 0.0) + jnp.where(zzl >= 1, b, 0.0)

            tiles(width, 256 if width % 256 == 0 else 128, body)

    L = seg_row.shape[1]
    s.segs[:, : reach * T] = jnp.full((1, reach * T), -1, jnp.int32)
    s.segs[:, reach * T :] = seg_row[...]
    row = seg_row[...]
    at_me = lax.broadcasted_iota(jnp.int32, (T, L), 1) == lax.broadcasted_iota(jnp.int32, (T, L), 0) + z * T
    row_f = jnp.broadcast_to(row.astype(F32), (T, L))
    qseg_f = jnp.sum(jnp.where(at_me, row_f, 0.0), axis=1, keepdims=True)
    begins = jnp.sum(jnp.where(row_f < qseg_f, 1.0, 0.0), axis=1, keepdims=True)
    position = (lax.broadcasted_iota(jnp.int32, (T, H), 0) + z * T).astype(F32) - begins
    angles = position * inverse[...]
    cos[...] = jnp.cos(angles)
    lane = lax.broadcasted_iota(jnp.int32, (T, H), 1)
    turned = jnp.sin(angles)
    sin[...] = jnp.where(lane < H // 2, -turned, turned)

    rows_i = lax.broadcasted_iota(jnp.int32, (T, span), 0) + reach * T
    cols_i = lax.broadcasted_iota(jnp.int32, (T, span), 1)
    kseg_f = s.segs[:, pl.ds(pl.multiple_of(z * T, T), span)].astype(F32)
    allowed = (cols_i <= rows_i) & (qseg_f == kseg_f)
    s.mask[...] = jnp.where(allowed, 1.0, 0.0).astype(F32)

    l_tok.wait()
    x = s.tok[...].astype(F32)
    scale = lax.rsqrt(jnp.mean(x * x, axis=-1, keepdims=True) + epsilon)
    s.x1[...] = (x * scale * g1[...]).astype(BF16)
    s.tokshare[...] = s.tok[mine, :].astype(F32)

    def rms(v):
        return lax.rsqrt(jnp.mean(v * v, axis=-1, keepdims=True) + epsilon)

    def rope(v):
        return v * cos[...] + pltpu.roll(v, H // 2, 1) * sin[...]

    def rope_back(g):
        return g * cos[...] + pltpu.roll(g * sin[...], H // 2, 1)

    own_rows = pl.ds(reach * T, T)
    l_kw.wait()
    l_vw.wait()
    def kv_copy(r, c):
        lanes = pl.ds(c * 2 * H, 2 * H)
        return remote(
            s.kv.at[pl.ds((reach - r + 1) * T, T), lanes], s.kv.at[pl.ds((reach - r) * T, T), lanes],
            s.kv_s.at[r - 1, c], s.kv_r.at[r - 1, c], ctx=z + 1,
        )

    def kv_send(r, c):
        @pl.when((z < n - 1) & (z >= r - 1))
        def _():
            kv_copy(r, c).start()

    for h in range(KH):
        hs = pl.ds(h * H, H)
        raw = dot(s.x1[...], s.kw[:, hs])
        s.k_raw[:, hs] = raw
        s.kv[own_rows, 2 * h * H : (2 * h + 1) * H] = rope(raw * rms(raw) * gk[...]).astype(BF16)
        s.kv[own_rows, (2 * h + 1) * H : (2 * h + 2) * H] = dot(s.x1[...], s.vw[:, hs]).astype(BF16)
        if h == 0:
            pl.semaphore_wait(barrier, (nt - 1) + (2 * n - 1))
        kv_send(1, h)
    l_cot.wait()
    pl.when(zh == 1)(lambda: mirror(0, s.cot, s.cot2).start())
    for r in range(1, reach + 1):

        @pl.when(z < r)
        def _():
            s.kv[pl.ds((reach - r) * T, T), :] = jnp.zeros((T, 2 * KV), BF16)

    l_qw.wait()
    s.q_raw[...] = dot(s.x1[...], s.qw[...])
    for h in range(QH):
        raw = s.q_raw[:, h * H : (h + 1) * H]
        s.q_rot[:, h * H : (h + 1) * H] = rope(raw * rms(raw) * gq[...]).astype(BF16)
    for r in range(1, reach + 1):
        for c in range(KH):

            @pl.when(z >= r)
            def _(r=r, c=c):
                kv_copy(r, c).wait_recv()

            if r < reach:
                kv_send(r + 1, c)
    def weights_of(h, g):
        hs = pl.ds(pl.multiple_of(h * H, H), H)
        q = s.q_rot[:, hs]
        k = s.kv[:, pl.ds(pl.multiple_of(2 * g * H, H), H)]
        return q, k, jnp.where(s.mask[...] > 0.0, jnp.exp(dot_nt(q, k) * inv_root), 0.0)

    def attend(h, _):
        g = h // group
        hs = pl.ds(pl.multiple_of(h * H, H), H)
        _q, _k, w = weights_of(h, g)
        v = s.kv[:, pl.ds(pl.multiple_of((2 * g + 1) * H, H), H)]
        total = jnp.sum(w, axis=-1, keepdims=True)
        att = dot(w.astype(BF16), v) / total
        s.tot[:, hs] = jnp.broadcast_to(total, (T, H))
        s.att[:, hs] = att
        s.att_low[:, hs] = att.astype(BF16)
        s.attt[hs, :] = att.T.astype(BF16)
        return 0

    lax.fori_loop(0, QH, attend, 0)

    l_ow.wait()

    def body(c, w):
        s.send_a[:, pl.ds(c, w)] = dot(s.att_low[...], s.ow[:, pl.ds(c, w)]).astype(BF16)

    tiles(D, TILE, body)
    scatter_start(0, s.send_a, s.recv0)
    gather_line_start(2, s.attt, att_all, (False,), True)

    def transpose_half(src, dst, place):
        for d in range(2):

            def body(c, w):
                cs = pl.ds(pl.multiple_of((d * n + zh * nl) * R + c, 128), w)
                rows = pl.ds(pl.multiple_of(d * nl * R + c, 128), w)
                dst[rows, place * T : (place + 1) * T] = src[:, cs].astype(F32).T.astype(BF16)

            tiles(nl * R, TILE, body)

    s.cotshare[...] = s.cot[mine, :].astype(F32)

    transpose_half(s.x1, s.x1t, 0)
    transpose_half(s.cot, s.cott, 0)
    l_dw.wait()

    def hidden_grad(cot, out):
        def body(c, w):
            out[:, pl.ds(c, w)] = dot_nt(cot[...], s.dw[pl.ds(c, w), :])

        tiles(F, TILE, body)

    def cot_share():
        mirror(0, s.cot, s.cot2).wait_recv()
        gather_start(9, s.cot2)

    hidden_grad(s.cot, s.gh)
    pl.when(z == nl - 1)(lambda: mirror(0, s.cot, s.cot2).start())

    s.resid[...] = scatter_sum(0, s.send_a, s.recv0, s.tokshare[...])
    resid = s.resid[...]
    s.x2[mine, :] = (resid * rms(resid) * g2[...]).astype(BF16)
    gather_start(1, s.x2)
    mirror(1, s.x2, s.x2b).start()
    gather_line_step(2, att_all, 1, (False,))
    l_gw.wait()
    l_uw.wait()
    gather_forward(1, s.x2)
    pl.when(z < nl - 1)(lambda: mirror(0, s.cot, s.cot2).start())
    gather_wait(1, s.x2)

    def mirrored_share():
        mirror(1, s.x2, s.x2b).wait_recv()
        gather_start(10, s.x2b)

    cot_share()

    def feed(x, grad_hidden, place):
        rows = pl.ds(place * T, T)

        def body(c, w):
            cs = pl.ds(c, w)
            gate = dot(x[...], s.gw[:, cs])
            up = dot(x[...], s.uw[:, cs])
            gh = grad_hidden[:, cs]
            sig = jax.nn.sigmoid(gate)
            act = gate * sig
            s.hid[rows, cs] = (act * up).astype(BF16)
            s.gg[rows, cs] = (gh * up * (sig * (1.0 + gate * (1.0 - sig)))).astype(BF16)
            s.gu[rows, cs] = (gh * act).astype(BF16)

        tiles(F, TILE, body)

    feed(s.x2, s.gh, 0)
    mirrored_share()
    gather_forward(9, s.cot2)
    gather_line_start(2, s.attt, att_all, (True,), False)
    gather_line_step(2, att_all, 2, (False,))
    own_part = pl.ds(0, T)

    def body(c, w):
        rs = pl.ds(c, w)
        s.send_a[:, rs] = (
            dot_nt(s.gg[own_part, :], s.gw[rs, :]) + dot_nt(s.gu[own_part, :], s.uw[rs, :])
        ).astype(BF16)

    tiles(D, TILE, body)
    transpose_half(s.x2, s.xt, 0)
    gather_forward(10, s.x2b)
    mirror(1, s.x2, s.x2b).wait_send()
    scatter_start(2, s.send_a, s.recv1)
    for d in range(2):
        mirror_x1(d).start()

    def body(c, w):
        s.send_b[:, pl.ds(c, w)] = dot(s.hid[own_part, :], s.dw[:, pl.ds(c, w)]).astype(BF16)

    tiles(D, TILE, body)
    gather_wait(9, s.cot2)
    hidden_grad(s.cot2, s.gh2)
    transpose_half(s.cot2, s.cott, 1)
    gather_wait(10, s.x2b)
    feed(s.x2b, s.gh2, 1)
    transpose_half(s.x2b, s.xt, 1)
    pl.semaphore_signal(s.credit, inc=1, device_id={"dp": 1 - dp}, device_id_type=MESH)

    grad_second = scatter_sum(2, s.send_a, s.recv1, jnp.zeros((S, D), F32))
    resid = s.resid[...]
    scale = rms(resid)
    normed = resid * scale
    s.gains[:, D : 2 * D] = jnp.sum(grad_second * normed, axis=0, keepdims=True)
    scaled = grad_second * g2[...]
    inner = jnp.mean(scaled * normed, axis=-1, keepdims=True)
    s.gresid[...] = s.cotshare[...] + scale * (scaled - normed * inner)
    s.gm[mine, :] = s.gresid[...].astype(BF16)
    gather_start(4, s.gm)
    columns_start(2, s.gm, s.gmc)

    class WeightJob:
        def __init__(self, k, left, grad):
            self.k, self.left, self.grad, self.cols = k, left, grad, grad.shape[1]

        def part(self, block, c, w):
            rows = pl.ds(pl.multiple_of(block * R, R), R)
            return dot(self.left[rows, :], self.grad[:, pl.ds(c, w)])

        def dp_slot(self, b):
            return s.gw.at[pl.ds(b * R, R), pl.ds(0, self.cols)]

        def dp_recv(self, b):
            return s.uw.at[pl.ds(pl.multiple_of((self.k * nl + b) * R, R), R), pl.ds(0, self.cols)]

        def chain_slot(self, up, step):
            i = nl + self.k * (nl - 1) + (step if up else nl - 2 - step)
            return s.gw.at[pl.ds(i * R, R), pl.ds(0, self.cols)]

        def chain(self, up, step):
            return s.chain.at[self.k, 0 if up or nl == 2 else 1, step, :, pl.ds(0, self.cols)]

    jobs = [
        WeightJob(0, s.cott, s.hid),
        WeightJob(1, s.xt, s.gg),
        WeightJob(2, s.xt, s.gu),
        WeightJob(3, s.x1t, s.dqkv),
    ]
    order = [b for i in range((nl + 1) // 2) for b in dict.fromkeys((nl - 1 - i, i))]

    def job_dp(k):
        for b in order:
            if k:
                job_dp_wait_send(jobs[k - 1], k - 1, b)
            job_dp_start(jobs[k], k, b)

    pl.semaphore_wait(s.credit, 1)
    job_dp(0)
    job_dp_wait_all(jobs[0], 0)
    chain_step(jobs[0], 0, 0)
    gather_forward(4, s.gm)
    gather_line_step(2, att_all, 1, (True,))
    job_dp(1)
    gather_wait(4, s.gm)
    scatter_start(3, s.send_b, s.recv2)
    for d in range(2):
        mirror_x1(d).wait_recv()

    def body(c, w):
        s.x1t[pl.ds(c, w), T : 2 * T] = s.x1b[:, pl.ds(c, w)].astype(F32).T.astype(BF16)

    tiles(D // 2, TILE, body)

    gatt = s.gh.at[:, pl.ds(0, QH * H)]

    def body(c, w):
        gatt[:, pl.ds(c, w)] = dot_nt(s.gm[...], s.ow[pl.ds(c, w), :])

    tiles(QH * H, TILE, body)
    s.gq_acc[...] = jnp.zeros((1, H), F32)

    def back(g, _):
        ks = pl.ds(pl.multiple_of(g * H, H), H)
        vs = pl.ds(pl.multiple_of(KV + g * H, H), H)
        v = s.kv[:, pl.ds(pl.multiple_of((2 * g + 1) * H, H), H)]
        grad_k = jnp.zeros((span, H), F32)
        grad_v = jnp.zeros((span, H), F32)
        for i in range(group):
            h = g * group + i
            hs = pl.ds(pl.multiple_of(h * H, H), H)
            q, k, w = weights_of(h, g)
            ga, total = gatt[:, hs], s.tot[:, hs]
            gs = (ga / total).astype(BF16)
            delta = jnp.sum(ga * s.att[:, hs], axis=-1, keepdims=True) / total[:, :1]
            ds = (w * (dot_nt(gs, v) - delta)).astype(BF16)
            grad_k = grad_k + dot_tn(ds, q) * inv_root
            grad_v = grad_v + dot_tn(w.astype(BF16), gs)
            gr = rope_back(dot(ds, k) * inv_root)
            raw = s.q_raw[:, hs]
            r = rms(raw)
            nq = raw * r
            s.gq_acc[...] += jnp.sum(gr * nq, axis=0, keepdims=True)
            sc = gr * gq[...]
            s.dqkv[:T, hs] = (r * (sc - nq * jnp.mean(sc * nq, axis=-1, keepdims=True))).astype(BF16)
        s.dkv[:, ks] = grad_k.astype(BF16)
        s.dkv[:, vs] = grad_v.astype(BF16)
        return 0

    lax.fori_loop(0, KH, back, 0)
    s.gains[:, 2 * D : 2 * D + H] = s.gq_acc[...]

    def dkv_copy(i):
        return remote(
            s.dkv.at[pl.ds(i * T, T)], s.dkv_in.at[i], s.dkv_s.at[i], s.dkv_r.at[i], ctx=z - 1
        )

    for i in range(reach):
        if i:

            @pl.when((z < n - 1) & (z + 1 >= reach - i + 1))
            def _():
                dkv_copy(i - 1).wait_recv()
                rows = pl.ds(i * T, T)
                s.dkv[rows, :] = (s.dkv[rows, :].astype(F32) + s.dkv_in[i - 1].astype(F32)).astype(BF16)

        @pl.when(z >= reach - i)
        def _():
            dkv_copy(i).start()

        if i == 0:
            job_dp_wait_all(jobs[1], 1)
            chain_step(jobs[1], 1, 0, (True,))
            pl.when(zh == 0)(lambda: chain_step(jobs[1], 1, 0, (False,), (0,)))
            job_dp(2)

    pl.when(zh == 0)(lambda: chain_step(jobs[1], 1, 0, (False,), (1,)))

    @pl.when(z < n - 1)
    def _():
        dkv_copy(reach - 1).wait_recv()

    own = s.dkv[pl.ds(reach * T, T), :].astype(F32)
    own = own + jnp.where(z < n - 1, s.dkv_in[reach - 1].astype(F32), 0.0)
    s.dqkv[:T, QH * H + KV :] = own[:, KV:].astype(BF16)
    gk_sum = jnp.zeros((1, H), F32)
    for h in range(KH):
        gr = rope_back(own[:, h * H : (h + 1) * H])
        raw = s.k_raw[:, h * H : (h + 1) * H]
        r = rms(raw)
        nk = raw * r
        gk_sum = gk_sum + jnp.sum(gr * nk, axis=0, keepdims=True)
        sc = gr * gk[...]
        s.dqkv[:T, QH * H + h * H : QH * H + (h + 1) * H] = (
            r * (sc - nk * jnp.mean(sc * nk, axis=-1, keepdims=True))
        ).astype(BF16)
    s.gains[:, 2 * D + H :] = gk_sum
    pl.when(zh == 1)(lambda: chain_step(jobs[1], 1, 0, (False,)))
    mirror_qkv().start()
    gather_line_step(2, att_all, 2, (True,))
    job_dp_wait_all(jobs[2], 2)
    chain_step(jobs[2], 2, 0)

    s.outsh[...] = scatter_sum(3, s.send_b, s.recv2, s.resid[...]).astype(BF16)
    spread_start(5, s.outsh, out_hbm, 0)
    q_c, k_c, v_c = pl.ds(0, QH * H), pl.ds(QH * H, KV), pl.ds(QH * H + KV, KV)

    def body(c, w):
        rs = pl.ds(c, w)
        s.send_a[:, rs] = (
            dot_nt(s.dqkv[:T, q_c], s.qw[rs, :])
            + dot_nt(s.dqkv[:T, k_c], s.kw[rs, :])
            + dot_nt(s.dqkv[:T, v_c], s.vw[rs, :])
        ).astype(BF16)

    tiles(D, TILE, body)
    scatter_start(6, s.send_a, s.recv3)
    grad_first = scatter_sum(6, s.send_a, s.recv3, jnp.zeros((S, D), F32))
    tokshare = s.tokshare[...]
    scale = rms(tokshare)
    normed = tokshare * scale
    s.gains[:, :D] = jnp.sum(grad_first * normed, axis=0, keepdims=True)
    scaled = grad_first * g1[...]
    inner = jnp.mean(scaled * normed, axis=-1, keepdims=True)
    s.tgsh[...] = (s.gresid[...] + scale * (scaled - normed * inner)).astype(BF16)
    for j in range(1, nt):
        remote(s.gains, s.gains_p.at[j - 1], s.pl_s.at[8, j - 1], s.pl_r.at[8, j - 1], tensor=t ^ j).start()
    spread_start(7, s.tgsh, tgrad_hbm, 1)
    for j in range(1, nt):
        remote(s.gains, s.gains_p.at[j - 1], s.pl_s.at[8, j - 1], s.pl_r.at[8, j - 1], tensor=t ^ j).wait()
    total = s.gains[...]
    for j in range(1, nt):
        total = total + s.gains_p[j - 1]
    s.gains2[...] = total

    def gain_copy(e, d):
        i = e * n + d
        return remote(
            s.gains2, s.gains_x.at[i - 1], s.ga_s.at[i], s.ga_r.at[i], dp=dp ^ e, ctx=lax.rem(z + d, n)
        )

    for e in range(2):
        for d in range(n):
            if e or d:
                gain_copy(e, d).start()
    columns_wait_recv(2, s.gm, s.gmc)
    share_start(2, s.gmc)
    stage = s.gh2.at[pl.ds(0, R), pl.ds(0, QH * H + 2 * KV)]

    def gate_copy():
        return pltpu.make_async_copy(s.gh.at[pl.ds(0, R)], gate_out, s.load_sem.at[2])

    def up_copy():
        return pltpu.make_async_copy(s.gh.at[pl.ds(0, R)], up_out, s.load_sem.at[3])

    def qkv_copies():
        parts = [(q_out, 0, QH * H), (k_out, QH * H, KV), (v_out, QH * H + KV, KV)]
        return [
            pltpu.make_async_copy(stage.at[:, pl.ds(a, w)], ref, s.load_sem.at[6 + i])
            for i, (ref, a, w) in enumerate(parts)
        ]

    for step in range(1, nl - 1):
        for k in range(3):
            chain_step(jobs[k], k, step)
    rows = pl.ds(0, R)
    chain_final(jobs[0], 0, s.gh.at[rows])
    width = min(256, F)
    flip = s.gh2.at[:, pl.ds(QH * H + 2 * KV, 2 * R)]

    def down_copy(i):
        return pltpu.make_async_copy(
            flip.at[pl.ds(0, width), pl.ds((i % 2) * R, R)],
            down_out.at[pl.ds(i * width, width)],
            s.load_sem.at[4 + i % 2],
        )

    count = F // width
    for i in range(count):
        if i >= 2:
            down_copy(i - 2).wait()
        flip[:width, (i % 2) * R : (i % 2 + 1) * R] = s.gh[rows, i * width : (i + 1) * width].T
        down_copy(i).start()
    for i in range(max(0, count - 2), count):
        down_copy(i).wait()
    mirror_qkv().wait_recv()
    job_dp(3)
    job_dp_wait_all(jobs[3], 3)
    chain_step(jobs[3], 3, 0)
    for step in range(1, nl - 1):
        chain_step(jobs[3], 3, step)


    chain_final(jobs[1], 1, s.gh.at[rows])
    gate_copy().start()
    for step in range(3, n):
        gather_line_step(2, att_all, step)
    gather_line_finish(2, s.attt, att_all)
    share_wait(2, s.gmc)

    def load(i):
        slot = lax.rem(i, 2)
        return pltpu.make_async_copy(
            att_all.at[i // n, lax.rem(i, n)],
            s.dw.at[pl.ds(pl.multiple_of(slot * QH * H, QH * H), QH * H), pl.ds(0, T)],
            s.stage_sem.at[slot],
        )

    load(0).start()
    s.outw[...] = jnp.zeros(s.outw.shape, F32)

    def step(i, _):
        @pl.when(i + 1 < 2 * n)
        def _():
            load(i + 1).start()

        load(i).wait()
        slot = lax.rem(i, 2)
        left = s.dw[pl.ds(pl.multiple_of(slot * QH * H, QH * H), QH * H), pl.ds(0, T)]
        s.outw[...] += dot(left, s.gmc[:, i].reshape(T, R))
        return 0

    lax.fori_loop(0, 2 * n, step, 0)

    def outw_copy():
        return pltpu.make_async_copy(s.outw, outw_out, s.load_sem.at[4])

    outw_copy().start()
    gate_copy().wait()
    chain_final(jobs[2], 2, s.gh.at[rows])
    up_copy().start()
    chain_final(jobs[3], 3, stage)
    for copy in qkv_copies():
        copy.start()
    for e in range(2):
        for d in range(n):
            if e or d:
                gain_copy(e, d).wait()
    total = s.gains2[...]
    for i in range(2 * n - 1):
        total = total + s.gains_x[i]
    s.gains[...] = total

    def gains_copy():
        return pltpu.make_async_copy(s.gains, gains_out, s.load_sem.at[2])

    gains_copy().start()

    columns_wait_send(2, s.gm, s.gmc)
    mirror(0, s.cot, s.cot2).wait_send()
    mirror_qkv().wait_send()
    for d in range(2):
        mirror_x1(d).wait_send()
    for b in order:
        job_dp_wait_send(jobs[-1], len(jobs) - 1, b)
    for st in range(nl - 1):
        for k, job in enumerate(jobs):
            chain_wait_send(job, k, st)
    for r in range(1, reach + 1):

        @pl.when((z < n - 1) & (z >= r - 1))
        def _(r=r):
            for c in range(KH):
                kv_copy(r, c).wait_send()

    for i in range(reach):

        @pl.when(z >= reach - i)
        def _():
            dkv_copy(i).wait_send()

    spread_wait(5, s.outsh, out_hbm, 0)
    spread_wait(7, s.tgsh, tgrad_hbm, 1)
    gains_copy().wait()
    up_copy().wait()
    outw_copy().wait()
    for copy in qkv_copies():
        copy.wait()


def run_layer(dm, *operands):
    T, D, H, F, n, nt, reach, S, R = dm.T, dm.D, dm.H, dm.F, dm.n, dm.nt, dm.reach, dm.S, dm.R
    QC, KV = dm.QH * H, dm.KH * H
    span = (reach + 1) * T
    G = 2 * D + 2 * H
    dma = pltpu.SemaphoreType.DMA
    scratch = dict(
        tok=((T, D), BF16), x1=((T, D), BF16), send_b=((T, D), BF16), cot=((T, D), BF16), x2=((T, D), BF16),
        outsh=((S, D), BF16), tgsh=((S, D), BF16), xt=((D // 2, 2 * T), BF16), cott=((D // 2, 2 * T), BF16),
        cot2=((T, D), BF16), x2b=((T, D), BF16),
        qw=((D, QC), BF16), kw=((D, KV), BF16), vw=((D, KV), BF16), ow=((QC, D), BF16),
        gw=((D, F), BF16), uw=((D, F), BF16), dw=((F, D), BF16),
        tokshare=((S, D), F32), cotshare=((S, D), F32), resid=((S, D), F32), gresid=((S, D), F32),
        k_raw=((T, KV), F32), q_raw=((T, QC), F32), q_rot=((T, QC), BF16), kv=((span, 2 * KV), BF16),
        mask=((T, span), F32), tot=((T, QC), F32), att=((T, QC), F32), att_low=((T, QC), BF16),
        attt=((QC, T), BF16), gq_acc=((1, H), F32),
        recv0=((6, S, D // 2) if nt == 4 else (nt - 1, S, D), BF16),
        recv1=((6, S, D // 2) if nt == 4 else (nt - 1, S, D), BF16), pair=((2, S, D // 2), BF16),
        gh=((T, F), F32), hid=((2 * T, F), BF16), gg=((2 * T, F), BF16), gu=((2 * T, F), BF16),
        dkv=((span, 2 * KV), BF16), dkv_in=((reach, T, 2 * KV), BF16), dqkv=((2 * T, QC + 2 * KV), BF16),
        chain=((4, 1 if n == 4 else 2, n // 2 - 1, R, F), BF16),

        gmc=((nt, 2 * n, S, R), BF16), x1b=((T, D // 2), BF16), x1t=((D // 2, 2 * T), BF16), gh2=((T, F), F32),
        cos=((T, H), F32), sin=((T, H), F32), segs=((1, reach * T + dm.L), jnp.int32),
        outw=((QC, R), F32), gain_in=((1, G), F32), gains=((1, G), F32), gains2=((1, G), F32), gains_p=((nt - 1, 1, G), F32),
        gains_x=((2 * n - 1, 1, G), F32),
    )
    sems = dict(
        load_sem=(9,), own_sem=(3,), pl_s=(13, nt - 1), pl_r=(13, nt - 1), ag_s=(3, 2, n - 1), ag_r=(3, 2, n - 1),
        agx_s=(3, 2 * n - 1), agx_r=(3, 2 * n - 1), aa_s=(3, 2 * n), aa_r=(3, 2 * n), stage_sem=(2,),
        dp_s=(4, n // 2), dp_r=(4, n // 2), ch_s=(4, 2, n // 2 - 1, 2), ch_r=(4, 2, n // 2 - 1, 2), mi_s=(5,), mi_r=(5,), kv_s=(reach, KV // H), kv_r=(reach, KV // H), pl2_s=(11,), pl2_r=(11,), rs_s=(7, 6), rs_r=(7, 6),
        dkv_s=(reach,), dkv_r=(reach,), ga_s=(2 * n,), ga_r=(2 * n,),
    )
    names = list(scratch) + list(sems) + ["credit"]
    shapes = [pltpu.VMEM(*v) for v in scratch.values()] + [dma(v) for v in sems.values()]
    shapes.append(pltpu.SemaphoreType.REGULAR)

    def body(*refs):
        fixed = len(refs) - len(names)
        s = Dims()
        for name, ref in zip(names, refs[fixed:]):
            setattr(s, name, ref)
        for alias, of in dm.alias.items():
            setattr(s, alias, getattr(s, of))
        layer_kernel(dm, *refs[:fixed], s)

    hbm = pl.BlockSpec(memory_space=pl.ANY)
    vmem = pl.BlockSpec(memory_space=pltpu.VMEM)
    return pl.pallas_call(
        body,
        out_shape=(
            jax.ShapeDtypeStruct((T, D), BF16),
            jax.ShapeDtypeStruct((T, D), BF16),
            jax.ShapeDtypeStruct((R, F), F32),
            jax.ShapeDtypeStruct((R, F), F32),
            jax.ShapeDtypeStruct((F, R), F32),
            jax.ShapeDtypeStruct((R, QC), F32),
            jax.ShapeDtypeStruct((R, KV), F32),
            jax.ShapeDtypeStruct((R, KV), F32),
            jax.ShapeDtypeStruct((QC, R), F32),
            jax.ShapeDtypeStruct((1, G), F32),
            jax.ShapeDtypeStruct((2, n, QC, T), BF16),
        ),
        in_specs=[hbm] * 2 + [vmem] * 6 + [hbm] * 7,
        out_specs=[hbm] * 11,
        scratch_shapes=shapes,
        compiler_params=pltpu.CompilerParams(
            collective_id=0, has_side_effects=True, vmem_limit_bytes=67043328
        ),
        name="layer",
    )(*operands)


FINISH_WINDOW = 64


def finish_pieces(shape):
    rows = shape[0]
    step = rows // 2 if rows % 32 == 0 else rows
    return [(r, step) for r in range(0, rows, step)]


def finish_kernel(dm, *refs):
    count = len(dm.finish)
    ins, gains, outs = refs[:count], refs[count], refs[count + 1 : 2 * count + 1]
    gain_outs = refs[2 * count + 1 : 2 * count + 5]
    bufs, load_sem, store_sem = refs[2 * count + 5 : 3 * count + 5], refs[-2], refs[-1]
    loads, stores = [], []
    for a, b, c in zip(ins, bufs, outs):
        for start, size in finish_pieces(a.shape):
            rows, i = pl.ds(start, size), len(loads)
            loads.append(pltpu.make_async_copy(a.at[rows], b.at[rows], load_sem.at[i]))
            stores.append(pltpu.make_async_copy(b.at[rows], c.at[rows], store_sem.at[i]))
    for load in loads[:FINISH_WINDOW]:
        load.start()
    place = 0
    for ref in gain_outs:
        ref[...] = gains[:, place : place + ref.shape[1]]
        place += ref.shape[1]
    for i, (load, store) in enumerate(zip(loads, stores)):
        load.wait()
        store.start()
        if i + FINISH_WINDOW < len(loads):
            loads[i + FINISH_WINDOW].start()
    for store in stores:
        store.wait()


def finish(dm, arrays, gains):
    dm.finish = arrays
    hbm = pl.BlockSpec(memory_space=pl.ANY)
    vmem = pl.BlockSpec(memory_space=pltpu.VMEM)
    shapes = [jax.ShapeDtypeStruct(a.shape, a.dtype) for a in arrays]
    gain_shapes = [jax.ShapeDtypeStruct((1, w), F32) for w in (dm.D, dm.D, dm.H, dm.H)]
    dma = pltpu.SemaphoreType.DMA((sum(len(finish_pieces(a.shape)) for a in arrays),))
    return pl.pallas_call(
        functools.partial(finish_kernel, dm),
        out_shape=tuple(shapes + gain_shapes),
        in_specs=[hbm] * len(arrays) + [vmem],
        out_specs=tuple([hbm] * len(arrays) + [vmem] * 4),
        scratch_shapes=[pltpu.VMEM(a.shape, a.dtype) for a in arrays] + [dma, dma],
        compiler_params=pltpu.CompilerParams(vmem_limit_bytes=67043328),
        name="finish",
    )(*arrays, gains)


def per_device(
    tokens,
    segments,
    first_gain,
    query_weight,
    key_matrix,
    value_matrix,
    query_norm_gain,
    key_gain,
    output_weight,
    second_gain,
    gate_weight,
    up_weight,
    down_weight,
    cotangent,
):
    _, T, D = tokens.shape
    dm = Dims()
    dm.T, dm.D, dm.H, dm.F = T, D, query_norm_gain.shape[0], gate_weight.shape[1]
    dm.QH, dm.KH = query_weight.shape[1] // dm.H, key_matrix.shape[1] // dm.H
    dm.n, dm.nt = lax.axis_size("ctx"), lax.axis_size("tensor")
    length = segments.shape[1]
    dm.reach = -(-(length // 2 - 1) // T)
    dm.S, dm.R = T // dm.nt, D // (2 * dm.n)
    dm.alias = {"send_a": "tok", "gm": "x2", "recv2": "recv0", "recv3": "recv1"}
    H = dm.H
    dm.L = length
    inverse = (1.0 / rope_base ** (np.arange(0, H, 2, dtype=np.float32) / np.float32(H))).astype(np.float32)
    inverse = np.concatenate([inverse, inverse])[None]
    out, tgrad, gate_g, up_g, down_g, q_g, k_g, v_g, out_g, gains = run_layer(
        dm,
        tokens.reshape(T, D),
        cotangent.reshape(T, D),
        first_gain.reshape(-1, H),
        second_gain.reshape(-1, H),
        query_norm_gain.reshape(1, H),
        key_gain.reshape(1, H),
        inverse,
        segments,
        query_weight,
        key_matrix,
        value_matrix,
        output_weight,
        gate_weight,
        up_weight,
        down_weight,
    )[:10]
    out, tgrad, gate_g, up_g, down_g, q_g, k_g, v_g, out_g, first_g, second_g, qn_g, kn_g = finish(
        dm, (out, tgrad, gate_g, up_g, down_g, q_g, k_g, v_g, out_g), gains
    )
    return (
        out.reshape(tokens.shape),
        tgrad.reshape(tokens.shape),
        first_g.reshape(D),
        q_g,
        k_g,
        v_g,
        qn_g.reshape(H),
        kn_g.reshape(H),
        out_g,
        second_g.reshape(D),
        gate_g,
        up_g,
        down_g,
    )


def solution(mesh):
    return jax.shard_map(
        per_device,
        mesh=mesh,
        in_specs=(
            P("dp", "ctx", None),
            P("dp", None),
            P(),
            P(None, "tensor"),
            P(None, "tensor"),
            P(None, "tensor"),
            P(),
            P(),
            P("tensor", None),
            P(),
            P(None, "tensor"),
            P(None, "tensor"),
            P("tensor", None),
            P("dp", "ctx", None),
        ),
        out_specs=(
            P("dp", "ctx", None),
            P("dp", "ctx", None),
            P(),
            P(("dp", "ctx"), "tensor"),
            P(("dp", "ctx"), "tensor"),
            P(("dp", "ctx"), "tensor"),
            P(),
            P(),
            P("tensor", ("dp", "ctx")),
            P(),
            P(("dp", "ctx"), "tensor"),
            P(("dp", "ctx"), "tensor"),
            P("tensor", ("dp", "ctx")),
        ),
        check_vma=False,
    )
```
